16 devices in a mesh: dp: 2 (over y, z), tp: 8 (over x, core).
Axes of the slice: x: 4, y: 2, z: 1, core: 2. Of those that a mesh axis runs over, the one named last changes fastest.
The devices are a block of a 4x4x8 slice.
Arguments:
- x_in: bfloat16 [16, 512, 6144], P('dp', 'tp'), parts along dimension 0
- ln_gamma: float32 [6144], replicated
- ln_beta: float32 [6144], replicated
- w_q: bfloat16 [6144, 6144], P(None, 'tp')
- b_q: float32 [6144], P('tp')
- w_kv: bfloat16 [6144, 256], replicated
- b_kv: float32 [256], replicated
- w_o: bfloat16 [6144, 6144], P('tp')
- b_o: float32 [6144], replicated
- grad_y: bfloat16 [16, 512, 6144], P('dp', 'tp'), parts along dimension 0
Outputs:
- output 1: bfloat16 [16, 512, 6144], P('dp', 'tp'), parts along dimension 0
- output 2: bfloat16 [16, 512, 6144], P('dp', 'tp'), parts along dimension 0
- output 3: float32 [12288], P('dp'), parts along dimension 0
- output 4: float32 [12288], P('dp'), parts along dimension 0
- output 5: float32 [12288, 6144], P('dp', 'tp'), parts along dimension 0
- output 6: float32 [12288], P(('dp', 'tp')), parts along dimension 0
- output 7: float32 [12288, 256], P('dp'), parts along dimension 0
- output 8: float32 [512], P('dp'), parts along dimension 0
- output 9: float32 [12288, 6144], P(('dp', 'tp')), parts along dimension 0
- output 10: float32 [12288], P('dp'), parts along dimension 0
There are 2 independent parts. The reference program is written for one: setup_inputs(seed, part) draws one part's arguments, and reference() takes and returns one part's arrays. A program takes and returns all parts, laid end to end along the dimension named above; an argument that names none is the same for every part.
All inputs are finite; a program needn't handle non-finite values.
Results may differ from the reference program's by a relative error of at most 0.0160206.
Values are sent between devices in bfloat16 or wider.
A program may use at most 768 MiB of HBM per device.

```python
import jax
import jax.numpy as jnp
from jax import lax

D = 6144
HEADS = 48
HEAD = 128
BATCH = 8
SEQ = 512
LN_EPS = 1e-5


def setup_inputs(seed: int = 0, part: int = 0) -> dict:
    q_width = HEADS * HEAD
    base_key = jax.random.key(seed)
    key_list = jax.random.split(base_key, 8)
    part_keys = jax.random.split(jax.random.fold_in(base_key, part), 2)
    out_gain = (SEQ / 64) ** 0.25
    x_in = jax.random.normal(part_keys[0], (BATCH, SEQ, D), jnp.float32).astype(jnp.bfloat16)
    grad_y = jax.random.normal(part_keys[1], (BATCH, SEQ, D), jnp.float32).astype(jnp.bfloat16)
    ln_gamma = 1.0 + 0.3 * jax.random.normal(key_list[0], (D,), jnp.float32)
    ln_beta = 0.3 * jax.random.normal(key_list[1], (D,), jnp.float32)
    w_q = (D ** -0.5 * jax.random.normal(key_list[2], (D, q_width), jnp.float32)).astype(jnp.bfloat16)
    b_q = 0.5 * jax.random.normal(key_list[3], (q_width,), jnp.float32)
    w_kv = (D ** -0.5 * jax.random.normal(key_list[4], (D, 2 * HEAD), jnp.float32)).astype(jnp.bfloat16)
    b_kv = 0.3 * jax.random.normal(key_list[5], (2 * HEAD,), jnp.float32)
    w_o = (out_gain * q_width ** -0.5 * jax.random.normal(key_list[6], (q_width, D), jnp.float32)).astype(jnp.bfloat16)
    b_o = 0.5 * jax.random.normal(key_list[7], (D,), jnp.float32)
    return {"x_in": x_in, "ln_gamma": ln_gamma, "ln_beta": ln_beta, "w_q": w_q, "b_q": b_q, "w_kv": w_kv, "b_kv": b_kv, "w_o": w_o, "b_o": b_o, "grad_y": grad_y}


def snap_bf16(values_in):
    return values_in.astype(jnp.bfloat16).astype(jnp.float32)


def layer_norm(x_wide, ln_gamma, ln_beta):
    centred = x_wide - jnp.mean(x_wide, axis=-1, keepdims=True)
    row_var = jnp.mean(centred * centred, axis=-1, keepdims=True)
    return centred * lax.rsqrt(row_var + LN_EPS) * ln_gamma + ln_beta


def block_forward(x_wide, ln_gamma, ln_beta, w_q, b_q, w_kv, b_kv, w_o, b_o):
    normed = snap_bf16(layer_norm(x_wide, ln_gamma, ln_beta))
    queries = snap_bf16(jnp.einsum("bsd,de->bse", normed, w_q) + b_q)
    key_val = snap_bf16(jnp.einsum("bsd,dc->bsc", normed, w_kv) + b_kv)
    key_rows = key_val[:, :, :HEAD]
    value_rows = key_val[:, :, HEAD:]
    q_heads = jnp.moveaxis(queries.reshape(BATCH, SEQ, HEADS, HEAD), 2, 0)
    positions = jnp.arange(SEQ)
    causal = positions[:, None] >= positions[None, :]

    def one_head(q_one):
        scores = jnp.einsum("bqc,bkc->bqk", q_one, key_rows) * HEAD ** -0.5
        attn_prob = snap_bf16(jax.nn.softmax(jnp.where(causal, scores, -1e30), axis=-1))
        return snap_bf16(jnp.einsum("bqk,bkc->bqc", attn_prob, value_rows))

    attended = lax.map(jax.checkpoint(one_head), q_heads)
    merged = jnp.moveaxis(attended, 0, 2).reshape(BATCH, SEQ, HEADS * HEAD)
    return x_wide + jnp.einsum("bse,ed->bsd", merged, w_o) + b_o


def reference(x_in, ln_gamma, ln_beta, w_q, b_q, w_kv, b_kv, w_o, b_o, grad_y):
    y_wide, pullback = jax.vjp(block_forward, x_in.astype(jnp.float32), ln_gamma, ln_beta, w_q.astype(jnp.float32), b_q, w_kv.astype(jnp.float32), b_kv, w_o.astype(jnp.float32), b_o)
    cotangents = pullback(grad_y.astype(jnp.float32))
    return (y_wide.astype(jnp.bfloat16), cotangents[0].astype(jnp.bfloat16), cotangents[1], cotangents[2], cotangents[3], cotangents[4], cotangents[5], cotangents[6], cotangents[7], cotangents[8])
```

```python
import jax
import jax.numpy as jnp
from jax import lax
from jax.sharding import PartitionSpec as P

LN_EPS = 1e-5


def norm_forward(x_loc, ln_gamma, ln_beta):
    x_wide = x_loc.astype(jnp.float32)
    centred = x_wide - jnp.mean(x_wide, axis=-1, keepdims=True)
    inv_std = lax.rsqrt(jnp.mean(centred * centred, axis=-1, keepdims=True) + LN_EPS)
    x_hat = centred * inv_std
    return x_hat, inv_std, (x_hat * ln_gamma + ln_beta).astype(jnp.bfloat16)


def norm_backward(grad_h, x_hat, inv_std, ln_gamma):
    grad_hat = grad_h * ln_gamma
    grad_in = inv_std * (grad_hat - jnp.mean(grad_hat, axis=-1, keepdims=True) - x_hat * jnp.mean(grad_hat * x_hat, axis=-1, keepdims=True))
    return grad_in, jnp.sum(grad_h * x_hat, axis=(0, 1)), jnp.sum(grad_h, axis=(0, 1))


def attn_forward(q_heads, key_rows, value_rows, causal):
    scores = jnp.einsum("bqhc,bkc->bhqk", q_heads, key_rows, preferred_element_type=jnp.float32) * q_heads.shape[-1] ** -0.5
    attn_prob = jax.nn.softmax(jnp.where(causal, scores, -1e30), axis=-1)
    prob_lo = attn_prob.astype(jnp.bfloat16)
    attended = jnp.einsum("bhqk,bkc->bqhc", prob_lo, value_rows, preferred_element_type=jnp.float32).astype(jnp.bfloat16)
    return attn_prob, prob_lo, attended


def attn_backward(grad_att, q_heads, key_rows, value_rows, attn_prob, prob_lo):
    grad_prob = jnp.einsum("bqhc,bkc->bhqk", grad_att, value_rows, preferred_element_type=jnp.float32).astype(jnp.bfloat16)
    row_dot = jnp.sum(attn_prob * grad_prob, axis=-1, keepdims=True)
    grad_score = (attn_prob * (grad_prob - row_dot) * q_heads.shape[-1] ** -0.5).astype(jnp.bfloat16)
    grad_q = jnp.einsum("bhqk,bkc->bqhc", grad_score, key_rows, preferred_element_type=jnp.float32).astype(jnp.bfloat16)
    grad_k = jnp.einsum("bhqk,bqhc->bkc", grad_score, q_heads, preferred_element_type=jnp.float32)
    grad_v = jnp.einsum("bhqk,bqhc->bkc", prob_lo, grad_att, preferred_element_type=jnp.float32)
    return grad_q, jnp.concatenate([grad_k, grad_v], axis=-1)


def solution(mesh):
    def device_block(x_loc, ln_gamma, ln_beta, w_q, b_q, w_kv, b_kv, w_o, b_o, dy_loc):
        head_dim = w_kv.shape[1] // 2
        local_heads = w_q.shape[1] // head_dim
        x_hat, inv_std, normed = norm_forward(x_loc, ln_gamma, ln_beta)
        normed_full = lax.all_gather(normed, "tp", axis=1, tiled=True)
        dy_full = lax.all_gather(dy_loc, "tp", axis=1, tiled=True)
        grad_bo_part = jnp.sum(dy_loc, axis=(0, 1), dtype=jnp.float32)

        batch_size = normed_full.shape[0]
        seq_len = normed_full.shape[1]
        queries = (jnp.einsum("bsd,de->bse", normed_full, w_q, preferred_element_type=jnp.float32) + b_q).astype(jnp.bfloat16)
        q_heads = queries.reshape(batch_size, seq_len, local_heads, head_dim)
        key_val = (jnp.einsum("bsd,dc->bsc", normed_full, w_kv, preferred_element_type=jnp.float32) + b_kv).astype(jnp.bfloat16)
        key_rows = key_val[:, :, :head_dim]
        value_rows = key_val[:, :, head_dim:]
        positions = jnp.arange(seq_len)
        causal = positions[:, None] >= positions[None, :]
        attn_prob, prob_lo, attended = attn_forward(q_heads, key_rows, value_rows, causal)
        merged = attended.reshape(queries.shape)
        out_part = jnp.einsum("bse,ed->bsd", merged, w_o, preferred_element_type=jnp.float32).astype(jnp.bfloat16)
        out_part, dy_full = lax.optimization_barrier((out_part, dy_full))
        out_loc = lax.psum_scatter(out_part, "tp", scatter_dimension=1, tiled=True)

        grad_att = jnp.einsum("bsd,ed->bse", dy_full, w_o, preferred_element_type=jnp.float32).astype(jnp.bfloat16)
        grad_q, kv_wide = attn_backward(grad_att.reshape(q_heads.shape), q_heads, key_rows, value_rows, attn_prob, prob_lo)
        grad_q = grad_q.reshape(queries.shape)
        grad_kv = lax.psum(kv_wide.astype(jnp.bfloat16), "tp")
        grad_h_part = jnp.einsum("bse,de->bsd", grad_q, w_q, preferred_element_type=jnp.float32).astype(jnp.bfloat16)
        grad_h_part, grad_q, merged, out_loc = lax.optimization_barrier((grad_h_part, grad_q, merged, out_loc))
        grad_h = lax.psum_scatter(grad_h_part, "tp", scatter_dimension=1, tiled=True).astype(jnp.float32)

        y_loc = (x_loc.astype(jnp.float32) + out_loc.astype(jnp.float32) + b_o).astype(jnp.bfloat16)
        grad_wo = jnp.einsum("bse,bsd->ed", merged, dy_full, preferred_element_type=jnp.float32)
        grad_wq = jnp.einsum("bsd,bse->de", normed_full, grad_q, preferred_element_type=jnp.float32)
        grad_bq = jnp.sum(grad_q, axis=(0, 1), dtype=jnp.float32)
        grad_wkv = jnp.einsum("bsd,bsc->dc", normed_full, grad_kv, preferred_element_type=jnp.float32)
        grad_bkv = jnp.sum(grad_kv, axis=(0, 1), dtype=jnp.float32)
        own_rows = x_loc.shape[1]
        kv_loc = lax.dynamic_slice_in_dim(grad_kv, lax.axis_index("tp") * own_rows, own_rows, axis=1)
        grad_h = grad_h + jnp.einsum("bsc,dc->bsd", kv_loc, w_kv, preferred_element_type=jnp.float32)
        grad_in, gamma_part, beta_part = norm_backward(grad_h, x_hat, inv_std, ln_gamma)
        grad_gamma, grad_beta, grad_bo = lax.psum((gamma_part, beta_part, grad_bo_part), "tp")
        grad_x = (dy_loc.astype(jnp.float32) + grad_in).astype(jnp.bfloat16)
        return (y_loc, grad_x, grad_gamma, grad_beta, grad_wq, grad_bq, grad_wkv, grad_bkv, grad_wo, grad_bo)

    return jax.shard_map(
        device_block,
        mesh=mesh,
        in_specs=(P("dp", "tp", None), P(None), P(None), P(None, "tp"), P("tp"), P(None, None), P(None), P("tp", None), P(None), P("dp", "tp", None)),
        out_specs=(P("dp", "tp", None), P("dp", "tp", None), P("dp"), P("dp"), P("dp", "tp"), P(("dp", "tp")), P("dp", None), P("dp"), P(("dp", "tp"), None), P("dp")),
        check_vma=False,
    )
```

```python
import functools

import jax
import jax.numpy as jnp
from jax import lax
from jax.experimental import pallas as pl
from jax.experimental.pallas import tpu as pltpu
from jax.sharding import PartitionSpec as P

LN_EPS = 1e-5
VMEM_LIMIT = 60 * 1024 * 1024
BF16 = jnp.bfloat16
F32 = jnp.float32

RIGHT, LEFT, PART, FAR_R, FAR_L, PASS_L, PASS_R, PASS_F = range(8)


def norm_backward(grad_h, x_hat, inv_std, ln_gamma):
    grad_hat = grad_h * ln_gamma
    grad_in = inv_std * (grad_hat - jnp.mean(grad_hat, axis=-1, keepdims=True) - x_hat * jnp.mean(grad_hat * x_hat, axis=-1, keepdims=True))
    return grad_in, jnp.sum(grad_h * x_hat, axis=(0, 1)), jnp.sum(grad_h, axis=(0, 1))


def norm_stats(x_wide):
    centred = x_wide - jnp.mean(x_wide, axis=-1, keepdims=True)
    inv_std = lax.rsqrt(jnp.mean(centred * centred, axis=-1, keepdims=True) + LN_EPS)
    return centred * inv_std, inv_std


def block_probs(q_blk, keys, first_row, scale):
    scores = lax.dot_general(q_blk, keys, (((1,), (1,)), ((), ())), preferred_element_type=F32) * scale
    rows = lax.broadcasted_iota(jnp.int32, scores.shape, 0) + first_row
    cols = lax.broadcasted_iota(jnp.int32, scores.shape, 1)
    scores = jnp.where(rows >= cols, scores, -1e30)
    weights = jnp.exp(scores - jnp.max(scores, axis=-1, keepdims=True))
    return weights / jnp.sum(weights, axis=-1, keepdims=True)


def attend(qkv, out, heads, dim):
    rows = qkv.shape[0]
    width = heads * dim

    @pl.loop(0, heads)
    def _(h):
        lanes = pl.ds(pl.multiple_of(h * dim, dim), dim)
        for first in range(0, rows, dim):
            last = first + dim
            probs = block_probs(qkv[first:last, lanes], qkv[:last, width : width + dim], first, dim**-0.5).astype(BF16)
            out[first:last, lanes] = jnp.dot(probs, qkv[:last, width + dim :], preferred_element_type=F32).astype(BF16)


def attend_backward(qkv, grad_att, grad_q, grad_kv, probs_s, scores_s, q_s, att_s, heads, dim):
    rows = qkv.shape[0]
    width = heads * dim
    scale = dim**-0.5
    grad_kv[...] = jnp.zeros_like(grad_kv)
    for first in range(0, rows, dim):
        last = first + dim

        @pl.loop(0, heads)
        def _(h):
            lanes = pl.ds(pl.multiple_of(h * dim, dim), dim)
            stack = pl.ds(pl.multiple_of(h * dim, dim), dim)
            keys = qkv[:last, width : width + dim]
            q_blk = qkv[first:last, lanes]
            a_blk = grad_att[first:last, lanes]
            probs = block_probs(q_blk, keys, first, scale)
            grad_p = lax.dot_general(a_blk, qkv[:last, width + dim :], (((1,), (1,)), ((), ())), preferred_element_type=F32)
            grad_p = grad_p.astype(BF16).astype(F32)
            row_dot = jnp.sum(probs * grad_p, axis=-1, keepdims=True)
            grad_s = (probs * (grad_p - row_dot) * scale).astype(BF16)
            grad_q[first:last, lanes] = jnp.dot(grad_s, keys, preferred_element_type=F32).astype(BF16)
            probs_s[stack, :last] = probs.astype(BF16)
            scores_s[stack, :last] = grad_s
            q_s[stack, :] = q_blk
            att_s[stack, :] = a_blk

        over_rows = (((0,), (0,)), ((), ()))
        grad_kv[:last, :dim] += lax.dot_general(scores_s[:, :last], q_s[...], over_rows, preferred_element_type=F32)
        grad_kv[:last, dim:] += lax.dot_general(probs_s[:, :last], att_s[...], over_rows, preferred_element_type=F32)


def gather_kernel(heads, dim, x_hbm, dy_hbm, gamma, beta, wq_hbm, wkv_hbm, bias, h_full, dy_full, qkv_out, att_out,
                  own, x_buf, w_buf, h_buf, qkv_buf, att_buf, send, recv, x_sem, dy_sem, keep_sem, w_sem, h_sem, out_sem):
    batch, rows, width = x_hbm.shape
    half = rows // 2
    units = 2 * batch
    ring = h_full.shape[1] // rows
    qkv_width = qkv_buf.shape[1]
    me = lax.axis_index("tp")
    partner = me + 1 - 2 * lax.rem(me, 2)
    right, left, far = lax.rem(me + 2, ring), lax.rem(me + ring - 2, ring), lax.rem(me + ring // 2, ring)

    barrier = pltpu.get_barrier_semaphore()
    for other in (left, right, partner):
        pl.semaphore_signal(barrier, inc=1, device_id={"tp": other}, device_id_type=pl.DeviceIdType.MESH)
    pl.semaphore_wait(barrier, 3)

    def block(full, b, owner, first=0, count=rows):
        return full.at[b, pl.ds(pl.multiple_of(owner * rows + first, half), count)]

    def remote(src, dst, kind, u, to):
        return pltpu.make_async_remote_copy(
            src_ref=src, dst_ref=dst, send_sem=send.at[kind, u], recv_sem=recv.at[kind, u],
            device_id={"tp": to}, device_id_type=pl.DeviceIdType.MESH)

    def move(kind, full, b, u):
        if kind in (RIGHT, LEFT, PART):
            src, dst = own.at[u], block(full, b, me)
        elif kind in (FAR_R, FAR_L):
            src = dst = block(full, b, left, 0, half) if kind == FAR_R else block(full, b, right, half, half)
        else:
            src = dst = block(full, b, {PASS_L: left, PASS_R: right, PASS_F: far}[kind])
        to = {RIGHT: right, FAR_R: right, LEFT: left, FAR_L: left}.get(kind, partner)
        return remote(src, dst, kind, u, to)

    def keep(full, b, u):
        return pltpu.make_async_copy(own.at[u], block(full, b, me), keep_sem.at[u])

    def load_x(b):
        return pltpu.make_async_copy(x_hbm.at[b], x_buf.at[lax.rem(b, 2)], x_sem.at[lax.rem(b, 2)])

    def load_dy(b):
        return pltpu.make_async_copy(dy_hbm.at[b], own.at[batch + b], dy_sem.at[b])

    def unit(u, low, high, act):
        @pl.when(jnp.logical_and(u >= low, u < jnp.minimum(high, batch)))
        def _():
            act(h_full, u, u)

        @pl.when(jnp.logical_and(u >= jnp.maximum(low, batch), u < high))
        def _():
            act(dy_full, u - batch, u)

    def normalise(b):
        load_x(b).wait()
        slot = lax.rem(b, 2)

        @pl.loop(0, rows, step=16)
        def _(r):
            at = pl.ds(pl.multiple_of(r, 16), 16)
            x_hat, _ = norm_stats(x_buf[slot, at, :].astype(F32))
            own[b, at, :] = (x_hat * gamma[...] + beta[...]).astype(BF16)

        @pl.when(b + 2 < batch)
        def _():
            load_x(b + 2).start()

    def launch(u):
        @pl.when(u < batch)
        def _():
            normalise(u)

        @pl.when(jnp.logical_and(u >= batch, u < units))
        def _():
            load_dy(u - batch).wait()

        def act(full, b, u):
            for kind in (RIGHT, LEFT, PART):
                move(kind, full, b, u).start()
            keep(full, b, u).start()

        unit(u, 0, units, act)

    load_x(0).start()
    load_x(1).start()
    weights = (pltpu.make_async_copy(wq_hbm, w_buf.at[:, pl.ds(0, heads * dim)], w_sem.at[0]),
               pltpu.make_async_copy(wkv_hbm, w_buf.at[:, pl.ds(heads * dim, 2 * dim)], w_sem.at[1]))
    launch(0)
    launch(1)
    for copy in weights:
        copy.start()
    for b in range(batch):
        load_dy(b).start()
    for copy in weights:
        copy.wait()

    def project(b):
        load = pltpu.make_async_copy(h_full.at[b], h_buf, h_sem.at[0])
        load.start()
        load.wait()

        @pl.loop(0, qkv_width, step=256)
        def _(n):
            at = pl.ds(pl.multiple_of(n, 256), 256)
            qkv_buf[:, at] = (jnp.dot(h_buf[...], w_buf[:, at], preferred_element_type=F32) + bias[:, at]).astype(BF16)

    def results(b):
        return (pltpu.make_async_copy(qkv_buf, qkv_out.at[b], out_sem.at[0]),
                pltpu.make_async_copy(att_buf, att_out.at[b], out_sem.at[1]))

    @pl.loop(0, units + 2)
    def _(s):
        def forward(full, b, u):
            move(RIGHT, full, b, u).wait_recv()
            move(FAR_R, full, b, u).start()
            move(LEFT, full, b, u).wait_recv()
            move(FAR_L, full, b, u).start()

        unit(s, 0, units, forward)
        launch(s + 2)

        def share(full, b, u):
            move(PASS_L, full, b, u).start()
            move(PASS_R, full, b, u).start()

        unit(s, 0, units, share)

        def share_far(full, b, u):
            move(FAR_R, full, b, u).wait_recv()
            move(FAR_L, full, b, u).wait_recv()
            move(PASS_F, full, b, u).start()

        unit(s - 1, 0, units, share_far)

        def complete(full, b, u):
            for kind in (PART, PASS_L, PASS_R, PASS_F):
                move(kind, full, b, u).wait_recv()
            keep(full, b, u).wait()

        unit(s - 2, 0, units, complete)

        @pl.when(jnp.logical_and(s >= 2, s < batch + 2))
        def _():
            b = s - 2

            @pl.when(b > 0)
            def _():
                for copy in results(b - 1):
                    copy.wait()

            project(b)
            attend(qkv_buf, att_buf, heads, dim)
            for copy in results(b):
                copy.start()

    for copy in results(batch - 1):
        copy.wait()

    @pl.loop(0, units)
    def _(u):
        def act(full, b, u):
            for kind in range(8):
                move(kind, full, b, u).wait_send()

        unit(u, 0, units, act)


def gather_and_attend(x_loc, dy_loc, gamma, beta, w_q, w_kv, bias, ring, dim):
    batch, rows, width = x_loc.shape
    q_width = w_q.shape[1]
    qkv_width = q_width + w_kv.shape[1]
    seq = rows * ring
    units = 2 * batch
    hbm = pl.BlockSpec(memory_space=pl.ANY)
    vmem = pl.BlockSpec(memory_space=pltpu.VMEM)
    dma = pltpu.SemaphoreType.DMA
    return pl.pallas_call(
        functools.partial(gather_kernel, q_width // dim, dim),
        name="gather_and_attend",
        out_shape=(
            jax.ShapeDtypeStruct((batch, seq, width), BF16), jax.ShapeDtypeStruct((batch, seq, width), BF16),
            jax.ShapeDtypeStruct((batch, seq, qkv_width), BF16), jax.ShapeDtypeStruct((batch, seq, q_width), BF16)),
        in_specs=[hbm, hbm, vmem, vmem, hbm, hbm, vmem],
        out_specs=(hbm, hbm, hbm, hbm),
        scratch_shapes=[
            pltpu.VMEM((units, rows, width), BF16), pltpu.VMEM((2, rows, width), BF16), pltpu.VMEM((width, qkv_width), BF16),
            pltpu.VMEM((seq, width), BF16), pltpu.VMEM((seq, qkv_width), BF16), pltpu.VMEM((seq, q_width), BF16),
            dma((8, units)), dma((8, units)), dma((2,)), dma((batch,)), dma((units,)), dma((2,)), dma((1,)), dma((2,))],
        compiler_params=pltpu.CompilerParams(collective_id=0, has_side_effects=True, vmem_limit_bytes=VMEM_LIMIT),
        cost_estimate=pl.CostEstimate(flops=2 * batch * seq * width * qkv_width, bytes_accessed=6 * batch * seq * width, transcendentals=0),
    )(x_loc, dy_loc, gamma, beta, w_q, w_kv, bias)


def attend_backward_kernel(heads, dim, qkv, grad_att, grad_q, grad_kv, total, probs_s, scores_s, q_s, att_s):
    attend_backward(qkv.at[0], grad_att.at[0], grad_q.at[0], total, probs_s, scores_s, q_s, att_s, heads, dim)
    grad_kv[0] = total[...].astype(BF16)


def attention_gradients(qkv, grad_att, dim):
    batch, seq, qkv_width = qkv.shape
    q_width = grad_att.shape[2]
    heads = q_width // dim
    one = lambda w: pl.BlockSpec((1, seq, w), lambda b: (b, 0, 0))
    return pl.pallas_call(
        functools.partial(attend_backward_kernel, heads, dim),
        name="attention_gradients",
        grid=(batch,),
        out_shape=(jax.ShapeDtypeStruct((batch, seq, q_width), BF16), jax.ShapeDtypeStruct((batch, seq, 2 * dim), BF16)),
        in_specs=[one(qkv_width), one(q_width)],
        out_specs=(one(q_width), one(2 * dim)),
        scratch_shapes=[
            pltpu.VMEM((seq, 2 * dim), F32), pltpu.VMEM((q_width, seq), BF16), pltpu.VMEM((q_width, seq), BF16),
            pltpu.VMEM((q_width, dim), BF16), pltpu.VMEM((q_width, dim), BF16)],
        compiler_params=pltpu.CompilerParams(vmem_limit_bytes=VMEM_LIMIT // 2),
        cost_estimate=pl.CostEstimate(flops=batch * heads * seq * seq * dim * 12, bytes_accessed=batch * seq * qkv_width * 8, transcendentals=0),
    )(qkv, grad_att)


def solution(mesh):
    ring = mesh.shape["tp"]

    def device_block(x_loc, ln_gamma, ln_beta, w_q, b_q, w_kv, b_kv, w_o, b_o, dy_loc):
        head_dim = w_kv.shape[1] // 2
        bias = jnp.concatenate([b_q, b_kv])[None, :]
        normed_full, dy_full, qkv, merged = gather_and_attend(x_loc, dy_loc, ln_gamma[None, :], ln_beta[None, :], w_q, w_kv, bias, ring, head_dim)
        out_part = jnp.einsum("bse,ed->bsd", merged, w_o, preferred_element_type=jnp.float32).astype(jnp.bfloat16)
        out_part, dy_full = lax.optimization_barrier((out_part, dy_full))
        out_loc = lax.psum_scatter(out_part, "tp", scatter_dimension=1, tiled=True)

        grad_att = jnp.einsum("bsd,ed->bse", dy_full, w_o, preferred_element_type=jnp.float32).astype(jnp.bfloat16)
        grad_q, grad_kv = attention_gradients(qkv, grad_att, head_dim)
        grad_kv = lax.psum(grad_kv, "tp")
        grad_h_part = jnp.einsum("bse,de->bsd", grad_q, w_q, preferred_element_type=jnp.float32).astype(jnp.bfloat16)
        grad_h_part, grad_q, merged, out_loc = lax.optimization_barrier((grad_h_part, grad_q, merged, out_loc))
        grad_h = lax.psum_scatter(grad_h_part, "tp", scatter_dimension=1, tiled=True).astype(jnp.float32)

        grad_bo_part = jnp.sum(dy_loc, axis=(0, 1), dtype=jnp.float32)
        y_loc = (x_loc.astype(jnp.float32) + out_loc.astype(jnp.float32) + b_o).astype(jnp.bfloat16)
        grad_wo = jnp.einsum("bse,bsd->ed", merged, dy_full, preferred_element_type=jnp.float32)
        grad_wq = jnp.einsum("bsd,bse->de", normed_full, grad_q, preferred_element_type=jnp.float32)
        grad_bq = jnp.sum(grad_q, axis=(0, 1), dtype=jnp.float32)
        grad_wkv = jnp.einsum("bsd,bsc->dc", normed_full, grad_kv, preferred_element_type=jnp.float32)
        grad_bkv = jnp.sum(grad_kv, axis=(0, 1), dtype=jnp.float32)
        own_rows = x_loc.shape[1]
        kv_loc = lax.dynamic_slice_in_dim(grad_kv, lax.axis_index("tp") * own_rows, own_rows, axis=1)
        grad_h = grad_h + jnp.einsum("bsc,dc->bsd", kv_loc, w_kv, preferred_element_type=jnp.float32)
        x_hat, inv_std = norm_stats(x_loc.astype(jnp.float32))
        grad_in, gamma_part, beta_part = norm_backward(grad_h, x_hat, inv_std, ln_gamma)
        grad_gamma, grad_beta, grad_bo = lax.psum((gamma_part, beta_part, grad_bo_part), "tp")
        grad_x = (dy_loc.astype(jnp.float32) + grad_in).astype(jnp.bfloat16)
        return (y_loc, grad_x, grad_gamma, grad_beta, grad_wq, grad_bq, grad_wkv, grad_bkv, grad_wo, grad_bo)

    return jax.shard_map(
        device_block,
        mesh=mesh,
        in_specs=(P("dp", "tp", None), P(None), P(None), P(None, "tp"), P("tp"), P(None, None), P(None), P("tp", None), P(None), P("dp", "tp", None)),
        out_specs=(P("dp", "tp", None), P("dp", "tp", None), P("dp"), P("dp"), P("dp", "tp"), P(("dp", "tp")), P("dp", None), P("dp"), P(("dp", "tp"), None), P("dp")),
        check_vma=False,
    )
```

```python
import functools

import jax
import jax.numpy as jnp
from jax import lax
from jax.experimental import pallas as pl
from jax.experimental.pallas import tpu as pltpu
from jax.sharding import PartitionSpec as P

LN_EPS = 1e-5
VMEM_LIMIT = 60 * 1024 * 1024
BF16 = jnp.bfloat16
F32 = jnp.float32

RIGHT, LEFT, PART, FAR_R, FAR_L, PASS_L, PASS_R, PASS_F = range(8)


def norm_stats(x_wide):
    centred = x_wide - jnp.mean(x_wide, axis=-1, keepdims=True)
    inv_std = lax.rsqrt(jnp.mean(centred * centred, axis=-1, keepdims=True) + LN_EPS)
    return centred * inv_std, inv_std


def causal_softmax(scores, first_row):
    rows = lax.broadcasted_iota(jnp.int32, scores.shape, 0) + first_row
    cols = lax.broadcasted_iota(jnp.int32, scores.shape, 1)
    scores = jnp.where(rows >= cols, scores, -1e30)
    weights = jnp.exp(scores - jnp.max(scores, axis=-1, keepdims=True))
    return weights / jnp.sum(weights, axis=-1, keepdims=True)


def attend(qkv, out, heads, dim):
    rows = qkv.shape[0]
    width = heads * dim

    @pl.loop(0, heads)
    def _(h):
        lanes = pl.ds(pl.multiple_of(h * dim, dim), dim)
        for first in range(0, rows, dim):
            last = first + dim
            scores = lax.dot_general(qkv[first:last, lanes], qkv[:last, width : width + dim], (((1,), (1,)), ((), ())), preferred_element_type=F32)
            probs = causal_softmax(scores * dim**-0.5, first).astype(BF16)
            out[first:last, lanes] = jnp.dot(probs, qkv[:last, width + dim :], preferred_element_type=F32).astype(BF16)


def attend_backward(qkv, grad_att, grad_q, grad_kv, scores_s, grad_p_s, probs_s, grad_s_s, q_s, att_s, heads, dim):
    rows = qkv.shape[0]
    width = heads * dim
    scale = dim**-0.5
    across = (((1,), (1,)), ((), ()))
    over_rows = (((0,), (0,)), ((), ()))
    chunk = dim // 2
    grad_kv[...] = jnp.zeros_like(grad_kv)
    for first in range(0, rows, dim):
        last = first + dim
        for h in range(heads):
            q_s[h * dim : (h + 1) * dim, :] = qkv[first:last, h * dim : (h + 1) * dim]
            att_s[h * dim : (h + 1) * dim, :] = grad_att[first:last, h * dim : (h + 1) * dim]
        keys = qkv[:last, width : width + dim]
        scores_s[:, :last] = lax.dot_general(q_s[...], keys, across, preferred_element_type=F32)
        grad_p_s[:, :last] = lax.dot_general(att_s[...], qkv[:last, width + dim :], across, preferred_element_type=F32)

        @pl.loop(0, width, step=chunk)
        def _(r):
            at = pl.ds(pl.multiple_of(r, chunk), chunk)
            row = first + lax.rem(r, dim)
            probs = causal_softmax(scores_s[at, :last] * scale, row)
            grad_p = grad_p_s[at, :last].astype(BF16).astype(F32)
            row_dot = jnp.sum(probs * grad_p, axis=-1, keepdims=True)
            grad_s_s[at, :last] = (probs * (grad_p - row_dot) * scale).astype(BF16)
            probs_s[at, :last] = probs.astype(BF16)

        stacked = jnp.dot(grad_s_s[:, :last], keys, preferred_element_type=F32).astype(BF16)
        for h in range(heads):
            grad_q[first:last, h * dim : (h + 1) * dim] = stacked[h * dim : (h + 1) * dim, :]
        grad_kv[:last, :dim] += lax.dot_general(grad_s_s[:, :last], q_s[...], over_rows, preferred_element_type=F32)
        grad_kv[:last, dim:] += lax.dot_general(probs_s[:, :last], att_s[...], over_rows, preferred_element_type=F32)


def gather_kernel(heads, dim, x_hbm, dy_hbm, gamma, beta, wq_hbm, wkv_hbm, bias, wo_hbm,
                  h_full, dy_full, qkv_out, att_out, dq_out, dkv_out, dbo,
                  own, x_buf, w_buf, wo_buf, h_buf, qkv_buf, att_buf, dq_buf, dkv_buf, total, scores_s, grad_p_s, probs_s, grad_s_s, q_s, att_s,
                  send, recv, x_sem, dy_sem, keep_sem, w_sem, h_sem, out_sem, back_sem):
    batch, rows, width = x_hbm.shape
    half = rows // 2
    units = 2 * batch
    ring = h_full.shape[1] // rows
    qkv_width = qkv_buf.shape[1]
    me = lax.axis_index("tp")
    partner = me + 1 - 2 * lax.rem(me, 2)
    right, left, far = lax.rem(me + 2, ring), lax.rem(me + ring - 2, ring), lax.rem(me + ring // 2, ring)

    barrier = pltpu.get_barrier_semaphore()
    for other in (left, right, partner):
        pl.semaphore_signal(barrier, inc=1, device_id={"tp": other}, device_id_type=pl.DeviceIdType.MESH)
    pl.semaphore_wait(barrier, 3)

    def block(full, b, owner, first=0, count=rows):
        return full.at[b, pl.ds(pl.multiple_of(owner * rows + first, half), count)]

    def remote(src, dst, kind, u, to):
        return pltpu.make_async_remote_copy(
            src_ref=src, dst_ref=dst, send_sem=send.at[kind, u], recv_sem=recv.at[kind, u],
            device_id={"tp": to}, device_id_type=pl.DeviceIdType.MESH)

    def move(kind, full, b, u):
        if kind in (RIGHT, LEFT, PART):
            src, dst = own.at[u], block(full, b, me)
        elif kind in (FAR_R, FAR_L):
            src = dst = block(full, b, left, 0, half) if kind == FAR_R else block(full, b, right, half, half)
        else:
            src = dst = block(full, b, {PASS_L: left, PASS_R: right, PASS_F: far}[kind])
        to = {RIGHT: right, FAR_R: right, LEFT: left, FAR_L: left}.get(kind, partner)
        return remote(src, dst, kind, u, to)

    def keep(full, b, u):
        return pltpu.make_async_copy(own.at[u], block(full, b, me), keep_sem.at[u])

    def load_x(b):
        return pltpu.make_async_copy(x_hbm.at[b], x_buf.at[lax.rem(b, 2)], x_sem.at[lax.rem(b, 2)])

    def load_dy(b):
        return pltpu.make_async_copy(dy_hbm.at[b], own.at[batch + b], dy_sem.at[b])

    def unit(u, low, high, act):
        @pl.when(jnp.logical_and(u >= low, u < jnp.minimum(high, batch)))
        def _():
            act(h_full, u, u)

        @pl.when(jnp.logical_and(u >= jnp.maximum(low, batch), u < high))
        def _():
            act(dy_full, u - batch, u)

    def normalise(b):
        load_x(b).wait()
        slot = lax.rem(b, 2)

        @pl.loop(0, rows, step=16)
        def _(r):
            at = pl.ds(pl.multiple_of(r, 16), 16)
            x_hat, _ = norm_stats(x_buf[slot, at, :].astype(F32))
            own[b, at, :] = (x_hat * gamma[...] + beta[...]).astype(BF16)

        @pl.when(b + 2 < batch)
        def _():
            load_x(b + 2).start()

    def launch(u):
        @pl.when(u < batch)
        def _():
            normalise(u)

        @pl.when(jnp.logical_and(u >= batch, u < units))
        def _():
            load_dy(u - batch).wait()

        def act(full, b, u):
            for kind in (RIGHT, LEFT, PART):
                move(kind, full, b, u).start()
            keep(full, b, u).start()

        unit(u, 0, units, act)

    load_x(0).start()
    load_x(1).start()
    weights = (pltpu.make_async_copy(wq_hbm, w_buf.at[:, pl.ds(0, heads * dim)], w_sem.at[0]),
               pltpu.make_async_copy(wkv_hbm, w_buf.at[:, pl.ds(heads * dim, 2 * dim)], w_sem.at[1]),
               pltpu.make_async_copy(wo_hbm, wo_buf, w_sem.at[2]))
    dbo[...] = jnp.zeros_like(dbo)
    launch(0)
    launch(1)
    for copy in weights:
        copy.start()
    for b in range(batch):
        load_dy(b).start()
    for copy in weights:
        copy.wait()

    def project(b):
        load = pltpu.make_async_copy(h_full.at[b], h_buf, h_sem.at[0])
        load.start()
        load.wait()

        @pl.loop(0, qkv_width, step=256)
        def _(n):
            at = pl.ds(pl.multiple_of(n, 256), 256)
            qkv_buf[:, at] = (jnp.dot(h_buf[...], w_buf[:, at], preferred_element_type=F32) + bias[:, at]).astype(BF16)

    def results(b):
        return (pltpu.make_async_copy(qkv_buf, qkv_out.at[b], out_sem.at[0]),
                pltpu.make_async_copy(att_buf, att_out.at[b], out_sem.at[1]))

    def back_results(b):
        return (pltpu.make_async_copy(dq_buf, dq_out.at[b], back_sem.at[0]),
                pltpu.make_async_copy(dkv_buf, dkv_out.at[b], back_sem.at[1]))

    def differentiate(b):
        load = pltpu.make_async_copy(dy_full.at[b], h_buf, h_sem.at[0])
        again = pltpu.make_async_copy(qkv_out.at[b], qkv_buf, h_sem.at[1])
        load.start()
        again.start()
        load.wait()

        @pl.loop(0, heads * dim, step=256)
        def _(n):
            at = pl.ds(pl.multiple_of(n, 256), 256)
            att_buf[:, at] = lax.dot_general(h_buf[...], wo_buf[at, :], (((1,), (1,)), ((), ())), preferred_element_type=F32).astype(BF16)

        @pl.loop(0, width, step=512)
        def _(n):
            at = pl.ds(pl.multiple_of(n, 512), 512)
            dbo[:, at] += jnp.sum(h_buf[:, at].astype(F32).reshape(-1, 8, 512), axis=0)

        again.wait()
        attend_backward(qkv_buf, att_buf, dq_buf, total, scores_s, grad_p_s, probs_s, grad_s_s, q_s, att_s, heads, dim)
        dkv_buf[...] = total[...].astype(BF16)

    @pl.loop(0, units + 2)
    def _(s):
        def forward(full, b, u):
            move(RIGHT, full, b, u).wait_recv()
            move(FAR_R, full, b, u).start()
            move(LEFT, full, b, u).wait_recv()
            move(FAR_L, full, b, u).start()

        unit(s, 0, units, forward)
        launch(s + 2)

        def share(full, b, u):
            move(PASS_L, full, b, u).start()
            move(PASS_R, full, b, u).start()

        unit(s, 0, units, share)

        def share_far(full, b, u):
            move(FAR_R, full, b, u).wait_recv()
            move(FAR_L, full, b, u).wait_recv()
            move(PASS_F, full, b, u).start()

        unit(s - 1, 0, units, share_far)

        def complete(full, b, u):
            for kind in (PART, PASS_L, PASS_R, PASS_F):
                move(kind, full, b, u).wait_recv()
            keep(full, b, u).wait()

        unit(s - 2, 0, units, complete)

        @pl.when(jnp.logical_and(s >= 2, s < batch + 2))
        def _():
            b = s - 2

            @pl.when(b > 0)
            def _():
                for copy in results(b - 1):
                    copy.wait()

            project(b)
            attend(qkv_buf, att_buf, heads, dim)
            for copy in results(b):
                copy.start()

        @pl.when(s >= batch + 2)
        def _():
            b = s - 2 - batch

            @pl.when(b == 0)
            def _():
                for copy in results(batch - 1):
                    copy.wait()

            @pl.when(b > 0)
            def _():
                for copy in back_results(b - 1):
                    copy.wait()

            differentiate(b)
            for copy in back_results(b):
                copy.start()

    for copy in back_results(batch - 1):
        copy.wait()

    @pl.loop(0, units)
    def _(u):
        def act(full, b, u):
            for kind in range(8):
                move(kind, full, b, u).wait_send()

        unit(u, 0, units, act)


def gather_and_attend(x_loc, dy_loc, gamma, beta, w_q, w_kv, bias, w_o, ring, dim):
    batch, rows, width = x_loc.shape
    q_width = w_q.shape[1]
    qkv_width = q_width + w_kv.shape[1]
    seq = rows * ring
    units = 2 * batch
    hbm = pl.BlockSpec(memory_space=pl.ANY)
    vmem = pl.BlockSpec(memory_space=pltpu.VMEM)
    dma = pltpu.SemaphoreType.DMA
    whole = lambda w: jax.ShapeDtypeStruct((batch, seq, w), BF16)
    return pl.pallas_call(
        functools.partial(gather_kernel, q_width // dim, dim),
        name="gather_and_attend",
        out_shape=(whole(width), whole(width), whole(qkv_width), whole(q_width), whole(q_width), whole(2 * dim), jax.ShapeDtypeStruct((8, width), F32)),
        in_specs=[hbm, hbm, vmem, vmem, hbm, hbm, vmem, hbm],
        out_specs=(hbm, hbm, hbm, hbm, hbm, hbm, vmem),
        scratch_shapes=[
            pltpu.VMEM((units, rows, width), BF16), pltpu.VMEM((2, rows, width), BF16), pltpu.VMEM((width, qkv_width), BF16),
            pltpu.VMEM((q_width, width), BF16), pltpu.VMEM((seq, width), BF16), pltpu.VMEM((seq, qkv_width), BF16), pltpu.VMEM((seq, q_width), BF16),
            pltpu.VMEM((seq, q_width), BF16), pltpu.VMEM((seq, 2 * dim), BF16), pltpu.VMEM((seq, 2 * dim), F32),
            pltpu.VMEM((q_width, seq), F32), pltpu.VMEM((q_width, seq), F32), pltpu.VMEM((q_width, seq), BF16), pltpu.VMEM((q_width, seq), BF16),
            pltpu.VMEM((q_width, dim), BF16), pltpu.VMEM((q_width, dim), BF16),
            dma((8, units)), dma((8, units)), dma((2,)), dma((batch,)), dma((units,)), dma((3,)), dma((2,)), dma((2,)), dma((2,))],
        compiler_params=pltpu.CompilerParams(collective_id=0, has_side_effects=True, vmem_limit_bytes=VMEM_LIMIT),
        cost_estimate=pl.CostEstimate(flops=4 * batch * seq * width * qkv_width, bytes_accessed=6 * batch * seq * width, transcendentals=0),
    )(x_loc, dy_loc, gamma, beta, w_q, w_kv, bias, w_o)


def scatter_kernel(att_hbm, dq_hbm, wo_hbm, wq_hbm, x_hbm, b_o, y_out, dh_out,
                   att_buf, dq_buf, wo_buf, wq_buf, stage, dh_buf, theirs, far_sum, near_sum, own_sum, far_in, near_in, x_buf, y_buf,
                   pair_send, pair_recv, far_send, far_recv, near_send, near_recv, free, load_sem, w_sem, dh_sem):
    batch, rows, width = x_hbm.shape
    ring = stage.shape[0] // rows
    half = width // 2
    tile = 512
    me = lax.axis_index("tp")
    partner = me + 1 - 2 * lax.rem(me, 2)
    right, left = lax.rem(me + 2, ring), lax.rem(me + ring - 2, ring)
    chips = ring // 2

    barrier = pltpu.get_barrier_semaphore()
    for other in (left, right, partner):
        pl.semaphore_signal(barrier, inc=1, device_id={"tp": other}, device_id_type=pl.DeviceIdType.MESH)
    pl.semaphore_wait(barrier, 3)

    def load(src, dst, n):
        return pltpu.make_async_copy(src, dst, load_sem.at[n])

    load_att = lambda b: load(att_hbm.at[b], att_buf, 0)
    load_dq = lambda b: load(dq_hbm.at[b], dq_buf, 1)
    load_x = lambda b: load(x_hbm.at[b], x_buf, 2)
    store_y = lambda b: load(y_buf, y_out.at[b], 3)
    load_wo = pltpu.make_async_copy(wo_hbm, wo_buf, w_sem.at[0])
    load_wq = pltpu.make_async_copy(wq_hbm, wq_buf, w_sem.at[1])

    def remote(src, dst, sems, to):
        return pltpu.make_async_remote_copy(
            src_ref=src, dst_ref=dst, send_sem=sems[0], recv_sem=sems[1], device_id={"tp": to}, device_id_type=pl.DeviceIdType.MESH)

    def block(owner):
        return pl.ds(pl.multiple_of(owner * rows, rows), rows)

    def pair(r):
        return remote(stage.at[block(lax.rem(partner + 2 * r, ring))], theirs.at[r], (pair_send.at[r], pair_recv.at[r]), partner)

    def far(u, way):
        cols = pl.ds(way * half, half)
        return remote(far_sum.at[lax.rem(u, 2), :, cols], far_in.at[lax.rem(u, 3), :, cols],
                      (far_send.at[lax.rem(u, 2), way], far_recv.at[lax.rem(u, 3), way]), (right, left)[way])

    def near(u, way):
        slot = lax.rem(u, 3)
        return remote(near_sum.at[slot, way], near_in.at[slot, way], (near_send.at[slot, way], near_recv.at[slot, way]), (right, left)[way])

    def columns(low, high, act):
        @pl.loop(low, high, step=tile)
        def _(n):
            act(pl.ds(pl.multiple_of(n, tile), tile))

    def part(u):
        load_att(u).wait()

        @pl.when(u > 0)
        def _():
            for r in range(chips):
                pair(r).wait_send()

        def act(at):
            stage[:, at] = jnp.dot(att_buf[...], wo_buf[:, at], preferred_element_type=F32).astype(BF16)

        columns(0, width, act)

        @pl.when(u + 1 < batch)
        def _():
            load_att(u + 1).start()

        @pl.when(u > 0)
        def _():
            pl.semaphore_wait(free, 1)

        for r in range(chips):
            pair(r).start()

    def combine(u):
        slot2, slot3 = lax.rem(u, 2), lax.rem(u, 3)
        for r in range(chips):
            pair(r).wait_recv()

        @pl.when(u >= 2)
        def _():
            for way in range(2):
                far(u - 2, way).wait_send()

        @pl.when(u >= 3)
        def _():
            for way in range(2):
                near(u - 3, way).wait_send()

        def chip_sum(r, at):
            return stage[block(lax.rem(me + 2 * r, ring)), at].astype(F32) + theirs[r, :, at].astype(F32)

        def act_far(at):
            far_sum[slot2, :, at] = chip_sum(chips // 2, at).astype(BF16)

        columns(0, width, act_far)
        for way in range(2):
            far(u, way).start()

        def act(at):
            near_sum[slot3, 0, :, at] = chip_sum(1, at).astype(BF16)
            near_sum[slot3, 1, :, at] = chip_sum(chips - 1, at).astype(BF16)
            own_sum[slot3, :, at] = chip_sum(0, at)

        columns(0, width, act)

        @pl.when(u + 1 < batch)
        def _():
            pl.semaphore_signal(free, inc=1, device_id={"tp": partner}, device_id_type=pl.DeviceIdType.MESH)

    def relay(u):
        slot = lax.rem(u, 3)
        for way in range(2):
            far(u, way).wait_recv()
        for way in range(2):
            def act(at):
                near_sum[slot, way, :, at] = (near_sum[slot, way, :, at].astype(F32) + far_in[slot, :, at].astype(F32)).astype(BF16)

            columns(way * half, way * half + half, act)
        for way in range(2):
            near(u, way).start()

    def finish(u):
        slot = lax.rem(u, 3)
        for way in range(2):
            near(u, way).wait_recv()
        load_x(u).wait()

        @pl.when(u > 0)
        def _():
            store_y(u - 1).wait()

        def act(at):
            total = own_sum[slot, :, at] + near_in[slot, 0, :, at].astype(F32) + near_in[slot, 1, :, at].astype(F32)
            y_buf[:, at] = (x_buf[:, at].astype(F32) + total + b_o[:, at]).astype(BF16)

        columns(0, width, act)
        store_y(u).start()

        @pl.when(u + 1 < batch)
        def _():
            load_x(u + 1).start()

    def store_dh(b, n):
        at = pl.ds(pl.multiple_of(n, tile), tile)
        slot = lax.rem(lax.div(n, tile), 2)
        return pltpu.make_async_copy(dh_buf.at[slot], dh_out.at[b, :, at], dh_sem.at[slot])

    def grad_part(b):
        load_dq(b).wait()

        @pl.loop(0, width, step=tile)
        def _(n):
            @pl.when(n >= 2 * tile)
            def _():
                store_dh(b, n - 2 * tile).wait()

            at = pl.ds(pl.multiple_of(n, tile), tile)
            dh_buf[lax.rem(lax.div(n, tile), 2)] = lax.dot_general(
                dq_buf[...], wq_buf[at, :], (((1,), (1,)), ((), ())), preferred_element_type=F32).astype(BF16)
            store_dh(b, n).start()

        @pl.when(b + 1 < batch)
        def _():
            load_dq(b + 1).start()

        for n in (width - 2 * tile, width - tile):
            store_dh(b, n).wait()

    load_att(0).start()
    load_wo.start()
    load_wq.start()
    load_dq(0).start()
    load_x(0).start()
    load_wo.wait()

    @pl.loop(0, batch + 3)
    def _(t):
        @pl.when(jnp.logical_and(t >= 1, t < batch + 1))
        def _():
            combine(t - 1)

        @pl.when(jnp.logical_and(t >= 2, t < batch + 2))
        def _():
            relay(t - 2)

        @pl.when(t >= 3)
        def _():
            finish(t - 3)

        @pl.when(t < batch)
        def _():
            part(t)

        @pl.when(t == 2)
        def _():
            load_wq.wait()

        @pl.when(jnp.logical_and(t >= 2, t < batch + 2))
        def _():
            grad_part(t - 2)

    for r in range(chips):
        pair(r).wait_send()
    for way in range(2):
        for u in (batch - 2, batch - 1):
            far(u, way).wait_send()
        for u in (batch - 3, batch - 2, batch - 1):
            near(u, way).wait_send()
    store_y(batch - 1).wait()


def project_and_scatter(merged, grad_q, w_o, w_q, x_loc, b_o, ring):
    batch, rows, width = x_loc.shape
    seq, q_width = merged.shape[1:]
    hbm = pl.BlockSpec(memory_space=pl.ANY)
    vmem = pl.BlockSpec(memory_space=pltpu.VMEM)
    dma = pltpu.SemaphoreType.DMA
    return pl.pallas_call(
        scatter_kernel,
        name="project_and_scatter",
        out_shape=(jax.ShapeDtypeStruct(x_loc.shape, BF16), jax.ShapeDtypeStruct((batch, seq, width), BF16)),
        in_specs=[hbm, hbm, hbm, hbm, hbm, vmem],
        out_specs=(hbm, hbm),
        scratch_shapes=[
            pltpu.VMEM((seq, q_width), BF16), pltpu.VMEM((seq, q_width), BF16), pltpu.VMEM((q_width, width), BF16), pltpu.VMEM((width, q_width), BF16),
            pltpu.VMEM((seq, width), BF16), pltpu.VMEM((2, seq, 512), BF16), pltpu.VMEM((ring // 2, rows, width), BF16),
            pltpu.VMEM((2, rows, width), BF16), pltpu.VMEM((3, 2, rows, width), BF16), pltpu.VMEM((3, rows, width), F32),
            pltpu.VMEM((3, rows, width), BF16), pltpu.VMEM((3, 2, rows, width), BF16), pltpu.VMEM((rows, width), BF16), pltpu.VMEM((rows, width), BF16),
            dma((ring // 2,)), dma((ring // 2,)), dma((2, 2)), dma((3, 2)), dma((3, 2)), dma((3, 2)), pltpu.SemaphoreType.REGULAR,
            dma((4,)), dma((2,)), dma((2,))],
        compiler_params=pltpu.CompilerParams(collective_id=1, has_side_effects=True, vmem_limit_bytes=VMEM_LIMIT),
        cost_estimate=pl.CostEstimate(flops=4 * batch * seq * width * q_width, bytes_accessed=4 * batch * seq * width, transcendentals=0),
    )(merged, grad_q, w_o, w_q, x_loc, b_o)


def norm_backward_kernel(dh, dkv, w_kv, x, dy, gamma, dx, sums):
    rows = x.shape[1]

    @pl.when(pl.program_id(0) == 0)
    def _():
        sums[...] = jnp.zeros_like(sums)

    @pl.loop(0, rows, step=16)
    def _(r):
        at = pl.ds(pl.multiple_of(r, 16), 16)
        from_kv = lax.dot_general(dkv[0, at, :], w_kv[...], (((1,), (1,)), ((), ())), preferred_element_type=F32)
        grad_h = dh[0, at, :].astype(F32) + from_kv
        x_hat, inv_std = norm_stats(x[0, at, :].astype(F32))
        grad_hat = grad_h * gamma[...]
        mean = jnp.mean(grad_hat, axis=-1, keepdims=True)
        along = jnp.mean(grad_hat * x_hat, axis=-1, keepdims=True)
        dx[0, at, :] = (dy[0, at, :].astype(F32) + inv_std * (grad_hat - mean - x_hat * along)).astype(BF16)
        by_sublane = lambda v: jnp.sum(v.reshape(-1, 8, v.shape[-1]), axis=0)
        sums[0] += by_sublane(grad_h * x_hat)
        sums[1] += by_sublane(grad_h)


def norm_backward(grad_h, grad_kv, w_kv, x_loc, dy_loc, gamma):
    batch, rows, width = x_loc.shape
    one = pl.BlockSpec((1, rows, width), lambda b: (b, 0, 0))
    still = lambda shape: pl.BlockSpec(shape, lambda b: (0,) * len(shape))
    return pl.pallas_call(
        norm_backward_kernel,
        name="norm_backward",
        grid=(batch,),
        out_shape=(jax.ShapeDtypeStruct(x_loc.shape, BF16), jax.ShapeDtypeStruct((2, 8, width), F32)),
        in_specs=[one, pl.BlockSpec((1, rows, grad_kv.shape[-1]), lambda b: (b, 0, 0)), still(w_kv.shape), one, one, still(gamma.shape)],
        out_specs=(one, still((2, 8, width))),
        compiler_params=pltpu.CompilerParams(vmem_limit_bytes=VMEM_LIMIT // 2),
        cost_estimate=pl.CostEstimate(flops=2 * batch * rows * width * 256, bytes_accessed=8 * batch * rows * width, transcendentals=0),
    )(grad_h, grad_kv, w_kv, x_loc, dy_loc, gamma)


def settle(values):
    block = pl.BlockSpec((1,) + values.shape[1:], lambda b: (b, 0, 0))

    def body(src, dst):
        dst[...] = src[...]

    return pl.pallas_call(
        body, name="settle", grid=(values.shape[0],), out_shape=jax.ShapeDtypeStruct(values.shape, values.dtype), in_specs=[block], out_specs=block,
        cost_estimate=pl.CostEstimate(flops=values.size * 100, bytes_accessed=values.size * 4, transcendentals=0))(values)


def sum_kernel(ring, parts, out, gathered, send, recv):
    me = lax.axis_index("tp")
    barrier = pltpu.get_barrier_semaphore()
    others = [lax.rem(me + k, ring) for k in range(1, ring)]
    for other in others:
        pl.semaphore_signal(barrier, inc=1, device_id={"tp": other}, device_id_type=pl.DeviceIdType.MESH)
    pl.semaphore_wait(barrier, ring - 1)

    def copy(k):
        return pltpu.make_async_remote_copy(
            src_ref=parts, dst_ref=gathered.at[me], send_sem=send.at[k], recv_sem=recv.at[k],
            device_id={"tp": lax.rem(me + k, ring)}, device_id_type=pl.DeviceIdType.MESH)

    for k in range(1, ring):
        copy(k).start()
    gathered[me] = parts[...]
    for k in range(1, ring):
        copy(k).wait_recv()
    total = gathered[0]
    for k in range(1, ring):
        total = total + gathered[k]
    out[...] = total
    for k in range(1, ring):
        copy(k).wait_send()


def sum_over_ring(parts, ring):
    vmem = pl.BlockSpec(memory_space=pltpu.VMEM)
    return pl.pallas_call(
        functools.partial(sum_kernel, ring),
        name="sum_over_ring",
        out_shape=jax.ShapeDtypeStruct(parts.shape, F32),
        in_specs=[vmem],
        out_specs=vmem,
        scratch_shapes=[pltpu.VMEM((ring,) + parts.shape, F32), pltpu.SemaphoreType.DMA((ring,)), pltpu.SemaphoreType.DMA((ring,))],
        compiler_params=pltpu.CompilerParams(collective_id=2, has_side_effects=True),
    )(parts)


def solution(mesh):
    ring = mesh.shape["tp"]

    def device_block(x_loc, ln_gamma, ln_beta, w_q, b_q, w_kv, b_kv, w_o, b_o, dy_loc):
        head_dim = w_kv.shape[1] // 2
        own_rows, width = x_loc.shape[1:]
        bias = jnp.concatenate([b_q, b_kv])[None, :]
        normed_full, dy_full, _, merged, grad_q, grad_kv, bo_rows = gather_and_attend(
            x_loc, dy_loc, ln_gamma[None, :], ln_beta[None, :], w_q, w_kv, bias, w_o, ring, head_dim)
        grad_kv = lax.psum(grad_kv, "tp")
        y_loc, grad_h_part = project_and_scatter(merged, grad_q, w_o, w_q, x_loc, b_o[None, :], ring)
        grad_h = lax.psum_scatter(grad_h_part, "tp", scatter_dimension=1, tiled=True)

        grad_h_part, grad_q, merged, y_loc, bo_rows = lax.optimization_barrier((grad_h_part, grad_q, merged, y_loc, bo_rows))
        y_loc = settle(y_loc)
        grad_bo = jnp.sum(bo_rows, axis=0)
        grad_wo = jnp.einsum("bse,bsd->ed", merged, dy_full, preferred_element_type=jnp.float32)
        grad_wq = jnp.einsum("bsd,bse->de", normed_full, grad_q, preferred_element_type=jnp.float32)
        grad_bq = jnp.sum(grad_q, axis=(0, 1), dtype=jnp.float32)
        grad_wkv = jnp.einsum("bsd,bsc->dc", normed_full, grad_kv, preferred_element_type=jnp.float32)
        grad_bkv = jnp.sum(grad_kv, axis=(0, 1), dtype=jnp.float32)
        kv_loc = lax.dynamic_slice_in_dim(grad_kv, lax.axis_index("tp") * own_rows, own_rows, axis=1)
        grad_x, parts = norm_backward(grad_h, kv_loc, w_kv, x_loc, dy_loc, ln_gamma[None, :])
        sums = sum_over_ring(jnp.sum(parts, axis=1).reshape(-1, 128), ring).reshape(2, width)
        return (y_loc, grad_x, sums[0], sums[1], grad_wq, grad_bq, grad_wkv, grad_bkv, grad_wo, grad_bo)

    return jax.shard_map(
        device_block,
        mesh=mesh,
        in_specs=(P("dp", "tp", None), P(None), P(None), P(None, "tp"), P("tp"), P(None, None), P(None), P("tp", None), P(None), P("dp", "tp", None)),
        out_specs=(P("dp", "tp", None), P("dp", "tp", None), P("dp"), P("dp"), P("dp", "tp"), P(("dp", "tp")), P("dp", None), P("dp"), P(("dp", "tp"), None), P("dp")),
        check_vma=False,
    )
```

```python
import functools

import jax
import jax.numpy as jnp
from jax import lax
from jax.experimental import pallas as pl
from jax.experimental.pallas import tpu as pltpu
from jax.sharding import PartitionSpec as P


LN_EPS = 1e-5
VMEM_LIMIT = 60 * 1024 * 1024
BF16 = jnp.bfloat16
F32 = jnp.float32

RIGHT, LEFT, PART, FAR_R, FAR_L, PASS_L, PASS_R, PASS_F = range(8)


def stack_heads(rows, dst, first, heads, dim):
    for h in range(heads):
        dst[h * dim : (h + 1) * dim, :] = rows[first : first + dim, h * dim : (h + 1) * dim]


def scaled_scores(scores_s, lanes, first, dim):
    scores = scores_s[: first + dim, lanes] * dim**-0.5
    keys = lax.broadcasted_iota(jnp.int32, scores.shape, 0)
    queries = lax.broadcasted_iota(jnp.int32, scores.shape, 1) + first
    return jnp.where(keys <= queries, scores, -1e30)


ACROSS = (((1,), (1,)), ((), ()))
DOWN = (((0,), (0,)), ((), ()))


def attend(qkv, out, stats, scores_s, probs_s, q_s, heads, dim):
    rows = qkv.shape[0]
    width = heads * dim
    for first in range(0, rows, dim):
        last = first + dim
        stack_heads(qkv, q_s, first, heads, dim)
        scores_s[:last, :] = lax.dot_general(qkv[:last, width : width + dim], q_s[...], ACROSS, preferred_element_type=F32)

        @pl.loop(0, heads, unroll=2)
        def _(h):
            lanes = pl.ds(pl.multiple_of(h * dim, dim), dim)
            scores = scaled_scores(scores_s, lanes, first, dim)
            top = jnp.max(scores, axis=0, keepdims=True)
            weights = jnp.exp(scores - top)
            share = 1.0 / jnp.sum(weights, axis=0, keepdims=True)
            probs_s[:last, lanes] = (weights * share).astype(BF16)
            stats[h, 0:1, first:last] = top
            stats[h, 1:2, first:last] = share

        turned = lax.dot_general(qkv[:last, width + dim :], probs_s[:last, :], DOWN, preferred_element_type=F32)
        for h in range(heads):
            out[first:last, h * dim : (h + 1) * dim] = turned[:, h * dim : (h + 1) * dim].T.astype(BF16)


def attend_backward(qkv, grad_att, grad_q, grad_kv, stats, scores_s, grad_p_s, probs_s, grad_s_s, q_s, att_s, heads, dim):
    rows = qkv.shape[0]
    width = heads * dim
    grad_kv[...] = jnp.zeros_like(grad_kv)
    for first in range(0, rows, dim):
        last = first + dim
        stack_heads(qkv, q_s, first, heads, dim)
        stack_heads(grad_att, att_s, first, heads, dim)
        scores_s[:last, :] = lax.dot_general(qkv[:last, width : width + dim], q_s[...], ACROSS, preferred_element_type=F32)
        grad_p_s[:last, :] = lax.dot_general(qkv[:last, width + dim :], att_s[...], ACROSS, preferred_element_type=F32)

        @pl.loop(0, heads, unroll=2)
        def _(h):
            lanes = pl.ds(pl.multiple_of(h * dim, dim), dim)
            scores = scaled_scores(scores_s, lanes, first, dim)
            probs = jnp.exp(scores - stats[h, 0:1, first:last]) * stats[h, 1:2, first:last]
            grad_p = grad_p_s[:last, lanes].astype(BF16).astype(F32)
            row_dot = jnp.sum(probs * grad_p, axis=0, keepdims=True)
            grad_s_s[:last, lanes] = (probs * (grad_p - row_dot) * dim**-0.5).astype(BF16)
            probs_s[:last, lanes] = probs.astype(BF16)

        turned = lax.dot_general(qkv[:last, width : width + dim], grad_s_s[:last, :], DOWN, preferred_element_type=F32)
        for h in range(heads):
            grad_q[first:last, h * dim : (h + 1) * dim] = turned[:, h * dim : (h + 1) * dim].T.astype(BF16)
        grad_kv[:last, :dim] += jnp.dot(grad_s_s[:last, :], q_s[...], preferred_element_type=F32)
        grad_kv[:last, dim:] += jnp.dot(probs_s[:last, :], att_s[...], preferred_element_type=F32)


def gather_kernel(heads, dim, x_hbm, dy_hbm, gamma, beta, wq_hbm, wkv_hbm, b_q, b_kv, wo_hbm,
                  h_full, dy_full, qkv_out, att_out, dq_out, dkv_out, dkv_twin, dbo, ln_stats,
                  own, x_buf, w_buf, wo_buf, h_buf, qkv_buf, att_buf, dq_buf, dkv_buf, total, stats, scores_s, grad_p_s, probs_s, grad_s_s, q_s, att_s,
                  send, recv, x_sem, dy_sem, keep_sem, w_sem, h_sem, out_sem, back_sem):
    batch, rows, width = x_hbm.shape
    half = rows // 2
    units = 2 * batch
    ring = h_full.shape[1] // rows
    me = lax.axis_index("tp")
    partner = me + 1 - 2 * lax.rem(me, 2)
    right, left, far = lax.rem(me + 2, ring), lax.rem(me + ring - 2, ring), lax.rem(me + ring // 2, ring)

    barrier = pltpu.get_barrier_semaphore()
    for other in (left, right, partner):
        pl.semaphore_signal(barrier, inc=1, device_id={"tp": other}, device_id_type=pl.DeviceIdType.MESH)
    pl.semaphore_wait(barrier, 3)

    def block(full, b, owner, first=0, count=rows):
        return full.at[b, pl.ds(pl.multiple_of(owner * rows + first, half), count)]

    def remote(src, dst, kind, u, to):
        return pltpu.make_async_remote_copy(
            src_ref=src, dst_ref=dst, send_sem=send.at[kind, u], recv_sem=recv.at[kind, u],
            device_id={"tp": to}, device_id_type=pl.DeviceIdType.MESH)

    def move(kind, full, b, u):
        if kind in (RIGHT, LEFT, PART):
            src, dst = own.at[u], block(full, b, me)
        elif kind in (FAR_R, FAR_L):
            src = dst = block(full, b, left, 0, half) if kind == FAR_R else block(full, b, right, half, half)
        else:
            src = dst = block(full, b, {PASS_L: left, PASS_R: right, PASS_F: far}[kind])
        to = {RIGHT: right, FAR_R: right, LEFT: left, FAR_L: left}.get(kind, partner)
        return remote(src, dst, kind, u, to)

    def keep(full, b, u):
        return pltpu.make_async_copy(own.at[u], block(full, b, me), keep_sem.at[u])

    def load_x(b):
        return pltpu.make_async_copy(x_hbm.at[b], x_buf.at[lax.rem(b, 2)], x_sem.at[lax.rem(b, 2)])

    def load_dy(b):
        return pltpu.make_async_copy(dy_hbm.at[b], own.at[batch + b], dy_sem.at[b])

    def unit(u, low, high, act):
        @pl.when(jnp.logical_and(u >= low, u < jnp.minimum(high, batch)))
        def _():
            act(h_full, u, u)

        @pl.when(jnp.logical_and(u >= jnp.maximum(low, batch), u < high))
        def _():
            act(dy_full, u - batch, u)

    def normalise(b):
        load_x(b).wait()
        slot = lax.rem(b, 2)

        @pl.loop(0, rows, step=16)
        def _(r):
            at = pl.ds(pl.multiple_of(r, 16), 16)
            x_wide = x_buf[slot, at, :].astype(F32)
            mean = jnp.mean(x_wide, axis=-1, keepdims=True)
            centred = x_wide - mean
            inv_std = lax.rsqrt(jnp.mean(centred * centred, axis=-1, keepdims=True) + LN_EPS)
            own[b, at, :] = (centred * inv_std * gamma[...] + beta[...]).astype(BF16)
            ln_stats[0, b, at, :] = jnp.broadcast_to(mean, (16, 128))
            ln_stats[1, b, at, :] = jnp.broadcast_to(inv_std, (16, 128))

        @pl.when(b + 2 < batch)
        def _():
            load_x(b + 2).start()

    def launch(u):
        @pl.when(u < batch)
        def _():
            normalise(u)

        @pl.when(jnp.logical_and(u >= batch, u < units))
        def _():
            load_dy(u - batch).wait()

        def act(full, b, u):
            for kind in (RIGHT, LEFT, PART):
                move(kind, full, b, u).start()
            keep(full, b, u).start()

        unit(u, 0, units, act)

    load_x(0).start()
    load_x(1).start()
    weights = (pltpu.make_async_copy(wq_hbm, w_buf.at[:, pl.ds(0, heads * dim)], w_sem.at[0]),
               pltpu.make_async_copy(wkv_hbm, w_buf.at[:, pl.ds(heads * dim, 2 * dim)], w_sem.at[1]),
               pltpu.make_async_copy(wo_hbm, wo_buf, w_sem.at[2]))
    dbo[...] = jnp.zeros_like(dbo)
    launch(0)
    launch(1)
    for copy in weights:
        copy.start()
    for b in range(batch):
        load_dy(b).start()
    for copy in weights:
        copy.wait()

    def project(b):
        load = pltpu.make_async_copy(h_full.at[b], h_buf, h_sem.at[0])
        load.start()
        load.wait()

        @pl.loop(0, heads * dim, step=256)
        def _(n):
            at = pl.ds(pl.multiple_of(n, 256), 256)
            qkv_buf[:, at] = (jnp.dot(h_buf[...], w_buf[:, at], preferred_element_type=F32) + b_q[:, at]).astype(BF16)

        at = pl.ds(heads * dim, 2 * dim)
        qkv_buf[:, at] = (jnp.dot(h_buf[...], w_buf[:, at], preferred_element_type=F32) + b_kv[...]).astype(BF16)

    def results(b):
        return (pltpu.make_async_copy(qkv_buf, qkv_out.at[b], out_sem.at[0]),
                pltpu.make_async_copy(att_buf, att_out.at[b], out_sem.at[1]))

    def back_results(b):
        return (pltpu.make_async_copy(dq_buf, dq_out.at[b], back_sem.at[0]),
                pltpu.make_async_copy(dkv_buf, dkv_out.at[b], back_sem.at[1]),
                pltpu.make_async_copy(dkv_buf, dkv_twin.at[b], back_sem.at[2]))

    def differentiate(b):
        load = pltpu.make_async_copy(dy_full.at[b], h_buf, h_sem.at[0])
        again = pltpu.make_async_copy(qkv_out.at[b], qkv_buf, h_sem.at[1])
        load.start()
        again.start()
        load.wait()

        @pl.loop(0, heads * dim, step=256)
        def _(n):
            at = pl.ds(pl.multiple_of(n, 256), 256)
            att_buf[:, at] = lax.dot_general(h_buf[...], wo_buf[at, :], (((1,), (1,)), ((), ())), preferred_element_type=F32).astype(BF16)

        @pl.loop(0, width, step=512)
        def _(n):
            at = pl.ds(pl.multiple_of(n, 512), 512)
            dbo[:, at] += jnp.sum(h_buf[:, at].astype(F32).reshape(-1, 8, 512), axis=0)

        again.wait()
        attend_backward(qkv_buf, att_buf, dq_buf, total, stats.at[b], scores_s, grad_p_s, probs_s, grad_s_s, q_s, att_s, heads, dim)
        dkv_buf[...] = total[...].astype(BF16)

    @pl.loop(0, units + 2)
    def _(s):
        def forward(full, b, u):
            move(RIGHT, full, b, u).wait_recv()
            move(FAR_R, full, b, u).start()
            move(LEFT, full, b, u).wait_recv()
            move(FAR_L, full, b, u).start()

        unit(s, 0, units, forward)
        launch(s + 2)

        def share(full, b, u):
            move(PASS_L, full, b, u).start()
            move(PASS_R, full, b, u).start()

        unit(s, 0, units, share)

        def share_far(full, b, u):
            move(FAR_R, full, b, u).wait_recv()
            move(FAR_L, full, b, u).wait_recv()
            move(PASS_F, full, b, u).start()

        unit(s - 1, 0, units, share_far)

        def complete(full, b, u):
            for kind in (PART, PASS_L, PASS_R, PASS_F):
                move(kind, full, b, u).wait_recv()
            keep(full, b, u).wait()

        unit(s - 2, 0, units, complete)

        @pl.when(jnp.logical_and(s >= 2, s < batch + 2))
        def _():
            b = s - 2

            @pl.when(b > 0)
            def _():
                for copy in results(b - 1):
                    copy.wait()

            project(b)
            attend(qkv_buf, att_buf, stats.at[b], scores_s, probs_s, q_s, heads, dim)
            for copy in results(b):
                copy.start()

        @pl.when(s >= batch + 2)
        def _():
            b = s - 2 - batch

            @pl.when(b == 0)
            def _():
                for copy in results(batch - 1):
                    copy.wait()

            @pl.when(b > 0)
            def _():
                for copy in back_results(b - 1):
                    copy.wait()

            differentiate(b)
            for copy in back_results(b):
                copy.start()

    for copy in back_results(batch - 1):
        copy.wait()

    @pl.loop(0, units)
    def _(u):
        def act(full, b, u):
            for kind in range(8):
                move(kind, full, b, u).wait_send()

        unit(u, 0, units, act)


def gather_and_attend(x_loc, dy_loc, gamma, beta, w_q, w_kv, b_q, b_kv, w_o, ring, dim):
    batch, rows, width = x_loc.shape
    q_width = w_q.shape[1]
    qkv_width = q_width + w_kv.shape[1]
    seq = rows * ring
    units = 2 * batch
    hbm = pl.BlockSpec(memory_space=pl.ANY)
    vmem = pl.BlockSpec(memory_space=pltpu.VMEM)
    dma = pltpu.SemaphoreType.DMA
    whole = lambda w: jax.ShapeDtypeStruct((batch, seq, w), BF16)
    return pl.pallas_call(
        functools.partial(gather_kernel, q_width // dim, dim),
        name="gather_and_attend",
        out_shape=(whole(width), whole(width), whole(qkv_width), whole(q_width), whole(q_width), whole(2 * dim), whole(2 * dim), jax.ShapeDtypeStruct((8, width), F32),
                   jax.ShapeDtypeStruct((2, batch, rows, 128), F32)),
        in_specs=[hbm, hbm, vmem, vmem, hbm, hbm, vmem, vmem, hbm],
        out_specs=(hbm, hbm, hbm, hbm, hbm, hbm, hbm, vmem, vmem),
        scratch_shapes=[
            pltpu.VMEM((units, rows, width), BF16), pltpu.VMEM((2, rows, width), BF16), pltpu.VMEM((width, qkv_width), BF16),
            pltpu.VMEM((q_width, width), BF16), pltpu.VMEM((seq, width), BF16), pltpu.VMEM((seq, qkv_width), BF16), pltpu.VMEM((seq, q_width), BF16),
            pltpu.VMEM((seq, q_width), BF16), pltpu.VMEM((seq, 2 * dim), BF16), pltpu.VMEM((seq, 2 * dim), F32),
            pltpu.VMEM((batch, q_width // dim, 8, seq), F32),
            pltpu.VMEM((seq, q_width), F32), pltpu.VMEM((seq, q_width), F32), pltpu.VMEM((seq, q_width), BF16), pltpu.VMEM((seq, q_width), BF16),
            pltpu.VMEM((q_width, dim), BF16), pltpu.VMEM((q_width, dim), BF16),
            dma((8, units)), dma((8, units)), dma((2,)), dma((batch,)), dma((units,)), dma((3,)), dma((2,)), dma((2,)), dma((3,))],
        compiler_params=pltpu.CompilerParams(collective_id=0, has_side_effects=True, vmem_limit_bytes=VMEM_LIMIT),
        cost_estimate=pl.CostEstimate(flops=4 * batch * seq * width * qkv_width, bytes_accessed=6 * batch * seq * width, transcendentals=0),
    )(x_loc, dy_loc, gamma, beta, w_q, w_kv, b_q, b_kv, w_o)


def scatter_kernel(att_hbm, dq_hbm, dkv_hbm, wo_hbm, wq_hbm, wkv_hbm, x_hbm, b_o, y_out, dh_early, dh_late,
                   att_buf, dq_buf, wo_buf, wq_buf, stage, dh_buf, theirs, far_sum, near_sum, own_sum, far_in, near_in, x_buf, y_buf,
                   pair_send, pair_recv, far_send, far_recv, near_send, near_recv, free, load_sem, w_sem, dh_sem):
    batch, rows, width = x_hbm.shape
    ring = stage.shape[0] // rows
    half = width // 2
    tile = 512
    me = lax.axis_index("tp")
    partner = me + 1 - 2 * lax.rem(me, 2)
    right, left = lax.rem(me + 2, ring), lax.rem(me + ring - 2, ring)
    chips = ring // 2

    barrier = pltpu.get_barrier_semaphore()
    for other in (left, right, partner):
        pl.semaphore_signal(barrier, inc=1, device_id={"tp": other}, device_id_type=pl.DeviceIdType.MESH)
    pl.semaphore_wait(barrier, 3)

    def load(src, dst, n):
        return pltpu.make_async_copy(src, dst, load_sem.at[n])

    load_att = lambda b: load(att_hbm.at[b], att_buf, 0)
    q_width = dq_hbm.shape[2]
    q_cols, kv_cols = pl.ds(0, q_width), pl.ds(q_width, dkv_hbm.shape[2])
    load_x = lambda b: load(x_hbm.at[b], x_buf, 2)
    store_y = lambda b: load(y_buf, y_out.at[b], 3)
    load_wo = pltpu.make_async_copy(wo_hbm, wo_buf, w_sem.at[0])
    load_back = (pltpu.make_async_copy(wq_hbm, wq_buf.at[:, q_cols], w_sem.at[1]), pltpu.make_async_copy(wkv_hbm, wq_buf.at[:, kv_cols], w_sem.at[2]))

    def load_grads(b):
        return load(dq_hbm.at[b], dq_buf.at[:, q_cols], 1), load(dkv_hbm.at[b], dq_buf.at[:, kv_cols], 4)

    def remote(src, dst, sems, to):
        return pltpu.make_async_remote_copy(
            src_ref=src, dst_ref=dst, send_sem=sems[0], recv_sem=sems[1], device_id={"tp": to}, device_id_type=pl.DeviceIdType.MESH)

    def block(owner):
        return pl.ds(pl.multiple_of(owner * rows, rows), rows)

    def pair(r):
        return remote(stage.at[block(lax.rem(partner + 2 * r, ring))], theirs.at[r], (pair_send.at[r], pair_recv.at[r]), partner)

    def far(u, way):
        cols = pl.ds(way * half, half)
        return remote(far_sum.at[lax.rem(u, 2), :, cols], far_in.at[lax.rem(u, 3), :, cols],
                      (far_send.at[lax.rem(u, 2), way], far_recv.at[lax.rem(u, 3), way]), (right, left)[way])

    def near(u, way):
        slot = lax.rem(u, 3)
        return remote(near_sum.at[slot, way], near_in.at[slot, way], (near_send.at[slot, way], near_recv.at[slot, way]), (right, left)[way])

    def columns(low, high, act):
        @pl.loop(low, high, step=tile)
        def _(n):
            act(pl.ds(pl.multiple_of(n, tile), tile))

    def part(u):
        load_att(u).wait()

        @pl.when(u > 0)
        def _():
            for r in range(chips):
                pair(r).wait_send()

        def act(at):
            stage[:, at] = jnp.dot(att_buf[...], wo_buf[:, at], preferred_element_type=F32).astype(BF16)

        columns(0, width, act)

        @pl.when(u + 1 < batch)
        def _():
            load_att(u + 1).start()

        @pl.when(u > 0)
        def _():
            pl.semaphore_wait(free, 1)

        for r in range(chips):
            pair(r).start()

    def combine(u):
        slot2, slot3 = lax.rem(u, 2), lax.rem(u, 3)
        for r in range(chips):
            pair(r).wait_recv()

        @pl.when(u >= 2)
        def _():
            for way in range(2):
                far(u - 2, way).wait_send()

        @pl.when(u >= 3)
        def _():
            for way in range(2):
                near(u - 3, way).wait_send()

        def chip_sum(r, at):
            return stage[block(lax.rem(me + 2 * r, ring)), at].astype(F32) + theirs[r, :, at].astype(F32)

        def act_far(at):
            far_sum[slot2, :, at] = chip_sum(chips // 2, at).astype(BF16)

        columns(0, width, act_far)
        for way in range(2):
            far(u, way).start()

        def act(at):
            near_sum[slot3, 0, :, at] = chip_sum(1, at).astype(BF16)
            near_sum[slot3, 1, :, at] = chip_sum(chips - 1, at).astype(BF16)
            own_sum[slot3, :, at] = chip_sum(0, at)

        columns(0, width, act)

        @pl.when(u + 1 < batch)
        def _():
            pl.semaphore_signal(free, inc=1, device_id={"tp": partner}, device_id_type=pl.DeviceIdType.MESH)

    def relay(u):
        slot = lax.rem(u, 3)
        for way in range(2):
            far(u, way).wait_recv()
        for way in range(2):
            def act(at):
                near_sum[slot, way, :, at] = (near_sum[slot, way, :, at].astype(F32) + far_in[slot, :, at].astype(F32)).astype(BF16)

            columns(way * half, way * half + half, act)
        for way in range(2):
            near(u, way).start()

    def finish(u):
        slot = lax.rem(u, 3)
        for way in range(2):
            near(u, way).wait_recv()
        load_x(u).wait()

        @pl.when(u > 0)
        def _():
            store_y(u - 1).wait()

        def act(at):
            total = own_sum[slot, :, at] + near_in[slot, 0, :, at].astype(F32) + near_in[slot, 1, :, at].astype(F32)
            y_buf[:, at] = (x_buf[:, at].astype(F32) + total + b_o[:, at]).astype(BF16)

        columns(0, width, act)
        store_y(u).start()

        @pl.when(u + 1 < batch)
        def _():
            load_x(u + 1).start()

    def store_dh(dh_out, b, n):
        at = pl.ds(pl.multiple_of(n, tile), tile)
        slot = lax.rem(lax.div(n, tile), 2)
        return pltpu.make_async_copy(dh_buf.at[slot], dh_out.at[b, :, at], dh_sem.at[slot])

    def grad_part(dh_out, b, place):
        for copy in load_grads(b):
            copy.wait()

        @pl.loop(0, width, step=tile)
        def _(n):
            @pl.when(n >= 2 * tile)
            def _():
                store_dh(dh_out, place, n - 2 * tile).wait()

            at = pl.ds(pl.multiple_of(n, tile), tile)
            dh_buf[lax.rem(lax.div(n, tile), 2)] = lax.dot_general(dq_buf[...], wq_buf[at, :], ACROSS, preferred_element_type=F32).astype(BF16)
            store_dh(dh_out, place, n).start()

        @pl.when(b + 1 < batch)
        def _():
            for copy in load_grads(b + 1):
                copy.start()

        for n in (width - 2 * tile, width - tile):
            store_dh(dh_out, place, n).wait()

    load_att(0).start()
    load_wo.start()
    for copy in load_back + load_grads(0):
        copy.start()
    load_x(0).start()
    load_wo.wait()

    @pl.loop(0, batch + 3)
    def _(t):
        @pl.when(jnp.logical_and(t >= 1, t < batch + 1))
        def _():
            combine(t - 1)

        @pl.when(jnp.logical_and(t >= 2, t < batch + 2))
        def _():
            relay(t - 2)

        @pl.when(t >= 3)
        def _():
            finish(t - 3)

        @pl.when(t < batch)
        def _():
            part(t)

        @pl.when(t == 2)
        def _():
            for copy in load_back:
                copy.wait()

        @pl.when(jnp.logical_and(t >= 2, t < batch // 2 + 2))
        def _():
            grad_part(dh_early, t - 2, t - 2)

        @pl.when(jnp.logical_and(t >= batch // 2 + 2, t < batch + 2))
        def _():
            grad_part(dh_late, t - 2, t - 2 - batch // 2)

    for r in range(chips):
        pair(r).wait_send()
    for way in range(2):
        for u in (batch - 2, batch - 1):
            far(u, way).wait_send()
        for u in (batch - 3, batch - 2, batch - 1):
            near(u, way).wait_send()
    store_y(batch - 1).wait()


def project_and_scatter(merged, grad_q, grad_kv, w_o, w_q, w_kv, x_loc, b_o, ring):
    batch, rows, width = x_loc.shape
    seq, q_width = merged.shape[1:]
    qkv_width = q_width + w_kv.shape[1]
    part = jax.ShapeDtypeStruct((batch // 2, seq, width), BF16)
    hbm = pl.BlockSpec(memory_space=pl.ANY)
    vmem = pl.BlockSpec(memory_space=pltpu.VMEM)
    dma = pltpu.SemaphoreType.DMA
    return pl.pallas_call(
        scatter_kernel,
        name="project_and_scatter",
        out_shape=(jax.ShapeDtypeStruct(x_loc.shape, BF16), part, part),
        in_specs=[hbm, hbm, hbm, hbm, hbm, hbm, hbm, vmem],
        out_specs=(hbm, hbm, hbm),
        scratch_shapes=[
            pltpu.VMEM((seq, q_width), BF16), pltpu.VMEM((seq, qkv_width), BF16), pltpu.VMEM((q_width, width), BF16), pltpu.VMEM((width, qkv_width), BF16),
            pltpu.VMEM((seq, width), BF16), pltpu.VMEM((2, seq, 512), BF16), pltpu.VMEM((ring // 2, rows, width), BF16),
            pltpu.VMEM((2, rows, width), BF16), pltpu.VMEM((3, 2, rows, width), BF16), pltpu.VMEM((3, rows, width), F32),
            pltpu.VMEM((3, rows, width), BF16), pltpu.VMEM((3, 2, rows, width), BF16), pltpu.VMEM((rows, width), BF16), pltpu.VMEM((rows, width), BF16),
            dma((ring // 2,)), dma((ring // 2,)), dma((2, 2)), dma((3, 2)), dma((3, 2)), dma((3, 2)), pltpu.SemaphoreType.REGULAR,
            dma((5,)), dma((3,)), dma((2,))],
        compiler_params=pltpu.CompilerParams(collective_id=1, has_side_effects=True, vmem_limit_bytes=VMEM_LIMIT),
        cost_estimate=pl.CostEstimate(flops=4 * batch * seq * width * q_width, bytes_accessed=4 * batch * seq * width, transcendentals=0),
    )(merged, grad_q, grad_kv, w_o, w_q, w_kv, x_loc, b_o)


def norm_backward_kernel(dh, x, dy, ln_stats, gamma, *refs):
    dx, sums = refs[-2:]
    rows, width = x.shape[1:]
    tile = 512

    @pl.when(pl.program_id(0) == 0)
    def _():
        sums[...] = jnp.zeros_like(sums)

    mean, inv_std = ln_stats[0, 0, :, :1], ln_stats[1, 0, :, :1]
    by_lane = lambda v: sum(v[:, n : n + 128] for n in range(0, tile, 128))
    by_sublane = lambda v: jnp.sum(v.reshape(-1, 8, tile), axis=0)
    plain = along = jnp.zeros((rows, 128), F32)
    for n in range(0, width, tile):
        at = slice(n, n + tile)
        grad_h = dh[0, :, at].astype(F32)
        x_hat = (x[0, :, at].astype(F32) - mean) * inv_std
        both = grad_h * x_hat
        plain = plain + by_lane(grad_h * gamma[:, at])
        along = along + by_lane(both * gamma[:, at])
        sums[0, :, at] += by_sublane(both)
        sums[1, :, at] += by_sublane(grad_h)
    plain = jnp.sum(plain, axis=-1, keepdims=True) / width
    along = jnp.sum(along, axis=-1, keepdims=True) / width
    for n in range(0, width, tile):
        at = slice(n, n + tile)
        x_hat = (x[0, :, at].astype(F32) - mean) * inv_std
        grad_in = inv_std * (dh[0, :, at].astype(F32) * gamma[:, at] - plain - x_hat * along)
        dx[0, :, at] = (dy[0, :, at].astype(F32) + grad_in).astype(BF16)


def norm_backward(grad_h, x_loc, dy_loc, ln_stats, gamma, first, started):
    rows, width = x_loc.shape[1:]
    count = grad_h.shape[0]
    block = lambda skip: pl.BlockSpec((1, rows, width), lambda b: (b + skip, 0, 0))
    still = lambda shape: pl.BlockSpec(shape, lambda b: (0,) * len(shape))
    extra = [] if started is None else [started]
    return pl.pallas_call(
        norm_backward_kernel,
        name="norm_backward",
        grid=(count,),
        out_shape=(jax.ShapeDtypeStruct(x_loc.shape, BF16), jax.ShapeDtypeStruct((2, 8, width), F32)),
        in_specs=[block(0), block(first), block(first), pl.BlockSpec((2, 1, rows, 128), lambda b: (0, b + first, 0, 0)), still(gamma.shape)]
        + [pl.BlockSpec(memory_space=pl.ANY)] * len(extra),
        out_specs=(block(first), still((2, 8, width))),
        input_output_aliases={5: 0} if extra else {},
        compiler_params=pltpu.CompilerParams(vmem_limit_bytes=VMEM_LIMIT),
        cost_estimate=pl.CostEstimate(flops=60 * count * rows * width, bytes_accessed=8 * count * rows * width, transcendentals=0),
    )(grad_h, x_loc, dy_loc, ln_stats, gamma, *extra)


def settle(values):
    block = pl.BlockSpec((1,) + values.shape[1:], lambda b: (b, 0, 0))

    def body(src, dst):
        dst[...] = src[...]

    return pl.pallas_call(
        body, name="settle", grid=(values.shape[0],), out_shape=jax.ShapeDtypeStruct(values.shape, values.dtype), in_specs=[block], out_specs=block,
        cost_estimate=pl.CostEstimate(flops=values.size * 100, bytes_accessed=values.size * 4, transcendentals=0))(values)


def sum_kernel(ring, parts, out, gathered, send, recv):
    me = lax.axis_index("tp")
    barrier = pltpu.get_barrier_semaphore()
    others = [lax.rem(me + k, ring) for k in range(1, ring)]
    for other in others:
        pl.semaphore_signal(barrier, inc=1, device_id={"tp": other}, device_id_type=pl.DeviceIdType.MESH)
    pl.semaphore_wait(barrier, ring - 1)

    def copy(k):
        return pltpu.make_async_remote_copy(
            src_ref=parts, dst_ref=gathered.at[me], send_sem=send.at[k], recv_sem=recv.at[k],
            device_id={"tp": lax.rem(me + k, ring)}, device_id_type=pl.DeviceIdType.MESH)

    for k in range(1, ring):
        copy(k).start()
    gathered[me] = parts[...]
    for k in range(1, ring):
        copy(k).wait_recv()
    total = gathered[0]
    for k in range(1, ring):
        total = total + gathered[k]
    out[...] = total
    for k in range(1, ring):
        copy(k).wait_send()


def sum_over_ring(parts, ring):
    vmem = pl.BlockSpec(memory_space=pltpu.VMEM)
    return pl.pallas_call(
        functools.partial(sum_kernel, ring),
        name="sum_over_ring",
        out_shape=jax.ShapeDtypeStruct(parts.shape, F32),
        in_specs=[vmem],
        out_specs=vmem,
        scratch_shapes=[pltpu.VMEM((ring,) + parts.shape, F32), pltpu.SemaphoreType.DMA((ring,)), pltpu.SemaphoreType.DMA((ring,))],
        compiler_params=pltpu.CompilerParams(collective_id=2, has_side_effects=True),
    )(parts)


def solution(mesh):
    ring = mesh.shape["tp"]

    def device_block(x_loc, ln_gamma, ln_beta, w_q, b_q, w_kv, b_kv, w_o, b_o, dy_loc):
        head_dim = w_kv.shape[1] // 2
        batch, _, width = x_loc.shape
        normed_full, dy_full, _, merged, grad_q, kv_part, kv_twin, bo_rows, ln_stats = gather_and_attend(
            x_loc, dy_loc, ln_gamma[None, :], ln_beta[None, :], w_q, w_kv, b_q[None, :], b_kv[None, :], w_o, ring, head_dim)
        grad_kv = lax.psum(kv_twin, "tp")
        y_loc, dh_early, dh_late = project_and_scatter(merged, grad_q, kv_part, w_o, w_q, w_kv, x_loc, b_o[None, :], ring)
        scatter = lambda part: lax.psum_scatter(part, "tp", scatter_dimension=1, tiled=True)
        dh_early_loc = scatter(dh_early)
        dh_late_loc = scatter(dh_late)

        grad_q, merged, y_loc, bo_rows = lax.optimization_barrier((grad_q, merged, y_loc, bo_rows))
        y_loc = settle(y_loc)
        grad_bo = jnp.sum(bo_rows, axis=0)
        grad_wo = jnp.einsum("bse,bsd->ed", merged, dy_full, preferred_element_type=jnp.float32)
        grad_wq = jnp.einsum("bsd,bse->de", normed_full, grad_q, preferred_element_type=jnp.float32)
        grad_bq = jnp.sum(grad_q, axis=(0, 1), dtype=jnp.float32)
        grad_wkv = jnp.einsum("bsd,bsc->dc", normed_full, grad_kv, preferred_element_type=jnp.float32)
        grad_bkv = jnp.sum(grad_kv, axis=(0, 1), dtype=jnp.float32)
        gamma = ln_gamma[None, :]
        started, parts_early = norm_backward(dh_early_loc, x_loc, dy_loc, ln_stats, gamma, 0, None)
        grad_x, parts_late = norm_backward(dh_late_loc, x_loc, dy_loc, ln_stats, gamma, batch // 2, started)
        sums = sum_over_ring(jnp.sum(parts_early + parts_late, axis=1).reshape(-1, 128), ring).reshape(2, width)
        return (y_loc, grad_x, sums[0], sums[1], grad_wq, grad_bq, grad_wkv, grad_bkv, grad_wo, grad_bo)

    return jax.shard_map(
        device_block,
        mesh=mesh,
        in_specs=(P("dp", "tp", None), P(None), P(None), P(None, "tp"), P("tp"), P(None, None), P(None), P("tp", None), P(None), P("dp", "tp", None)),
        out_specs=(P("dp", "tp", None), P("dp", "tp", None), P("dp"), P("dp"), P("dp", "tp"), P(("dp", "tp")), P("dp", None), P("dp"), P(("dp", "tp"), None), P("dp")),
        check_vma=False,
    )
```

```python
import functools

import jax
import jax.numpy as jnp
from jax import lax
from jax.experimental import pallas as pl
from jax.experimental.pallas import tpu as pltpu
from jax.sharding import PartitionSpec as P


LN_EPS = 1e-5
VMEM_LIMIT = 60 * 1024 * 1024
BF16 = jnp.bfloat16
F32 = jnp.float32

RIGHT, LEFT, PART, FAR_R, FAR_L, PASS_L, PASS_R, PASS_F = range(8)


def stack_heads(rows, dst, first, heads, dim):
    for h in range(heads):
        dst[h * dim : (h + 1) * dim, :] = rows[first : first + dim, h * dim : (h + 1) * dim]


def scaled_scores(scores_s, lanes, first, dim):
    scores = scores_s[: first + dim, lanes] * dim**-0.5
    keys = lax.broadcasted_iota(jnp.int32, scores.shape, 0)
    queries = lax.broadcasted_iota(jnp.int32, scores.shape, 1) + first
    return jnp.where(keys <= queries, scores, -1e30)


ACROSS = (((1,), (1,)), ((), ()))
DOWN = (((0,), (0,)), ((), ()))


def attend(qkv, out, stats, scores_s, probs_s, q_s, heads, dim):
    rows = qkv.shape[0]
    width = heads * dim
    for first in range(0, rows, dim):
        last = first + dim
        stack_heads(qkv, q_s, first, heads, dim)
        scores_s[:last, :] = lax.dot_general(qkv[:last, width : width + dim], q_s[...], ACROSS, preferred_element_type=F32)

        @pl.loop(0, heads, unroll=2)
        def _(h):
            lanes = pl.ds(pl.multiple_of(h * dim, dim), dim)
            scores = scaled_scores(scores_s, lanes, first, dim)
            top = jnp.max(scores, axis=0, keepdims=True)
            weights = jnp.exp(scores - top)
            share = 1.0 / jnp.sum(weights, axis=0, keepdims=True)
            probs_s[:last, lanes] = (weights * share).astype(BF16)
            stats[h, 0:1, first:last] = top
            stats[h, 1:2, first:last] = share

        turned = lax.dot_general(qkv[:last, width + dim :], probs_s[:last, :], DOWN, preferred_element_type=F32)
        for h in range(heads):
            out[first:last, h * dim : (h + 1) * dim] = turned[:, h * dim : (h + 1) * dim].T.astype(BF16)


def attend_backward(qkv, grad_att, grad_q, grad_kv, stats, scores_s, grad_p_s, probs_s, grad_s_s, q_s, att_s, heads, dim):
    rows = qkv.shape[0]
    width = heads * dim
    grad_kv[...] = jnp.zeros_like(grad_kv)
    for first in range(0, rows, dim):
        last = first + dim
        stack_heads(qkv, q_s, first, heads, dim)
        stack_heads(grad_att, att_s, first, heads, dim)
        scores_s[:last, :] = lax.dot_general(qkv[:last, width : width + dim], q_s[...], ACROSS, preferred_element_type=F32)
        grad_p_s[:last, :] = lax.dot_general(qkv[:last, width + dim :], att_s[...], ACROSS, preferred_element_type=F32)

        @pl.loop(0, heads, unroll=2)
        def _(h):
            lanes = pl.ds(pl.multiple_of(h * dim, dim), dim)
            scores = scaled_scores(scores_s, lanes, first, dim)
            probs = jnp.exp(scores - stats[h, 0:1, first:last]) * stats[h, 1:2, first:last]
            grad_p = grad_p_s[:last, lanes].astype(BF16).astype(F32)
            row_dot = jnp.sum(probs * grad_p, axis=0, keepdims=True)
            grad_s_s[:last, lanes] = (probs * (grad_p - row_dot) * dim**-0.5).astype(BF16)
            probs_s[:last, lanes] = probs.astype(BF16)

        turned = lax.dot_general(qkv[:last, width : width + dim], grad_s_s[:last, :], DOWN, preferred_element_type=F32)
        for h in range(heads):
            grad_q[first:last, h * dim : (h + 1) * dim] = turned[:, h * dim : (h + 1) * dim].T.astype(BF16)
        grad_kv[:last, :dim] += jnp.dot(grad_s_s[:last, :], q_s[...], preferred_element_type=F32)
        grad_kv[:last, dim:] += jnp.dot(probs_s[:last, :], att_s[...], preferred_element_type=F32)


def gather_kernel(heads, dim, x_hbm, dy_hbm, gamma, beta, wq_hbm, wkv_hbm, b_q, b_kv, wo_hbm,
                  h_full, dy_full, att_out, o_part, dq_out, dkv_out, dkv_twin, dbo, ln_stats,
                  own, x_buf, w_buf, wo_buf, h_buf, qkv_buf, att_buf, da_buf, dq_buf, dkv_buf, o_buf, total, stats,
                  scores_s, grad_p_s, probs_s, grad_s_s, q_s, att_s,
                  send, recv, x_sem, dy_sem, keep_sem, w_sem, h_sem, att_sem, back_sem, o_sem):
    batch, rows, width = x_hbm.shape
    half = rows // 2
    units = 2 * batch
    ring = h_full.shape[1] // rows
    tile = 512
    me = lax.axis_index("tp")
    partner = me + 1 - 2 * lax.rem(me, 2)
    right, left, far = lax.rem(me + 2, ring), lax.rem(me + ring - 2, ring), lax.rem(me + ring // 2, ring)

    barrier = pltpu.get_barrier_semaphore()
    for other in (left, right, partner):
        pl.semaphore_signal(barrier, inc=1, device_id={"tp": other}, device_id_type=pl.DeviceIdType.MESH)
    pl.semaphore_wait(barrier, 3)

    def block(full, b, owner, first=0, count=rows):
        return full.at[b, pl.ds(pl.multiple_of(owner * rows + first, half), count)]

    def remote(src, dst, kind, u, to):
        return pltpu.make_async_remote_copy(
            src_ref=src, dst_ref=dst, send_sem=send.at[kind, u], recv_sem=recv.at[kind, u],
            device_id={"tp": to}, device_id_type=pl.DeviceIdType.MESH)

    def move(kind, full, b, u):
        if kind in (RIGHT, LEFT, PART):
            src, dst = own.at[u], block(full, b, me)
        elif kind in (FAR_R, FAR_L):
            src = dst = block(full, b, left, 0, half) if kind == FAR_R else block(full, b, right, half, half)
        else:
            src = dst = block(full, b, {PASS_L: left, PASS_R: right, PASS_F: far}[kind])
        to = {RIGHT: right, FAR_R: right, LEFT: left, FAR_L: left}.get(kind, partner)
        return remote(src, dst, kind, u, to)

    def keep(full, b, u):
        return pltpu.make_async_copy(own.at[u], block(full, b, me), keep_sem.at[u])

    def load_x(b):
        return pltpu.make_async_copy(x_hbm.at[b], x_buf.at[lax.rem(b, 2)], x_sem.at[lax.rem(b, 2)])

    def load_dy(b):
        return pltpu.make_async_copy(dy_hbm.at[b], own.at[2 * b + 1], dy_sem.at[b])

    def turn(u, low, high, h_act, dy_act):
        b = lax.div(u, 2)
        inside = jnp.logical_and(u >= low, u < high)

        @pl.when(jnp.logical_and(inside, lax.rem(u, 2) == 0))
        def _():
            h_act(b)

        @pl.when(jnp.logical_and(inside, lax.rem(u, 2) == 1))
        def _():
            dy_act(b)

    def unit(u, low, high, act):
        turn(u, low, high, lambda b: act(h_full, b, u), lambda b: act(dy_full, b, u))

    def normalise(b):
        load_x(b).wait()
        slot = lax.rem(b, 2)

        @pl.loop(0, rows, step=16)
        def _(r):
            at = pl.ds(pl.multiple_of(r, 16), 16)
            x_wide = x_buf[slot, at, :].astype(F32)
            mean = jnp.mean(x_wide, axis=-1, keepdims=True)
            centred = x_wide - mean
            inv_std = lax.rsqrt(jnp.mean(centred * centred, axis=-1, keepdims=True) + LN_EPS)
            own[2 * b, at, :] = (centred * inv_std * gamma[...] + beta[...]).astype(BF16)
            ln_stats[0, b, at, :] = jnp.broadcast_to(mean, (16, 128))
            ln_stats[1, b, at, :] = jnp.broadcast_to(inv_std, (16, 128))

        @pl.when(b + 2 < batch)
        def _():
            load_x(b + 2).start()

    def launch(u):
        turn(u, 0, units, normalise, lambda b: load_dy(b).wait())

        def act(full, b, u):
            for kind in (RIGHT, LEFT, PART):
                move(kind, full, b, u).start()
            keep(full, b, u).start()

        unit(u, 0, units, act)

    load_x(0).start()
    load_dy(0).start()
    load_x(1).start()
    weights = (pltpu.make_async_copy(wq_hbm, w_buf.at[:, pl.ds(0, heads * dim)], w_sem.at[0]),
               pltpu.make_async_copy(wkv_hbm, w_buf.at[:, pl.ds(heads * dim, 2 * dim)], w_sem.at[1]),
               pltpu.make_async_copy(wo_hbm, wo_buf, w_sem.at[2]))
    launch(0)
    launch(1)
    for copy in weights:
        copy.start()
    for b in range(1, batch):
        load_dy(b).start()
    dbo[...] = jnp.zeros_like(dbo)
    for copy in weights:
        copy.wait()

    def load_block(full, b):
        load = pltpu.make_async_copy(full.at[b], h_buf, h_sem.at[0])
        load.start()
        load.wait()

    def project(b):
        load_block(h_full, b)

        @pl.loop(0, heads * dim, step=256)
        def _(n):
            at = pl.ds(pl.multiple_of(n, 256), 256)
            qkv_buf[:, at] = (jnp.dot(h_buf[...], w_buf[:, at], preferred_element_type=F32) + b_q[:, at]).astype(BF16)

        at = pl.ds(heads * dim, 2 * dim)
        qkv_buf[:, at] = (jnp.dot(h_buf[...], w_buf[:, at], preferred_element_type=F32) + b_kv[...]).astype(BF16)

    def store_att(b):
        return pltpu.make_async_copy(att_buf, att_out.at[b], att_sem.at[0])

    def store_o(b, n):
        at = pl.ds(pl.multiple_of(n, tile), tile)
        slot = lax.rem(lax.div(n, tile), 2)
        return pltpu.make_async_copy(o_buf.at[slot], o_part.at[b, :, at], o_sem.at[slot])

    def attend_and_project(b):
        @pl.when(b > 0)
        def _():
            store_att(b - 1).wait()

        attend(qkv_buf, att_buf, stats, scores_s, probs_s, q_s, heads, dim)
        store_att(b).start()

        @pl.loop(0, width, step=tile)
        def _(n):
            @pl.when(n >= 2 * tile)
            def _():
                store_o(b, n - 2 * tile).wait()

            at = pl.ds(pl.multiple_of(n, tile), tile)
            o_buf[lax.rem(lax.div(n, tile), 2)] = jnp.dot(att_buf[...], wo_buf[:, at], preferred_element_type=F32).astype(BF16)
            store_o(b, n).start()

        for n in (width - 2 * tile, width - tile):
            store_o(b, n).wait()

    def grad_attended(b):
        load_block(dy_full, b)

        @pl.loop(0, heads * dim, step=256)
        def _(n):
            at = pl.ds(pl.multiple_of(n, 256), 256)
            da_buf[:, at] = lax.dot_general(h_buf[...], wo_buf[at, :], ACROSS, preferred_element_type=F32).astype(BF16)

        @pl.loop(0, width, step=tile)
        def _(n):
            at = pl.ds(pl.multiple_of(n, tile), tile)
            dbo[:, at] += jnp.sum(h_buf[:, at].astype(F32).reshape(-1, 8, tile), axis=0)

    def back_results(b):
        return (pltpu.make_async_copy(dq_buf, dq_out.at[b], back_sem.at[0]),
                pltpu.make_async_copy(dkv_buf, dkv_out.at[b], back_sem.at[1]),
                pltpu.make_async_copy(dkv_buf, dkv_twin.at[b], back_sem.at[2]))

    def differentiate(b):
        @pl.when(b > 0)
        def _():
            for copy in back_results(b - 1):
                copy.wait()

        attend_backward(qkv_buf, da_buf, dq_buf, total, stats, scores_s, grad_p_s, probs_s, grad_s_s, q_s, att_s, heads, dim)
        dkv_buf[...] = total[...].astype(BF16)
        for copy in back_results(b):
            copy.start()

    @pl.loop(0, units + 2)
    def _(s):
        def forward(full, b, u):
            move(RIGHT, full, b, u).wait_recv()
            move(FAR_R, full, b, u).start()
            move(LEFT, full, b, u).wait_recv()
            move(FAR_L, full, b, u).start()

        unit(s, 0, units, forward)
        launch(s + 2)

        def share(full, b, u):
            move(PASS_L, full, b, u).start()
            move(PASS_R, full, b, u).start()

        unit(s, 0, units, share)
        turn(s - 2, 0, units, attend_and_project, differentiate)

        def share_far(full, b, u):
            move(FAR_R, full, b, u).wait_recv()
            move(FAR_L, full, b, u).wait_recv()
            move(PASS_F, full, b, u).start()

        unit(s - 1, 0, units, share_far)

        def complete(full, b, u):
            for kind in (PART, PASS_L, PASS_R, PASS_F):
                move(kind, full, b, u).wait_recv()
            keep(full, b, u).wait()

        unit(s - 1, 0, units, complete)
        turn(s - 1, 0, units, project, grad_attended)

    store_att(batch - 1).wait()
    for copy in back_results(batch - 1):
        copy.wait()

    @pl.loop(0, units)
    def _(u):
        def act(full, b, u):
            for kind in range(8):
                move(kind, full, b, u).wait_send()

        unit(u, 0, units, act)


def gather_and_attend(x_loc, dy_loc, gamma, beta, w_q, w_kv, b_q, b_kv, w_o, ring, dim):
    batch, rows, width = x_loc.shape
    q_width = w_q.shape[1]
    qkv_width = q_width + w_kv.shape[1]
    seq = rows * ring
    units = 2 * batch
    heads = q_width // dim
    hbm = pl.BlockSpec(memory_space=pl.ANY)
    vmem = pl.BlockSpec(memory_space=pltpu.VMEM)
    dma = pltpu.SemaphoreType.DMA
    whole = lambda w: jax.ShapeDtypeStruct((batch, seq, w), BF16)
    return pl.pallas_call(
        functools.partial(gather_kernel, heads, dim),
        name="gather_and_attend",
        out_shape=(whole(width), whole(width), whole(q_width), whole(width), whole(q_width), whole(2 * dim), whole(2 * dim),
                   jax.ShapeDtypeStruct((8, width), F32), jax.ShapeDtypeStruct((2, batch, rows, 128), F32)),
        in_specs=[hbm, hbm, vmem, vmem, hbm, hbm, vmem, vmem, hbm],
        out_specs=(hbm,) * 7 + (vmem, vmem),
        scratch_shapes=[
            pltpu.VMEM((units, rows, width), BF16), pltpu.VMEM((2, rows, width), BF16), pltpu.VMEM((width, qkv_width), BF16),
            pltpu.VMEM((q_width, width), BF16), pltpu.VMEM((seq, width), BF16), pltpu.VMEM((seq, qkv_width), BF16), pltpu.VMEM((seq, q_width), BF16),
            pltpu.VMEM((seq, q_width), BF16), pltpu.VMEM((seq, q_width), BF16), pltpu.VMEM((seq, 2 * dim), BF16), pltpu.VMEM((2, seq, 512), BF16),
            pltpu.VMEM((seq, 2 * dim), F32), pltpu.VMEM((heads, 8, seq), F32),
            pltpu.VMEM((seq, q_width), F32), pltpu.VMEM((seq, q_width), F32), pltpu.VMEM((seq, q_width), BF16), pltpu.VMEM((seq, q_width), BF16),
            pltpu.VMEM((q_width, dim), BF16), pltpu.VMEM((q_width, dim), BF16),
            dma((8, units)), dma((8, units)), dma((2,)), dma((batch,)), dma((units,)), dma((3,)), dma((1,)), dma((1,)), dma((3,)), dma((2,))],
        compiler_params=pltpu.CompilerParams(collective_id=0, has_side_effects=True, vmem_limit_bytes=VMEM_LIMIT),
        cost_estimate=pl.CostEstimate(flops=6 * batch * seq * width * qkv_width, bytes_accessed=6 * batch * seq * width, transcendentals=0),
    )(x_loc, dy_loc, gamma, beta, w_q, w_kv, b_q, b_kv, w_o)


def scatter_kernel(o_part, dq_hbm, dkv_hbm, wq_hbm, wkv_hbm, x_hbm, b_o, y_out, dh_early, dh_late, dh_sum,
                   dq_buf, w_buf, ours, dh_buf, theirs, far_sum, near_sum, own_sum, far_in, near_in, x_buf, y_buf,
                   ours_sem, pair_send, pair_recv, far_send, far_recv, near_send, near_recv, free, load_sem, w_sem, dh_sem):
    batch, rows, width = x_hbm.shape
    early = dh_early.shape[0]
    units = batch + early
    ring = o_part.shape[1] // rows
    half = width // 2
    tile = 512
    me = lax.axis_index("tp")
    partner = me + 1 - 2 * lax.rem(me, 2)
    right, left = lax.rem(me + 2, ring), lax.rem(me + ring - 2, ring)
    chips = ring // 2

    barrier = pltpu.get_barrier_semaphore()
    for other in (left, right, partner):
        pl.semaphore_signal(barrier, inc=1, device_id={"tp": other}, device_id_type=pl.DeviceIdType.MESH)
    pl.semaphore_wait(barrier, 3)

    def load(src, dst, n):
        return pltpu.make_async_copy(src, dst, load_sem.at[n])

    q_width = dq_hbm.shape[2]
    q_cols, kv_cols = pl.ds(0, q_width), pl.ds(q_width, dkv_hbm.shape[2])
    load_x = lambda b: load(x_hbm.at[b], x_buf, 0)
    store_y = lambda u: load(y_buf, y_out.at[u], 1)
    store_sum = lambda u: load(y_buf, dh_sum.at[u - batch], 1)
    load_w = (pltpu.make_async_copy(wq_hbm, w_buf.at[:, q_cols], w_sem.at[0]), pltpu.make_async_copy(wkv_hbm, w_buf.at[:, kv_cols], w_sem.at[1]))

    def load_grads(b):
        return load(dq_hbm.at[b], dq_buf.at[:, q_cols], 2), load(dkv_hbm.at[b], dq_buf.at[:, kv_cols], 3)

    def remote(src, dst, sems, to):
        return pltpu.make_async_remote_copy(
            src_ref=src, dst_ref=dst, send_sem=sems[0], recv_sem=sems[1], device_id={"tp": to}, device_id_type=pl.DeviceIdType.MESH)

    def block(owner):
        return pl.ds(pl.multiple_of(owner * rows, rows), rows)

    def sourced(u, act):
        @pl.when(u < batch)
        def _():
            act(o_part.at[u])

        @pl.when(u >= batch)
        def _():
            act(dh_early.at[u - batch])

    def mine(part, u, r):
        slot = lax.rem(u, 2)
        return pltpu.make_async_copy(part.at[block(lax.rem(me + 2 * r, ring))], ours.at[slot, r], ours_sem.at[slot, r])

    def pair(part, u, r):
        slot = lax.rem(u, 2)
        return remote(part.at[block(lax.rem(partner + 2 * r, ring))], theirs.at[slot, r], (pair_send.at[slot, r], pair_recv.at[slot, r]), partner)

    def far(u, way):
        cols = pl.ds(way * half, half)
        return remote(far_sum.at[lax.rem(u, 2), :, cols], far_in.at[lax.rem(u, 3), :, cols],
                      (far_send.at[lax.rem(u, 2), way], far_recv.at[lax.rem(u, 3), way]), (right, left)[way])

    def near(u, way):
        slot = lax.rem(u, 3)
        return remote(near_sum.at[slot, way], near_in.at[slot, way], (near_send.at[slot, way], near_recv.at[slot, way]), (right, left)[way])

    def columns(low, high, act):
        @pl.loop(low, high, step=tile)
        def _(n):
            act(pl.ds(pl.multiple_of(n, tile), tile))

    def fetch(u):
        @pl.when(u >= 2)
        def _():
            pl.semaphore_wait(free, 1)
            for r in range(chips):
                pair(o_part.at[0], u, r).wait_send()

        def act(part):
            for r in range(chips):
                pair(part, u, r).start()
            for r in range(chips):
                mine(part, u, r).start()

        sourced(u, act)

    def combine(u):
        slot2, slot3 = lax.rem(u, 2), lax.rem(u, 3)
        for r in range(chips):
            mine(o_part.at[0], u, r).wait()
            pair(o_part.at[0], u, r).wait_recv()

        @pl.when(u >= 2)
        def _():
            for way in range(2):
                far(u - 2, way).wait_send()

        @pl.when(u >= 3)
        def _():
            for way in range(2):
                near(u - 3, way).wait_send()

        def chip_sum(r, at):
            return ours[slot2, r, :, at].astype(F32) + theirs[slot2, r, :, at].astype(F32)

        def act_far(at):
            far_sum[slot2, :, at] = chip_sum(chips // 2, at).astype(BF16)

        columns(0, width, act_far)
        for way in range(2):
            far(u, way).start()

        def act(at):
            near_sum[slot3, 0, :, at] = chip_sum(1, at).astype(BF16)
            near_sum[slot3, 1, :, at] = chip_sum(chips - 1, at).astype(BF16)
            own_sum[slot3, :, at] = chip_sum(0, at)

        columns(0, width, act)

        @pl.when(u + 2 < units)
        def _():
            pl.semaphore_signal(free, inc=1, device_id={"tp": partner}, device_id_type=pl.DeviceIdType.MESH)

    def relay(u):
        slot = lax.rem(u, 3)
        for way in range(2):
            far(u, way).wait_recv()
        for way in range(2):
            def act(at):
                near_sum[slot, way, :, at] = (near_sum[slot, way, :, at].astype(F32) + far_in[slot, :, at].astype(F32)).astype(BF16)

            columns(way * half, way * half + half, act)
        for way in range(2):
            near(u, way).start()

    def finish(u):
        slot = lax.rem(u, 3)
        for way in range(2):
            near(u, way).wait_recv()

        @pl.when(u > 0)
        def _():
            store_y(0).wait()

        def total(at):
            return own_sum[slot, :, at] + near_in[slot, 0, :, at].astype(F32) + near_in[slot, 1, :, at].astype(F32)

        @pl.when(u < batch)
        def _():
            load_x(u).wait()

            def act(at):
                y_buf[:, at] = (x_buf[:, at].astype(F32) + total(at) + b_o[:, at]).astype(BF16)

            columns(0, width, act)
            store_y(u).start()

        @pl.when(u >= batch)
        def _():
            def act(at):
                y_buf[:, at] = total(at).astype(BF16)

            columns(0, width, act)
            store_sum(u).start()

        @pl.when(u + 1 < batch)
        def _():
            load_x(u + 1).start()

    def store_dh(dh_out, b, n):
        at = pl.ds(pl.multiple_of(n, tile), tile)
        slot = lax.rem(lax.div(n, tile), 2)
        return pltpu.make_async_copy(dh_buf.at[slot], dh_out.at[b, :, at], dh_sem.at[slot])

    def grad_part(b):
        for copy in load_grads(b):
            copy.wait()

        @pl.loop(0, width, step=tile)
        def _(n):
            @pl.when(n >= 2 * tile)
            def _():
                store_dh(dh_late, 0, n - 2 * tile).wait()

            at = pl.ds(pl.multiple_of(n, tile), tile)
            dh_buf[lax.rem(lax.div(n, tile), 2)] = lax.dot_general(dq_buf[...], w_buf[at, :], ACROSS, preferred_element_type=F32).astype(BF16)

            @pl.when(b < early)
            def _():
                store_dh(dh_early, b, n).start()

            @pl.when(b >= early)
            def _():
                store_dh(dh_late, b - early, n).start()

        @pl.when(b + 1 < batch)
        def _():
            for copy in load_grads(b + 1):
                copy.start()

        for n in (width - 2 * tile, width - tile):
            store_dh(dh_late, 0, n).wait()

    fetch(0)
    for copy in load_w + load_grads(0):
        copy.start()
    load_x(0).start()

    @pl.loop(0, units + 3)
    def _(t):
        @pl.when(jnp.logical_and(t >= 1, t < units + 1))
        def _():
            combine(t - 1)

        @pl.when(jnp.logical_and(t >= 2, t < units + 2))
        def _():
            relay(t - 2)

        @pl.when(t >= 3)
        def _():
            finish(t - 3)

        @pl.when(t + 1 < units)
        def _():
            fetch(t + 1)

        @pl.when(t == 2)
        def _():
            for copy in load_w:
                copy.wait()

        @pl.when(jnp.logical_and(t >= 2, t < batch + 2))
        def _():
            grad_part(t - 2)

    for way in range(2):
        for u in (units - 2, units - 1):
            far(u, way).wait_send()
        for u in (units - 3, units - 2, units - 1):
            near(u, way).wait_send()
    for u in (units - 2, units - 1):
        for r in range(chips):
            pair(o_part.at[0], u, r).wait_send()
    store_y(0).wait()


def project_and_scatter(o_part, grad_q, grad_kv, w_q, w_kv, x_loc, b_o, early, ring):
    batch, rows, width = x_loc.shape
    seq, q_width = grad_q.shape[1:]
    qkv_width = q_width + w_kv.shape[1]
    chips = ring // 2
    part = lambda n: jax.ShapeDtypeStruct((n, seq, width), BF16)
    hbm = pl.BlockSpec(memory_space=pl.ANY)
    vmem = pl.BlockSpec(memory_space=pltpu.VMEM)
    dma = pltpu.SemaphoreType.DMA
    return pl.pallas_call(
        scatter_kernel,
        name="project_and_scatter",
        out_shape=(jax.ShapeDtypeStruct(x_loc.shape, BF16), part(early), part(batch - early), jax.ShapeDtypeStruct((early, rows, width), BF16)),
        in_specs=[hbm] * 6 + [vmem],
        out_specs=(hbm,) * 4,
        scratch_shapes=[
            pltpu.VMEM((seq, qkv_width), BF16), pltpu.VMEM((width, qkv_width), BF16), pltpu.VMEM((2, chips, rows, width), BF16),
            pltpu.VMEM((2, seq, 512), BF16), pltpu.VMEM((2, chips, rows, width), BF16),
            pltpu.VMEM((2, rows, width), BF16), pltpu.VMEM((3, 2, rows, width), BF16), pltpu.VMEM((3, rows, width), F32),
            pltpu.VMEM((3, rows, width), BF16), pltpu.VMEM((3, 2, rows, width), BF16), pltpu.VMEM((rows, width), BF16), pltpu.VMEM((rows, width), BF16),
            dma((2, chips)), dma((2, chips)), dma((2, chips)), dma((2, 2)), dma((3, 2)), dma((3, 2)), dma((3, 2)), pltpu.SemaphoreType.REGULAR,
            dma((4,)), dma((2,)), dma((2,))],
        compiler_params=pltpu.CompilerParams(collective_id=1, has_side_effects=True, vmem_limit_bytes=VMEM_LIMIT),
        cost_estimate=pl.CostEstimate(flops=4 * batch * seq * width * q_width, bytes_accessed=6 * batch * seq * width, transcendentals=0),
    )(o_part, grad_q, grad_kv, w_q, w_kv, x_loc, b_o)


def norm_backward_kernel(dh, x, dy, ln_stats, gamma, *refs):
    dx, sums = refs[-2:]
    rows, width = x.shape[1:]
    tile = 512

    @pl.when(pl.program_id(0) == 0)
    def _():
        sums[...] = jnp.zeros_like(sums)

    mean, inv_std = ln_stats[0, 0, :, :1], ln_stats[1, 0, :, :1]
    by_lane = lambda v: sum(v[:, n : n + 128] for n in range(0, tile, 128))
    by_sublane = lambda v: jnp.sum(v.reshape(-1, 8, tile), axis=0)
    plain = along = jnp.zeros((rows, 128), F32)
    for n in range(0, width, tile):
        at = slice(n, n + tile)
        grad_h = dh[0, :, at].astype(F32)
        x_hat = (x[0, :, at].astype(F32) - mean) * inv_std
        both = grad_h * x_hat
        plain = plain + by_lane(grad_h * gamma[:, at])
        along = along + by_lane(both * gamma[:, at])
        sums[0, :, at] += by_sublane(both)
        sums[1, :, at] += by_sublane(grad_h)
    plain = jnp.sum(plain, axis=-1, keepdims=True) / width
    along = jnp.sum(along, axis=-1, keepdims=True) / width
    for n in range(0, width, tile):
        at = slice(n, n + tile)
        x_hat = (x[0, :, at].astype(F32) - mean) * inv_std
        grad_in = inv_std * (dh[0, :, at].astype(F32) * gamma[:, at] - plain - x_hat * along)
        dx[0, :, at] = (dy[0, :, at].astype(F32) + grad_in).astype(BF16)


def norm_backward(grad_h, x_loc, dy_loc, ln_stats, gamma, first, started):
    rows, width = x_loc.shape[1:]
    count = grad_h.shape[0]
    block = lambda skip: pl.BlockSpec((1, rows, width), lambda b: (b + skip, 0, 0))
    still = lambda shape: pl.BlockSpec(shape, lambda b: (0,) * len(shape))
    extra = [] if started is None else [started]
    return pl.pallas_call(
        norm_backward_kernel,
        name="norm_backward",
        grid=(count,),
        out_shape=(jax.ShapeDtypeStruct(x_loc.shape, BF16), jax.ShapeDtypeStruct((2, 8, width), F32)),
        in_specs=[block(0), block(first), block(first), pl.BlockSpec((2, 1, rows, 128), lambda b: (0, b + first, 0, 0)), still(gamma.shape)]
        + [pl.BlockSpec(memory_space=pl.ANY)] * len(extra),
        out_specs=(block(first), still((2, 8, width))),
        input_output_aliases={5: 0} if extra else {},
        compiler_params=pltpu.CompilerParams(vmem_limit_bytes=VMEM_LIMIT),
        cost_estimate=pl.CostEstimate(flops=60 * count * rows * width, bytes_accessed=8 * count * rows * width, transcendentals=0),
    )(grad_h, x_loc, dy_loc, ln_stats, gamma, *extra)


def settle(values):
    block = pl.BlockSpec((1,) + values.shape[1:], lambda b: (b, 0, 0))

    def body(src, dst):
        dst[...] = src[...]

    return pl.pallas_call(
        body, name="settle", grid=(values.shape[0],), out_shape=jax.ShapeDtypeStruct(values.shape, values.dtype), in_specs=[block], out_specs=block,
        cost_estimate=pl.CostEstimate(flops=values.size * 100, bytes_accessed=values.size * 4, transcendentals=0))(values)


def sum_kernel(ring, parts, out, gathered, send, recv):
    me = lax.axis_index("tp")
    barrier = pltpu.get_barrier_semaphore()
    others = [lax.rem(me + k, ring) for k in range(1, ring)]
    for other in others:
        pl.semaphore_signal(barrier, inc=1, device_id={"tp": other}, device_id_type=pl.DeviceIdType.MESH)
    pl.semaphore_wait(barrier, ring - 1)

    def copy(k):
        return pltpu.make_async_remote_copy(
            src_ref=parts, dst_ref=gathered.at[me], send_sem=send.at[k], recv_sem=recv.at[k],
            device_id={"tp": lax.rem(me + k, ring)}, device_id_type=pl.DeviceIdType.MESH)

    for k in range(1, ring):
        copy(k).start()
    gathered[me] = parts[...]
    for k in range(1, ring):
        copy(k).wait_recv()
    total = gathered[0]
    for k in range(1, ring):
        total = total + gathered[k]
    out[...] = total
    for k in range(1, ring):
        copy(k).wait_send()


def sum_over_ring(parts, ring):
    vmem = pl.BlockSpec(memory_space=pltpu.VMEM)
    return pl.pallas_call(
        functools.partial(sum_kernel, ring),
        name="sum_over_ring",
        out_shape=jax.ShapeDtypeStruct(parts.shape, F32),
        in_specs=[vmem],
        out_specs=vmem,
        scratch_shapes=[pltpu.VMEM((ring,) + parts.shape, F32), pltpu.SemaphoreType.DMA((ring,)), pltpu.SemaphoreType.DMA((ring,))],
        compiler_params=pltpu.CompilerParams(collective_id=2, has_side_effects=True),
    )(parts)


def solution(mesh):
    ring = mesh.shape["tp"]

    def device_block(x_loc, ln_gamma, ln_beta, w_q, b_q, w_kv, b_kv, w_o, b_o, dy_loc):
        head_dim = w_kv.shape[1] // 2
        batch, _, width = x_loc.shape
        normed_full, dy_full, merged, o_part, grad_q, kv_part, kv_twin, bo_rows, ln_stats = gather_and_attend(
            x_loc, dy_loc, ln_gamma[None, :], ln_beta[None, :], w_q, w_kv, b_q[None, :], b_kv[None, :], w_o, ring, head_dim)
        early = 3 * batch // 8
        grad_kv = lax.psum(kv_twin, "tp")
        y_loc, _, dh_part, dh_early = project_and_scatter(o_part, grad_q, kv_part, w_q, w_kv, x_loc, b_o[None, :], early, ring)
        dh_late = lax.psum_scatter(dh_part, "tp", scatter_dimension=1, tiled=True)

        grad_q, merged, y_loc, bo_rows = lax.optimization_barrier((grad_q, merged, y_loc, bo_rows))
        y_loc = settle(y_loc)
        grad_bo = jnp.sum(bo_rows, axis=0)
        grad_wo = jnp.einsum("bse,bsd->ed", merged, dy_full, preferred_element_type=jnp.float32)
        grad_wq = jnp.einsum("bsd,bse->de", normed_full, grad_q, preferred_element_type=jnp.float32)
        grad_bq = jnp.sum(grad_q, axis=(0, 1), dtype=jnp.float32)
        grad_wkv = jnp.einsum("bsd,bsc->dc", normed_full, grad_kv, preferred_element_type=jnp.float32)
        grad_bkv = jnp.sum(grad_kv, axis=(0, 1), dtype=jnp.float32)
        gamma = ln_gamma[None, :]
        started, parts_early = norm_backward(dh_early, x_loc, dy_loc, ln_stats, gamma, 0, None)
        grad_x, parts_late = norm_backward(dh_late, x_loc, dy_loc, ln_stats, gamma, early, started)
        sums = sum_over_ring(jnp.sum(parts_early + parts_late, axis=1).reshape(-1, 128), ring).reshape(2, width)
        return (y_loc, grad_x, sums[0], sums[1], grad_wq, grad_bq, grad_wkv, grad_bkv, grad_wo, grad_bo)

    return jax.shard_map(
        device_block,
        mesh=mesh,
        in_specs=(P("dp", "tp", None), P(None), P(None), P(None, "tp"), P("tp"), P(None, None), P(None), P("tp", None), P(None), P("dp", "tp", None)),
        out_specs=(P("dp", "tp", None), P("dp", "tp", None), P("dp"), P("dp"), P("dp", "tp"), P(("dp", "tp")), P("dp", None), P("dp"), P(("dp", "tp"), None), P("dp")),
        check_vma=False,
    )
```

```python
import functools

import jax
import jax.numpy as jnp
from jax import lax
from jax.experimental import pallas as pl
from jax.experimental.pallas import tpu as pltpu
from jax.sharding import PartitionSpec as P

LN_EPS = 1e-5
VMEM_LIMIT = 64 * 1024 * 1024 - 65536
BF16 = jnp.bfloat16
F32 = jnp.float32

RIGHT, LEFT, PART, FAR_R, FAR_L, PASS_L, PASS_R, PASS_F = range(8)


def stack_heads(rows, dst, first, heads, dim):
    for h in range(heads):
        dst[h * dim : (h + 1) * dim, :] = rows[first : first + dim, h * dim : (h + 1) * dim]


def scaled_scores(scores_s, lanes, first, dim):
    scores = scores_s[: first + dim, lanes] * dim**-0.5
    keys = lax.broadcasted_iota(jnp.int32, scores.shape, 0)
    queries = lax.broadcasted_iota(jnp.int32, scores.shape, 1) + first
    return jnp.where(keys <= queries, scores, -1e30)


ACROSS = (((1,), (1,)), ((), ()))
DOWN = (((0,), (0,)), ((), ()))


def attend(qkv, out, stats, scores_s, probs_s, q_s, heads, dim):
    rows = qkv.shape[0]
    width = heads * dim
    for first in range(0, rows, dim):
        last = first + dim
        stack_heads(qkv, q_s, first, heads, dim)
        scores_s[:last, :] = lax.dot_general(qkv[:last, width : width + dim], q_s[...], ACROSS, preferred_element_type=F32)

        @pl.loop(0, heads, unroll=2)
        def _(h):
            lanes = pl.ds(pl.multiple_of(h * dim, dim), dim)
            scores = scaled_scores(scores_s, lanes, first, dim)
            top = jnp.max(scores, axis=0, keepdims=True)
            weights = jnp.exp(scores - top)
            share = 1.0 / jnp.sum(weights, axis=0, keepdims=True)
            probs_s[:last, lanes] = (weights * share).astype(BF16)
            stats[h, 0:1, first:last] = top
            stats[h, 1:2, first:last] = share

        turned = lax.dot_general(qkv[:last, width + dim :], probs_s[:last, :], DOWN, preferred_element_type=F32)
        for h in range(heads):
            out[first:last, h * dim : (h + 1) * dim] = turned[:, h * dim : (h + 1) * dim].T.astype(BF16)


def attend_backward(qkv, grad_att, grad_q, grad_kv, stats, scores_s, grad_p_s, probs_s, grad_s_s, q_s, att_s, heads, dim):
    rows = qkv.shape[0]
    width = heads * dim
    grad_kv[...] = jnp.zeros_like(grad_kv)
    for first in range(0, rows, dim):
        last = first + dim
        stack_heads(qkv, q_s, first, heads, dim)
        stack_heads(grad_att, att_s, first, heads, dim)
        scores_s[:last, :] = lax.dot_general(qkv[:last, width : width + dim], q_s[...], ACROSS, preferred_element_type=F32)
        grad_p_s[:last, :] = lax.dot_general(qkv[:last, width + dim :], att_s[...], ACROSS, preferred_element_type=F32)

        @pl.loop(0, heads, unroll=2)
        def _(h):
            lanes = pl.ds(pl.multiple_of(h * dim, dim), dim)
            scores = scaled_scores(scores_s, lanes, first, dim)
            probs = jnp.exp(scores - stats[h, 0:1, first:last]) * stats[h, 1:2, first:last]
            grad_p = grad_p_s[:last, lanes].astype(BF16).astype(F32)
            row_dot = jnp.sum(probs * grad_p, axis=0, keepdims=True)
            grad_s_s[:last, lanes] = (probs * (grad_p - row_dot) * dim**-0.5).astype(BF16)
            probs_s[:last, lanes] = probs.astype(BF16)

        turned = lax.dot_general(qkv[:last, width : width + dim], grad_s_s[:last, :], DOWN, preferred_element_type=F32)
        for h in range(heads):
            grad_q[first:last, h * dim : (h + 1) * dim] = turned[:, h * dim : (h + 1) * dim].T.astype(BF16)
        grad_kv[:last, :dim] += jnp.dot(grad_s_s[:last, :], q_s[...], preferred_element_type=F32)
        grad_kv[:last, dim:] += jnp.dot(probs_s[:last, :], att_s[...], preferred_element_type=F32)


def block_kernel(heads, dim, x_hbm, dy_hbm, gamma, beta, wq_hbm, wkv_hbm, b_q, b_kv, wo_hbm, b_o,
                 h_full, dy_full, att_out, o_part, dq_out, dkv_part, dkv_full, y_out, dh_early, dh_late, dh_sum, dbo, ln_stats,
                 own, w_buf, wo_buf, h_buf, qkv_buf, att_buf, da_buf, dq_buf, dkv_buf, part_buf, total, stats,
                 scores_s, grad_p_s, probs_s, grad_s_s, q_s, att_s, theirs, far_in, near_in, kv_theirs, kv_far_in, kv_near_in,
                 send, recv, x_sem, dy_sem, keep_sem, w_sem, h_sem, att_sem, dq_sem, dkv_sem, part_sem, load_sem,
                 ours_sem, pair_send, pair_recv, far_send, far_recv, near_send, near_recv, free,
                 kv_ours_sem, kv_pair_send, kv_pair_recv, kv_far_send, kv_far_recv, kv_near_send, kv_near_recv, kv_send, kv_recv, kv_keep_sem):
    batch, rows, width = x_hbm.shape
    early = dh_early.shape[0]
    half = rows // 2
    wide = width // 2
    units = 2 * batch
    scatters = batch + early
    ring = h_full.shape[1] // rows
    chips = ring // 2
    q_width = heads * dim
    kv_width = 2 * dim
    tile = 512
    me = lax.axis_index("tp")
    partner = me + 1 - 2 * lax.rem(me, 2)
    right, left, far_chip = lax.rem(me + 2, ring), lax.rem(me + ring - 2, ring), lax.rem(me + ring // 2, ring)
    OURS, NEAR, SUM, FAR, X, Y = 0, 4, 10, 13, units, units + 1

    barrier = pltpu.get_barrier_semaphore()
    for other in (left, right, partner):
        pl.semaphore_signal(barrier, inc=1, device_id={"tp": other}, device_id_type=pl.DeviceIdType.MESH)
    pl.semaphore_wait(barrier, 3)

    def remote(src, dst, sems, to):
        return pltpu.make_async_remote_copy(
            src_ref=src, dst_ref=dst, send_sem=sems[0], recv_sem=sems[1], device_id={"tp": to}, device_id_type=pl.DeviceIdType.MESH)

    def columns(low, high, act, step=tile):
        @pl.loop(low, high, step=step)
        def _(n):
            act(pl.ds(pl.multiple_of(n, step), step))

    def block(full, b, owner, first=0, count=rows):
        return full.at[b, pl.ds(pl.multiple_of(owner * rows + first, half), count)]

    def move(kind, full, b, u):
        if kind in (RIGHT, LEFT, PART):
            src, dst = own.at[u], block(full, b, me)
        elif kind in (FAR_R, FAR_L):
            src = dst = block(full, b, left, 0, half) if kind == FAR_R else block(full, b, right, half, half)
        else:
            src = dst = block(full, b, {PASS_L: left, PASS_R: right, PASS_F: far_chip}[kind])
        to = {RIGHT: right, FAR_R: right, LEFT: left, FAR_L: left}.get(kind, partner)
        return remote(src, dst, (send.at[kind, u], recv.at[kind, u]), to)

    def keep(full, b, u):
        return pltpu.make_async_copy(own.at[u], block(full, b, me), keep_sem.at[u])

    def load_x(b):
        return pltpu.make_async_copy(x_hbm.at[b], own.at[units + lax.rem(b, 2)], x_sem.at[lax.rem(b, 2)])

    def load_dy(b):
        return pltpu.make_async_copy(dy_hbm.at[b], own.at[2 * b + 1], dy_sem.at[b])

    def turn(u, h_act, dy_act):
        b = lax.div(u, 2)
        inside = jnp.logical_and(u >= 0, u < units)

        @pl.when(jnp.logical_and(inside, lax.rem(u, 2) == 0))
        def _():
            h_act(b)

        @pl.when(jnp.logical_and(inside, lax.rem(u, 2) == 1))
        def _():
            dy_act(b)

    def unit(u, act):
        turn(u, lambda b: act(h_full, b, u), lambda b: act(dy_full, b, u))

    def normalise(b):
        load_x(b).wait()
        slot = units + lax.rem(b, 2)

        @pl.loop(0, rows, step=16)
        def _(r):
            at = pl.ds(pl.multiple_of(r, 16), 16)
            x_wide = own[slot, at, :].astype(F32)
            mean = jnp.mean(x_wide, axis=-1, keepdims=True)
            centred = x_wide - mean
            inv_std = lax.rsqrt(jnp.mean(centred * centred, axis=-1, keepdims=True) + LN_EPS)
            own[2 * b, at, :] = (centred * inv_std * gamma[...] + beta[...]).astype(BF16)
            ln_stats[0, b, at, :] = jnp.broadcast_to(mean, (16, 128))
            ln_stats[1, b, at, :] = jnp.broadcast_to(inv_std, (16, 128))

        @pl.when(b + 2 < batch)
        def _():
            load_x(b + 2).start()

    def launch(u):
        turn(u, normalise, lambda b: load_dy(b).wait())

        def act(full, b, u):
            for kind in (RIGHT, LEFT, PART):
                move(kind, full, b, u).start()
            keep(full, b, u).start()

        unit(u, act)

    def forward(full, b, u):
        move(RIGHT, full, b, u).wait_recv()
        move(FAR_R, full, b, u).start()
        move(LEFT, full, b, u).wait_recv()
        move(FAR_L, full, b, u).start()

    def share(full, b, u):
        move(PASS_L, full, b, u).start()
        move(PASS_R, full, b, u).start()

    def share_far(full, b, u):
        move(FAR_R, full, b, u).wait_recv()
        move(FAR_L, full, b, u).wait_recv()
        move(PASS_F, full, b, u).start()

    def complete(full, b, u):
        for kind in (PART, PASS_L, PASS_R, PASS_F):
            move(kind, full, b, u).wait_recv()
        keep(full, b, u).wait()

    def retire(full, b, u):
        for kind in range(8):
            move(kind, full, b, u).wait_send()

    def load_block(full, b):
        load = pltpu.make_async_copy(full.at[b], h_buf, h_sem.at[0])
        load.start()
        load.wait()

    def project(b):
        load_block(h_full, b)

        def act(at):
            qkv_buf[:, at] = (jnp.dot(h_buf[...], w_buf[:, at], preferred_element_type=F32) + b_q[:, at]).astype(BF16)

        columns(0, q_width, act, 256)
        at = pl.ds(q_width, kv_width)
        qkv_buf[:, at] = (jnp.dot(h_buf[...], w_buf[:, at], preferred_element_type=F32) + b_kv[...]).astype(BF16)

    def store_att(b):
        return pltpu.make_async_copy(att_buf, att_out.at[b], att_sem.at[0])

    def store_part(out, b, n):
        at = pl.ds(pl.multiple_of(n, tile), tile)
        slot = lax.rem(lax.div(n, tile), 2)
        return pltpu.make_async_copy(part_buf.at[slot], out.at[b, :, at], part_sem.at[slot])

    def make_part(product, store):
        @pl.loop(0, width, step=tile)
        def _(n):
            @pl.when(n >= 2 * tile)
            def _():
                store_part(o_part, 0, n - 2 * tile).wait()

            part_buf[lax.rem(lax.div(n, tile), 2)] = product(pl.ds(pl.multiple_of(n, tile), tile)).astype(BF16)
            store(n)

        for n in (width - 2 * tile, width - tile):
            store_part(o_part, 0, n).wait()

    def attend_and_project(b):
        @pl.when(b > 0)
        def _():
            store_att(b - 1).wait()

        attend(qkv_buf, att_buf, stats, scores_s, probs_s, q_s, heads, dim)
        store_att(b).start()
        make_part(lambda at: jnp.dot(att_buf[...], wo_buf[:, at], preferred_element_type=F32), lambda n: store_part(o_part, b, n).start())

    def grad_attended(b):
        load_block(dy_full, b)

        def act(at):
            da_buf[:, at] = lax.dot_general(h_buf[...], wo_buf[at, :], ACROSS, preferred_element_type=F32).astype(BF16)

        columns(0, q_width, act, 256)

        def add(at):
            dbo[:, at] += jnp.sum(h_buf[:, at].astype(F32).reshape(-1, 8, tile), axis=0)

        columns(0, width, add)

    def store_dq(b):
        return pltpu.make_async_copy(dq_buf, dq_out.at[b], dq_sem.at[0])

    def store_dkv(b, owner):
        return pltpu.make_async_copy(dkv_buf.at[pl.ds(owner * rows, rows)], dkv_part.at[owner, pl.ds(pl.multiple_of(b * rows, rows), rows)], dkv_sem.at[owner])

    def stored(b):
        store_dq(b).wait()
        for owner in range(ring):
            store_dkv(b, owner).wait()

    def differentiate(b):
        @pl.when(b > 0)
        def _():
            stored(b - 1)

        attend_backward(qkv_buf, da_buf, dq_buf, total, stats, scores_s, grad_p_s, probs_s, grad_s_s, q_s, att_s, heads, dim)
        dkv_buf[...] = total[...].astype(BF16)
        store_dq(b).start()
        for owner in range(ring):
            store_dkv(b, owner).start()

    def grad_part(b):
        copies = [pltpu.make_async_copy(dq_out.at[b], qkv_buf.at[:, pl.ds(0, q_width)], load_sem.at[ring])]
        for owner in range(ring):
            copies.append(pltpu.make_async_copy(dkv_part.at[owner, pl.ds(pl.multiple_of(b * rows, rows), rows)],
                                                qkv_buf.at[pl.ds(owner * rows, rows), pl.ds(q_width, kv_width)], load_sem.at[owner]))
        for copy in copies:
            copy.start()
        for copy in copies:
            copy.wait()

        def store(n):
            @pl.when(b < early)
            def _():
                store_part(dh_early, b, n).start()

            @pl.when(b >= early)
            def _():
                store_part(dh_late, b - early, n).start()

        make_part(lambda at: lax.dot_general(qkv_buf[...], w_buf[at, :], ACROSS, preferred_element_type=F32), store)

    def line(owner):
        return pl.ds(pl.multiple_of(owner * rows, rows), rows)

    def sourced(u, act):
        @pl.when(u < batch)
        def _():
            act(o_part.at[u])

        @pl.when(u >= batch)
        def _():
            act(dh_early.at[u - batch])

    def mine(part, r):
        return pltpu.make_async_copy(part.at[line(lax.rem(me + 2 * r, ring))], own.at[OURS + r], ours_sem.at[r])

    def pair(part, r):
        return remote(part.at[line(lax.rem(partner + 2 * r, ring))], theirs.at[r], (pair_send.at[r], pair_recv.at[r]), partner)

    def far(u, way):
        cols = pl.ds(way * wide, wide)
        return remote(own.at[FAR + lax.rem(u, 2), :, cols], far_in.at[lax.rem(u, 3), :, cols],
                      (far_send.at[lax.rem(u, 2), way], far_recv.at[lax.rem(u, 3), way]), (right, left)[way])

    def near(u, way):
        slot = lax.rem(u, 3)
        return remote(own.at[NEAR + 2 * slot + way], near_in.at[slot, way], (near_send.at[slot, way], near_recv.at[slot, way]), (right, left)[way])

    def fetch(u):
        @pl.when(u >= 1)
        def _():
            pl.semaphore_wait(free, 1)
            for r in range(chips):
                pair(o_part.at[0], r).wait_send()

        def act(part):
            for r in range(chips):
                pair(part, r).start()
            for r in range(chips):
                mine(part, r).start()

        sourced(u, act)

    def combine(u):
        slot2, slot3 = lax.rem(u, 2), lax.rem(u, 3)
        for r in range(chips):
            mine(o_part.at[0], r).wait()
            pair(o_part.at[0], r).wait_recv()

        @pl.when(u >= 2)
        def _():
            for way in range(2):
                far(u - 2, way).wait_send()

        @pl.when(u >= 3)
        def _():
            for way in range(2):
                near(u - 3, way).wait_send()

        def chip_sum(r, at):
            return (own[OURS + r, :, at].astype(F32) + theirs[r, :, at].astype(F32)).astype(BF16)

        def act_far(at):
            own[FAR + slot2, :, at] = chip_sum(chips // 2, at)

        columns(0, width, act_far)
        for way in range(2):
            far(u, way).start()

        def act(at):
            own[NEAR + 2 * slot3, :, at] = chip_sum(1, at)
            own[NEAR + 2 * slot3 + 1, :, at] = chip_sum(chips - 1, at)
            own[SUM + slot3, :, at] = chip_sum(0, at)

        columns(0, width, act)

        @pl.when(u + 1 < scatters)
        def _():
            pl.semaphore_signal(free, inc=1, device_id={"tp": partner}, device_id_type=pl.DeviceIdType.MESH)

    def relay(u):
        slot = lax.rem(u, 3)
        for way in range(2):
            far(u, way).wait_recv()
        for way in range(2):
            def act(at):
                place = NEAR + 2 * slot + way
                own[place, :, at] = (own[place, :, at].astype(F32) + far_in[slot, :, at].astype(F32)).astype(BF16)

            columns(way * wide, way * wide + wide, act)
        for way in range(2):
            near(u, way).start()

    def scatter_x(u):
        return pltpu.make_async_copy(x_hbm.at[u], own.at[X], load_sem.at[ring + 1])

    def store_y(out, b):
        return pltpu.make_async_copy(own.at[Y], out.at[b], load_sem.at[ring + 2])

    def finish(u):
        slot = lax.rem(u, 3)
        for way in range(2):
            near(u, way).wait_recv()

        @pl.when(u > 0)
        def _():
            store_y(y_out, 0).wait()

        def whole(at):
            return own[SUM + slot, :, at].astype(F32) + near_in[slot, 0, :, at].astype(F32) + near_in[slot, 1, :, at].astype(F32)

        @pl.when(u < batch)
        def _():
            scatter_x(u).wait()

            def act(at):
                own[Y, :, at] = (own[X, :, at].astype(F32) + whole(at) + b_o[:, at]).astype(BF16)

            columns(0, width, act)
            store_y(y_out, u).start()

        @pl.when(u >= batch)
        def _():
            def act(at):
                own[Y, :, at] = whole(at).astype(BF16)

            columns(0, width, act)
            store_y(dh_sum, u - batch).start()

        @pl.when(u + 1 < batch)
        def _():
            scatter_x(u + 1).start()

    pick = lambda ref, n: ref.at[:, pl.ds(n * kv_width, kv_width)]
    kv_ours = [pick(probs_s, 0), pick(probs_s, 1), pick(probs_s, 2), pick(grad_s_s, 0)]
    kv_far, kv_sum = pick(grad_s_s, 1), pick(da_buf, 2)
    kv_near = [pick(da_buf, 0), pick(da_buf, 1)]
    kv_rows = batch * rows
    kv_half = kv_rows // 2

    def kv_mine(r):
        return pltpu.make_async_copy(dkv_part.at[lax.rem(me + 2 * r, ring)], kv_ours[r], kv_ours_sem.at[r])

    def kv_pair(r):
        return remote(dkv_part.at[lax.rem(partner + 2 * r, ring)], kv_theirs.at[r], (kv_pair_send.at[r], kv_pair_recv.at[r]), partner)

    def kv_far_copy(way):
        at = pl.ds(way * kv_half, kv_half)
        return remote(kv_far.at[at], kv_far_in.at[at], (kv_far_send.at[way], kv_far_recv.at[way]), (right, left)[way])

    def kv_near_copy(way):
        return remote(kv_near[way], kv_near_in.at[way], (kv_near_send.at[way], kv_near_recv.at[way]), (right, left)[way])

    def kv_move(kind):
        if kind in (RIGHT, LEFT, PART):
            src, dst = kv_sum, dkv_full.at[me]
        elif kind in (FAR_R, FAR_L):
            src = dst = dkv_full.at[left, pl.ds(0, kv_half)] if kind == FAR_R else dkv_full.at[right, pl.ds(kv_half, kv_half)]
        else:
            src = dst = dkv_full.at[{PASS_L: left, PASS_R: right, PASS_F: far_chip}[kind]]
        to = {RIGHT: right, FAR_R: right, LEFT: left, FAR_L: left}.get(kind, partner)
        return remote(src, dst, (kv_send.at[kind], kv_recv.at[kind]), to)

    def kv_keep():
        return pltpu.make_async_copy(kv_sum, dkv_full.at[me], kv_keep_sem.at[0])

    def kv_steps():
        def start():
            stored(batch - 1)
            for r in range(chips):
                kv_pair(r).start()
                kv_mine(r).start()

        def sum_chip():
            for r in range(chips):
                kv_mine(r).wait()
                kv_pair(r).wait_recv()
            chip = lambda r: (kv_ours[r][...].astype(F32) + kv_theirs[r].astype(F32)).astype(BF16)
            kv_far[...] = chip(chips // 2)
            for way in range(2):
                kv_far_copy(way).start()
            kv_near[0][...] = chip(1)
            kv_near[1][...] = chip(chips - 1)

        def relay_far():
            for way in range(2):
                kv_far_copy(way).wait_recv()
            for way in range(2):
                at = slice(way * kv_half, way * kv_half + kv_half)
                kv_near[way][at, :] = (kv_near[way][at, :].astype(F32) + kv_far_in[at, :].astype(F32)).astype(BF16)
            for way in range(2):
                kv_near_copy(way).start()

        def sum_all():
            for way in range(2):
                kv_near_copy(way).wait_recv()
            chip = kv_ours[0][...].astype(F32) + kv_theirs[0].astype(F32)
            kv_sum[...] = (chip + kv_near_in[0].astype(F32) + kv_near_in[1].astype(F32)).astype(BF16)
            for kind in (RIGHT, LEFT, PART):
                kv_move(kind).start()
            kv_keep().start()

        def spread():
            kv_move(RIGHT).wait_recv()
            kv_move(FAR_R).start()
            kv_move(LEFT).wait_recv()
            kv_move(FAR_L).start()
            kv_move(PASS_L).start()
            kv_move(PASS_R).start()

        def spread_far():
            kv_move(FAR_R).wait_recv()
            kv_move(FAR_L).wait_recv()
            kv_move(PASS_F).start()

        def settle_kv():
            for kind in (PART, PASS_L, PASS_R, PASS_F):
                kv_move(kind).wait_recv()
            kv_keep().wait()
            for kind in range(8):
                kv_move(kind).wait_send()
            for way in range(2):
                kv_far_copy(way).wait_send()
                kv_near_copy(way).wait_send()
            for r in range(chips):
                kv_pair(r).wait_send()

        return start, sum_chip, relay_far, sum_all, spread, spread_far, settle_kv

    load_x(0).start()
    load_dy(0).start()
    load_x(1).start()
    weights = (pltpu.make_async_copy(wq_hbm, w_buf.at[:, pl.ds(0, q_width)], w_sem.at[0]),
               pltpu.make_async_copy(wkv_hbm, w_buf.at[:, pl.ds(q_width, kv_width)], w_sem.at[1]),
               pltpu.make_async_copy(wo_hbm, wo_buf, w_sem.at[2]))
    launch(0)
    launch(1)
    for copy in weights:
        copy.start()
    for b in range(1, batch):
        load_dy(b).start()
    dbo[...] = jnp.zeros_like(dbo)
    for copy in weights:
        copy.wait()

    lead = units - 2

    @pl.loop(0, lead + scatters + 3)
    def _(s):
        t = s - lead
        when = lambda low, high: pl.when(jnp.logical_and(t >= low, t < high))

        @pl.when(s < units)
        def _():
            unit(s, forward)

        launch(s + 2)

        @pl.when(s < units)
        def _():
            unit(s, share)

        unit(s - 2, retire)

        @when(1, scatters + 1)
        def _():
            combine(t - 1)

        @when(2, scatters + 2)
        def _():
            relay(t - 2)

        turn(s - 2, attend_and_project, differentiate)
        unit(s - 1, share_far)
        unit(s - 1, complete)
        turn(s - 1, project, grad_attended)

        @when(3, scatters + 3)
        def _():
            finish(t - 3)

        @when(0, scatters)
        def _():
            fetch(t)

        @when(2, 3)
        def _():
            scatter_x(0).start()

        for n, act in enumerate(kv_steps()):
            @when(4 + n, 5 + n)
            def _():
                act()

        @when(4, 4 + batch)
        def _():
            grad_part(t - 4)

    store_att(batch - 1).wait()
    store_y(y_out, 0).wait()
    for r in range(chips):
        pair(o_part.at[0], r).wait_send()
    for way in range(2):
        for u in (scatters - 2, scatters - 1):
            far(u, way).wait_send()
        for u in (scatters - 3, scatters - 2, scatters - 1):
            near(u, way).wait_send()


def attention_block(x_loc, dy_loc, gamma, beta, w_q, w_kv, b_q, b_kv, w_o, b_o, early, ring, dim):
    batch, rows, width = x_loc.shape
    q_width, kv_width = w_q.shape[1], w_kv.shape[1]
    qkv_width = q_width + kv_width
    seq = rows * ring
    units = 2 * batch
    chips = ring // 2
    heads = q_width // dim
    hbm = pl.BlockSpec(memory_space=pl.ANY)
    vmem = pl.BlockSpec(memory_space=pltpu.VMEM)
    dma = pltpu.SemaphoreType.DMA
    full = lambda n, w: jax.ShapeDtypeStruct((n, seq, w), BF16)
    at_home = lambda n: jax.ShapeDtypeStruct((n, rows, width), BF16)
    owned = jax.ShapeDtypeStruct((ring, batch * rows, kv_width), BF16)
    lo, hi = (lambda *shape: pltpu.VMEM(shape, BF16)), (lambda *shape: pltpu.VMEM(shape, F32))
    return pl.pallas_call(
        functools.partial(block_kernel, heads, dim),
        name="attention_block",
        out_shape=(full(batch, width), full(batch, width), full(batch, q_width), full(batch, width), full(batch, q_width), owned, owned, at_home(batch),
                   full(early, width), full(batch - early, width), at_home(early),
                   jax.ShapeDtypeStruct((8, width), F32), jax.ShapeDtypeStruct((2, batch, rows, 128), F32)),
        in_specs=[hbm, hbm, vmem, vmem, hbm, hbm, vmem, vmem, hbm, vmem],
        out_specs=(hbm,) * 11 + (vmem, vmem),
        scratch_shapes=[
            lo(units + 2, rows, width), lo(width, qkv_width), lo(q_width, width), lo(seq, width), lo(seq, qkv_width), lo(seq, q_width), lo(seq, q_width),
            lo(seq, q_width), lo(seq, kv_width), lo(2, seq, 512), hi(seq, kv_width), hi(heads, 8, seq),
            hi(seq, q_width), hi(seq, q_width), lo(seq, q_width), lo(seq, q_width), lo(q_width, dim), lo(q_width, dim),
            lo(chips, rows, width), lo(3, rows, width), lo(3, 2, rows, width),
            lo(chips, batch * rows, kv_width), lo(batch * rows, kv_width), lo(2, batch * rows, kv_width),
            dma((8, units)), dma((8, units)), dma((2,)), dma((batch,)), dma((units,)), dma((3,)), dma((1,)), dma((1,)), dma((1,)), dma((ring,)), dma((2,)),
            dma((ring + 3,)),
            dma((chips,)), dma((chips,)), dma((chips,)), dma((2, 2)), dma((3, 2)), dma((3, 2)), dma((3, 2)), pltpu.SemaphoreType.REGULAR,
            dma((chips,)), dma((chips,)), dma((chips,)), dma((2,)), dma((2,)), dma((2,)), dma((2,)), dma((8,)), dma((8,)), dma((1,))],
        compiler_params=pltpu.CompilerParams(collective_id=0, has_side_effects=True, vmem_limit_bytes=VMEM_LIMIT),
        cost_estimate=pl.CostEstimate(flops=8 * batch * seq * width * qkv_width, bytes_accessed=12 * batch * seq * width, transcendentals=0),
    )(x_loc, dy_loc, gamma, beta, w_q, w_kv, b_q, b_kv, w_o, b_o)


def norm_backward_kernel(dh, x, dy, ln_stats, gamma, *refs):
    dx, sums = refs[-2:]
    rows, width = x.shape[1:]
    tile = 512

    @pl.when(pl.program_id(0) == 0)
    def _():
        sums[...] = jnp.zeros_like(sums)

    mean, inv_std = ln_stats[0, 0, :, :1], ln_stats[1, 0, :, :1]
    by_lane = lambda v: sum(v[:, n : n + 128] for n in range(0, tile, 128))
    by_sublane = lambda v: jnp.sum(v.reshape(-1, 8, tile), axis=0)
    plain = along = jnp.zeros((rows, 128), F32)
    for n in range(0, width, tile):
        at = slice(n, n + tile)
        grad_h = dh[0, :, at].astype(F32)
        x_hat = (x[0, :, at].astype(F32) - mean) * inv_std
        both = grad_h * x_hat
        plain = plain + by_lane(grad_h * gamma[:, at])
        along = along + by_lane(both * gamma[:, at])
        sums[0, :, at] += by_sublane(both)
        sums[1, :, at] += by_sublane(grad_h)
    plain = jnp.sum(plain, axis=-1, keepdims=True) / width
    along = jnp.sum(along, axis=-1, keepdims=True) / width
    for n in range(0, width, tile):
        at = slice(n, n + tile)
        x_hat = (x[0, :, at].astype(F32) - mean) * inv_std
        grad_in = inv_std * (dh[0, :, at].astype(F32) * gamma[:, at] - plain - x_hat * along)
        dx[0, :, at] = (dy[0, :, at].astype(F32) + grad_in).astype(BF16)


def norm_backward(grad_h, x_loc, dy_loc, ln_stats, gamma, first, started):
    rows, width = x_loc.shape[1:]
    count = grad_h.shape[0]
    block = lambda skip: pl.BlockSpec((1, rows, width), lambda b: (b + skip, 0, 0))
    still = lambda shape: pl.BlockSpec(shape, lambda b: (0,) * len(shape))
    extra = [] if started is None else [started]
    return pl.pallas_call(
        norm_backward_kernel,
        name="norm_backward",
        grid=(count,),
        out_shape=(jax.ShapeDtypeStruct(x_loc.shape, BF16), jax.ShapeDtypeStruct((2, 8, width), F32)),
        in_specs=[block(0), block(first), block(first), pl.BlockSpec((2, 1, rows, 128), lambda b: (0, b + first, 0, 0)), still(gamma.shape)]
        + [pl.BlockSpec(memory_space=pl.ANY)] * len(extra),
        out_specs=(block(first), still((2, 8, width))),
        input_output_aliases={5: 0} if extra else {},
        compiler_params=pltpu.CompilerParams(vmem_limit_bytes=VMEM_LIMIT),
        cost_estimate=pl.CostEstimate(flops=60 * count * rows * width, bytes_accessed=8 * count * rows * width, transcendentals=0),
    )(grad_h, x_loc, dy_loc, ln_stats, gamma, *extra)


def settle(values):
    block = pl.BlockSpec((1,) + values.shape[1:], lambda b: (b, 0, 0))

    def body(src, dst):
        dst[...] = src[...]

    return pl.pallas_call(
        body, name="settle", grid=(values.shape[0],), out_shape=jax.ShapeDtypeStruct(values.shape, values.dtype), in_specs=[block], out_specs=block,
        cost_estimate=pl.CostEstimate(flops=values.size * 100, bytes_accessed=values.size * 4, transcendentals=0))(values)


def sum_kernel(ring, parts, out, gathered, send, recv):
    me = lax.axis_index("tp")
    barrier = pltpu.get_barrier_semaphore()
    others = [lax.rem(me + k, ring) for k in range(1, ring)]
    for other in others:
        pl.semaphore_signal(barrier, inc=1, device_id={"tp": other}, device_id_type=pl.DeviceIdType.MESH)
    pl.semaphore_wait(barrier, ring - 1)

    def copy(k):
        return pltpu.make_async_remote_copy(
            src_ref=parts, dst_ref=gathered.at[me], send_sem=send.at[k], recv_sem=recv.at[k],
            device_id={"tp": lax.rem(me + k, ring)}, device_id_type=pl.DeviceIdType.MESH)

    for k in range(1, ring):
        copy(k).start()
    gathered[me] = parts[...]
    for k in range(1, ring):
        copy(k).wait_recv()
    total = gathered[0]
    for k in range(1, ring):
        total = total + gathered[k]
    out[...] = total
    for k in range(1, ring):
        copy(k).wait_send()


def sum_over_ring(parts, ring):
    vmem = pl.BlockSpec(memory_space=pltpu.VMEM)
    return pl.pallas_call(
        functools.partial(sum_kernel, ring),
        name="sum_over_ring",
        out_shape=jax.ShapeDtypeStruct(parts.shape, F32),
        in_specs=[vmem],
        out_specs=vmem,
        scratch_shapes=[pltpu.VMEM((ring,) + parts.shape, F32), pltpu.SemaphoreType.DMA((ring,)), pltpu.SemaphoreType.DMA((ring,))],
        compiler_params=pltpu.CompilerParams(collective_id=2, has_side_effects=True),
    )(parts)


def solution(mesh):
    ring = mesh.shape["tp"]

    def device_block(x_loc, ln_gamma, ln_beta, w_q, b_q, w_kv, b_kv, w_o, b_o, dy_loc):
        head_dim = w_kv.shape[1] // 2
        batch, own_rows, width = x_loc.shape
        early = 3 * batch // 8
        normed_full, dy_full, merged, _, grad_q, _, kv_owned, y_loc, _, dh_part, dh_early, bo_rows, ln_stats = attention_block(
            x_loc, dy_loc, ln_gamma[None, :], ln_beta[None, :], w_q, w_kv, b_q[None, :], b_kv[None, :], w_o, b_o[None, :], early, ring, head_dim)
        dh_late = lax.psum_scatter(dh_part, "tp", scatter_dimension=1, tiled=True)
        kv_owned = kv_owned.reshape(ring, batch, own_rows, 2 * head_dim)
        grad_kv = jnp.moveaxis(kv_owned, 0, 1).reshape(batch, ring * own_rows, 2 * head_dim)

        grad_q, merged, y_loc, bo_rows = lax.optimization_barrier((grad_q, merged, y_loc, bo_rows))
        y_loc = settle(y_loc)
        grad_bo = jnp.sum(bo_rows, axis=0)
        grad_wo = jnp.einsum("bse,bsd->ed", merged, dy_full, preferred_element_type=jnp.float32)
        grad_wq = jnp.einsum("bsd,bse->de", normed_full, grad_q, preferred_element_type=jnp.float32)
        grad_bq = jnp.sum(grad_q, axis=(0, 1), dtype=jnp.float32)
        grad_wkv = jnp.einsum("bsd,bsc->dc", normed_full, grad_kv, preferred_element_type=jnp.float32)
        grad_bkv = jnp.sum(grad_kv, axis=(0, 1), dtype=jnp.float32)
        gamma = ln_gamma[None, :]
        started, parts_early = norm_backward(dh_early, x_loc, dy_loc, ln_stats, gamma, 0, None)
        grad_x, parts_late = norm_backward(dh_late, x_loc, dy_loc, ln_stats, gamma, early, started)
        sums = sum_over_ring(jnp.sum(parts_early + parts_late, axis=1).reshape(-1, 128), ring).reshape(2, width)
        return (y_loc, grad_x, sums[0], sums[1], grad_wq, grad_bq, grad_wkv, grad_bkv, grad_wo, grad_bo)

    return jax.shard_map(
        device_block,
        mesh=mesh,
        in_specs=(P("dp", "tp", None), P(None), P(None), P(None, "tp"), P("tp"), P(None, None), P(None), P("tp", None), P(None), P("dp", "tp", None)),
        out_specs=(P("dp", "tp", None), P("dp", "tp", None), P("dp"), P("dp"), P("dp", "tp"), P(("dp", "tp")), P("dp", None), P("dp"), P(("dp", "tp"), None), P("dp")),
        check_vma=False,
    )
```

```python
import functools

import jax
import jax.numpy as jnp
from jax import lax
from jax.experimental import pallas as pl
from jax.experimental.pallas import tpu as pltpu
from jax.sharding import PartitionSpec as P

LN_EPS = 1e-5
VMEM_LIMIT = 64 * 1024 * 1024 - 65536
BF16 = jnp.bfloat16
F32 = jnp.float32

RIGHT, LEFT, PART, FAR_R, FAR_L, PASS_L, PASS_R, PASS_F = range(8)


def stack_heads(rows, dst, first, heads, dim):
    for h in range(heads):
        dst[h * dim : (h + 1) * dim, :] = rows[first : first + dim, h * dim : (h + 1) * dim]


def scaled_scores(scores_s, lanes, first, dim):
    scores = scores_s[: first + dim, lanes] * dim**-0.5
    keys = lax.broadcasted_iota(jnp.int32, scores.shape, 0)
    queries = lax.broadcasted_iota(jnp.int32, scores.shape, 1) + first
    return jnp.where(keys <= queries, scores, -1e30)


ACROSS = (((1,), (1,)), ((), ()))
DOWN = (((0,), (0,)), ((), ()))


def attend(qkv, out, stats, scores_s, probs_s, q_s, heads, dim):
    rows = qkv.shape[0]
    width = heads * dim
    for first in range(0, rows, dim):
        last = first + dim
        stack_heads(qkv, q_s, first, heads, dim)
        scores_s[:last, :] = lax.dot_general(qkv[:last, width : width + dim], q_s[...], ACROSS, preferred_element_type=F32)

        @pl.loop(0, heads, unroll=2)
        def _(h):
            lanes = pl.ds(pl.multiple_of(h * dim, dim), dim)
            scores = scaled_scores(scores_s, lanes, first, dim)
            top = jnp.max(scores, axis=0, keepdims=True)
            weights = jnp.exp(scores - top)
            share = 1.0 / jnp.sum(weights, axis=0, keepdims=True)
            probs_s[:last, lanes] = (weights * share).astype(BF16)
            stats[h, 0:1, first:last] = top
            stats[h, 1:2, first:last] = share

        turned = lax.dot_general(qkv[:last, width + dim :], probs_s[:last, :], DOWN, preferred_element_type=F32)
        for h in range(heads):
            out[first:last, h * dim : (h + 1) * dim] = turned[:, h * dim : (h + 1) * dim].T.astype(BF16)


def attend_backward(qkv, grad_att, grad_q, grad_kv, stats, scores_s, grad_p_s, probs_s, grad_s_s, q_s, att_s, heads, dim):
    rows = qkv.shape[0]
    width = heads * dim
    grad_kv[...] = jnp.zeros_like(grad_kv)
    for first in range(0, rows, dim):
        last = first + dim
        stack_heads(qkv, q_s, first, heads, dim)
        stack_heads(grad_att, att_s, first, heads, dim)
        scores_s[:last, :] = lax.dot_general(qkv[:last, width : width + dim], q_s[...], ACROSS, preferred_element_type=F32)
        grad_p_s[:last, :] = lax.dot_general(qkv[:last, width + dim :], att_s[...], ACROSS, preferred_element_type=F32)

        @pl.loop(0, heads, unroll=2)
        def _(h):
            lanes = pl.ds(pl.multiple_of(h * dim, dim), dim)
            scores = scaled_scores(scores_s, lanes, first, dim)
            probs = jnp.exp(scores - stats[h, 0:1, first:last]) * stats[h, 1:2, first:last]
            grad_p = grad_p_s[:last, lanes].astype(BF16).astype(F32)
            row_dot = jnp.sum(probs * grad_p, axis=0, keepdims=True)
            grad_s_s[:last, lanes] = (probs * (grad_p - row_dot) * dim**-0.5).astype(BF16)
            probs_s[:last, lanes] = probs.astype(BF16)

        turned = lax.dot_general(qkv[:last, width : width + dim], grad_s_s[:last, :], DOWN, preferred_element_type=F32)
        for h in range(heads):
            grad_q[first:last, h * dim : (h + 1) * dim] = turned[:, h * dim : (h + 1) * dim].T.astype(BF16)
        grad_kv[:last, :dim] += jnp.dot(grad_s_s[:last, :], q_s[...], preferred_element_type=F32)
        grad_kv[:last, dim:] += jnp.dot(probs_s[:last, :], att_s[...], preferred_element_type=F32)


def block_kernel(heads, dim, x_hbm, dy_hbm, gamma, beta, wq_hbm, wkv_hbm, b_q, b_kv, wo_hbm, b_o,
                 h_full, dy_full, att_out, o_part, dq_out, dkv_part, dkv_full, y_out, dh_early, dh_late, dh_theirs, dh_chip, dh_sum, dbo, dbq, ln_stats,
                 own, bias, w_buf, wo_buf, h_buf, qkv_buf, att_buf, da_buf, dq_buf, dkv_buf, part_buf, total, stats,
                 scores_s, grad_p_s, probs_s, grad_s_s, q_s, att_s, theirs, far_in, near_in, kv_theirs, kv_far_in, kv_near_in,
                 send, recv, x_sem, dy_sem, keep_sem, w_sem, h_sem, att_sem, dq_sem, dkv_sem, part_sem, load_sem,
                 ours_sem, pair_send, pair_recv, far_send, far_recv, near_send, near_recv, free,
                 kv_ours_sem, kv_pair_send, kv_pair_recv, kv_far_send, kv_far_recv, kv_near_send, kv_near_recv, kv_send, kv_recv, kv_keep_sem, late_send, late_recv, late_sem):
    batch, rows, width = x_hbm.shape
    early = dh_early.shape[0]
    half = rows // 2
    wide = width // 2
    units = 2 * batch
    scatters = batch + early
    ring = h_full.shape[1] // rows
    chips = ring // 2
    q_width = heads * dim
    kv_width = 2 * dim
    tile = 512
    me = lax.axis_index("tp")
    partner = me + 1 - 2 * lax.rem(me, 2)
    right, left, far_chip = lax.rem(me + 2, ring), lax.rem(me + ring - 2, ring), lax.rem(me + ring // 2, ring)
    OURS, NEAR, SUM, FAR, X, Y = 0, 4, 10, 13, units, units + 1

    barrier = pltpu.get_barrier_semaphore()
    for other in (left, right, partner):
        pl.semaphore_signal(barrier, inc=1, device_id={"tp": other}, device_id_type=pl.DeviceIdType.MESH)
    pl.semaphore_wait(barrier, 3)

    def remote(src, dst, sems, to):
        return pltpu.make_async_remote_copy(
            src_ref=src, dst_ref=dst, send_sem=sems[0], recv_sem=sems[1], device_id={"tp": to}, device_id_type=pl.DeviceIdType.MESH)

    def columns(low, high, act, step=tile):
        @pl.loop(low, high, step=step)
        def _(n):
            act(pl.ds(pl.multiple_of(n, step), step))

    def block(full, b, owner, first=0, count=rows):
        return full.at[b, pl.ds(pl.multiple_of(owner * rows + first, half), count)]

    def move(kind, full, b, u):
        if kind in (RIGHT, LEFT, PART):
            src, dst = own.at[u], block(full, b, me)
        elif kind in (FAR_R, FAR_L):
            src = dst = block(full, b, left, 0, half) if kind == FAR_R else block(full, b, right, half, half)
        else:
            src = dst = block(full, b, {PASS_L: left, PASS_R: right, PASS_F: far_chip}[kind])
        to = {RIGHT: right, FAR_R: right, LEFT: left, FAR_L: left}.get(kind, partner)
        return remote(src, dst, (send.at[kind, u], recv.at[kind, u]), to)

    def keep(full, b, u):
        return pltpu.make_async_copy(own.at[u], block(full, b, me), keep_sem.at[u])

    def load_x(b):
        return pltpu.make_async_copy(x_hbm.at[b], own.at[units + lax.rem(b, 2)], x_sem.at[lax.rem(b, 2)])

    def load_dy(b):
        return pltpu.make_async_copy(dy_hbm.at[b], own.at[2 * b + 1], dy_sem.at[b])

    def turn(u, h_act, dy_act):
        b = lax.div(u, 2)
        inside = jnp.logical_and(u >= 0, u < units)

        @pl.when(jnp.logical_and(inside, lax.rem(u, 2) == 0))
        def _():
            h_act(b)

        @pl.when(jnp.logical_and(inside, lax.rem(u, 2) == 1))
        def _():
            dy_act(b)

    def unit(u, act):
        turn(u, lambda b: act(h_full, b, u), lambda b: act(dy_full, b, u))

    def normalise(b):
        load_x(b).wait()
        slot = units + lax.rem(b, 2)

        @pl.loop(0, rows, step=16)
        def _(r):
            at = pl.ds(pl.multiple_of(r, 16), 16)
            x_wide = own[slot, at, :].astype(F32)
            mean = jnp.mean(x_wide, axis=-1, keepdims=True)
            centred = x_wide - mean
            inv_std = lax.rsqrt(jnp.mean(centred * centred, axis=-1, keepdims=True) + LN_EPS)
            own[2 * b, at, :] = (centred * inv_std * gamma[...] + beta[...]).astype(BF16)
            ln_stats[0, b, at, :] = jnp.broadcast_to(mean, (16, 128))
            ln_stats[1, b, at, :] = jnp.broadcast_to(inv_std, (16, 128))

        @pl.when(b + 2 < batch)
        def _():
            load_x(b + 2).start()

    def launch(u):
        turn(u, normalise, lambda b: load_dy(b).wait())

        def act(full, b, u):
            for kind in (RIGHT, LEFT, PART):
                move(kind, full, b, u).start()
            keep(full, b, u).start()

        unit(u, act)

    def forward(full, b, u):
        move(RIGHT, full, b, u).wait_recv()
        move(FAR_R, full, b, u).start()
        move(LEFT, full, b, u).wait_recv()
        move(FAR_L, full, b, u).start()

    def share(full, b, u):
        move(PASS_L, full, b, u).start()
        move(PASS_R, full, b, u).start()

    def share_far(full, b, u):
        move(FAR_R, full, b, u).wait_recv()
        move(FAR_L, full, b, u).wait_recv()
        move(PASS_F, full, b, u).start()

    def complete(full, b, u):
        for kind in (PART, PASS_L, PASS_R, PASS_F):
            move(kind, full, b, u).wait_recv()
        keep(full, b, u).wait()

    def retire(full, b, u):
        for kind in range(8):
            move(kind, full, b, u).wait_send()

    def load_block(full, b):
        load = pltpu.make_async_copy(full.at[b], h_buf, h_sem.at[0])
        load.start()
        load.wait()

    def project(b):
        load_block(h_full, b)

        def act(at):
            qkv_buf[:, at] = (jnp.dot(h_buf[...], w_buf[:, at], preferred_element_type=F32) + bias[:, at]).astype(BF16)

        columns(0, q_width + kv_width, act, 256)

    def store_att(b):
        return pltpu.make_async_copy(att_buf, att_out.at[b], att_sem.at[0])

    def store_part(out, b, n):
        at = pl.ds(pl.multiple_of(n, tile), tile)
        slot = lax.rem(lax.div(n, tile), 2)
        return pltpu.make_async_copy(part_buf.at[slot], out.at[b, :, at], part_sem.at[slot])

    def make_part(product, store):
        @pl.loop(0, width, step=tile)
        def _(n):
            @pl.when(n >= 2 * tile)
            def _():
                store_part(o_part, 0, n - 2 * tile).wait()

            part_buf[lax.rem(lax.div(n, tile), 2)] = product(pl.ds(pl.multiple_of(n, tile), tile)).astype(BF16)
            store(n)

        for n in (width - 2 * tile, width - tile):
            store_part(o_part, 0, n).wait()

    def attend_and_project(b):
        @pl.when(b > 0)
        def _():
            store_att(b - 1).wait()

        attend(qkv_buf, att_buf, stats, scores_s, probs_s, q_s, heads, dim)
        store_att(b).start()
        make_part(lambda at: jnp.dot(att_buf[...], wo_buf[:, at], preferred_element_type=F32), lambda n: store_part(o_part, b, n).start())

    def grad_attended(b):
        load_block(dy_full, b)

        def act(at):
            da_buf[:, at] = lax.dot_general(h_buf[...], wo_buf[at, :], ACROSS, preferred_element_type=F32).astype(BF16)

        columns(0, q_width, act, 256)

        def add(at):
            dbo[:, at] += jnp.sum(h_buf[:, at].astype(F32).reshape(-1, 8, tile), axis=0)

        columns(0, width, add)

    def store_dq(b):
        return pltpu.make_async_copy(dq_buf, dq_out.at[b], dq_sem.at[0])

    def store_dkv(b, owner):
        return pltpu.make_async_copy(dkv_buf.at[pl.ds(owner * rows, rows)], dkv_part.at[owner, pl.ds(pl.multiple_of(b * rows, rows), rows)], dkv_sem.at[owner])

    def stored(b):
        store_dq(b).wait()
        for owner in range(ring):
            store_dkv(b, owner).wait()

    def differentiate(b):
        @pl.when(b > 0)
        def _():
            stored(b - 1)

        attend_backward(qkv_buf, da_buf, dq_buf, total, stats, scores_s, grad_p_s, probs_s, grad_s_s, q_s, att_s, heads, dim)
        dkv_buf[...] = total[...].astype(BF16)

        def add(at):
            dbq[:, at] += jnp.sum(dq_buf[:, at].astype(F32).reshape(-1, 8, 256), axis=0)

        columns(0, q_width, add, 256)
        store_dq(b).start()
        for owner in range(ring):
            store_dkv(b, owner).start()

    def grad_part(b):
        copies = [pltpu.make_async_copy(dq_out.at[b], qkv_buf.at[:, pl.ds(0, q_width)], load_sem.at[ring])]
        for owner in range(ring):
            copies.append(pltpu.make_async_copy(dkv_part.at[owner, pl.ds(pl.multiple_of(b * rows, rows), rows)],
                                                qkv_buf.at[pl.ds(owner * rows, rows), pl.ds(q_width, kv_width)], load_sem.at[owner]))
        for copy in copies:
            copy.start()
        for copy in copies:
            copy.wait()

        def store(n):
            @pl.when(b < early)
            def _():
                store_part(dh_early, b, n).start()

            @pl.when(b >= early)
            def _():
                store_part(dh_late, b - early, n).start()

        make_part(lambda at: lax.dot_general(qkv_buf[...], w_buf[at, :], ACROSS, preferred_element_type=F32), store)

    def line(owner):
        return pl.ds(pl.multiple_of(owner * rows, rows), rows)

    def sourced(u, act):
        @pl.when(u < batch)
        def _():
            act(o_part.at[u])

        @pl.when(u >= batch)
        def _():
            act(dh_early.at[u - batch])

    def mine(part, r):
        return pltpu.make_async_copy(part.at[line(lax.rem(me + 2 * r, ring))], own.at[OURS + r], ours_sem.at[r])

    def pair(part, r):
        return remote(part.at[line(lax.rem(partner + 2 * r, ring))], theirs.at[r], (pair_send.at[r], pair_recv.at[r]), partner)

    def far(u, way):
        cols = pl.ds(way * wide, wide)
        return remote(own.at[FAR + lax.rem(u, 2), :, cols], far_in.at[lax.rem(u, 3), :, cols],
                      (far_send.at[lax.rem(u, 2), way], far_recv.at[lax.rem(u, 3), way]), (right, left)[way])

    def near(u, way):
        slot = lax.rem(u, 3)
        return remote(own.at[NEAR + 2 * slot + way], near_in.at[slot, way], (near_send.at[slot, way], near_recv.at[slot, way]), (right, left)[way])

    def fetch(u):
        @pl.when(u >= 1)
        def _():
            pl.semaphore_wait(free, 1)
            for r in range(chips):
                pair(o_part.at[0], r).wait_send()

        def act(part):
            for r in range(chips):
                pair(part, r).start()
            for r in range(chips):
                mine(part, r).start()

        sourced(u, act)

    def combine(u):
        slot2, slot3 = lax.rem(u, 2), lax.rem(u, 3)
        for r in range(chips):
            mine(o_part.at[0], r).wait()
            pair(o_part.at[0], r).wait_recv()

        @pl.when(u >= 2)
        def _():
            for way in range(2):
                far(u - 2, way).wait_send()

        @pl.when(u >= 3)
        def _():
            for way in range(2):
                near(u - 3, way).wait_send()

        def chip_sum(r, at):
            return (own[OURS + r, :, at].astype(F32) + theirs[r, :, at].astype(F32)).astype(BF16)

        def act_far(at):
            own[FAR + slot2, :, at] = chip_sum(chips // 2, at)

        columns(0, width, act_far)
        for way in range(2):
            far(u, way).start()

        def act(at):
            own[NEAR + 2 * slot3, :, at] = chip_sum(1, at)
            own[NEAR + 2 * slot3 + 1, :, at] = chip_sum(chips - 1, at)
            own[SUM + slot3, :, at] = chip_sum(0, at)

        columns(0, width, act)

        @pl.when(u + 1 < scatters)
        def _():
            pl.semaphore_signal(free, inc=1, device_id={"tp": partner}, device_id_type=pl.DeviceIdType.MESH)

    def relay(u):
        slot = lax.rem(u, 3)
        for way in range(2):
            far(u, way).wait_recv()
        for way in range(2):
            def act(at):
                place = NEAR + 2 * slot + way
                own[place, :, at] = (own[place, :, at].astype(F32) + far_in[slot, :, at].astype(F32)).astype(BF16)

            columns(way * wide, way * wide + wide, act)
        for way in range(2):
            near(u, way).start()

    def scatter_x(u):
        return pltpu.make_async_copy(x_hbm.at[u], own.at[X], load_sem.at[ring + 1])

    def store_y(out, b):
        return pltpu.make_async_copy(own.at[Y], out.at[b], load_sem.at[ring + 2])

    def finish(u):
        slot = lax.rem(u, 3)
        for way in range(2):
            near(u, way).wait_recv()

        @pl.when(u > 0)
        def _():
            store_y(y_out, 0).wait()

        def whole(at):
            return own[SUM + slot, :, at].astype(F32) + near_in[slot, 0, :, at].astype(F32) + near_in[slot, 1, :, at].astype(F32)

        @pl.when(u < batch)
        def _():
            scatter_x(u).wait()

            def act(at):
                own[Y, :, at] = (own[X, :, at].astype(F32) + whole(at) + b_o[:, at]).astype(BF16)

            columns(0, width, act)
            store_y(y_out, u).start()

        @pl.when(u >= batch)
        def _():
            def act(at):
                own[Y, :, at] = whole(at).astype(BF16)

            columns(0, width, act)
            store_y(dh_sum, u - batch).start()

        @pl.when(u + 1 < batch)
        def _():
            scatter_x(u + 1).start()

    core = lax.rem(me, 2)

    def late_pair(v, chip):
        return remote(dh_late.at[v, line(2 * chip + 1 - core)], dh_theirs.at[v, pl.ds(chip * rows, rows)], (late_send.at[v, chip], late_recv.at[v, chip]), partner)

    def late_loads(v):
        copies = [pltpu.make_async_copy(dh_late.at[v, line(2 * chip + core)], h_buf.at[pl.ds(chip * rows, rows)], late_sem.at[chip]) for chip in range(chips)]
        return copies + [pltpu.make_async_copy(dh_theirs.at[v], h_buf.at[pl.ds(chips * rows, chips * rows)], late_sem.at[chips])]

    def late_store(v):
        return pltpu.make_async_copy(h_buf.at[pl.ds(0, chips * rows)], dh_chip.at[v], late_sem.at[chips + 1])

    def late_sum(v):
        for chip in range(chips):
            late_pair(v, chip).wait_recv()

        @pl.when(v > 0)
        def _():
            late_store(v - 1).wait()

        for copy in late_loads(v):
            copy.start()
        for copy in late_loads(v):
            copy.wait()

        def act(at):
            mine_, theirs_ = h_buf[: chips * rows, at].astype(F32), h_buf[chips * rows :, at].astype(F32)
            h_buf[: chips * rows, at] = (mine_ + theirs_).astype(BF16)

        columns(0, width, act)
        late_store(v).start()

    pick = lambda ref, n: ref.at[:, pl.ds(n * kv_width, kv_width)]
    kv_ours = [pick(probs_s, 0), pick(probs_s, 1), pick(probs_s, 2), pick(grad_s_s, 0)]
    kv_far, kv_sum = pick(grad_s_s, 1), pick(da_buf, 2)
    kv_near = [pick(da_buf, 0), pick(da_buf, 1)]
    kv_rows = batch * rows
    kv_half = kv_rows // 2

    def kv_mine(r):
        return pltpu.make_async_copy(dkv_part.at[lax.rem(me + 2 * r, ring)], kv_ours[r], kv_ours_sem.at[r])

    def kv_pair(r):
        return remote(dkv_part.at[lax.rem(partner + 2 * r, ring)], kv_theirs.at[r], (kv_pair_send.at[r], kv_pair_recv.at[r]), partner)

    def kv_far_copy(way):
        at = pl.ds(way * kv_half, kv_half)
        return remote(kv_far.at[at], kv_far_in.at[at], (kv_far_send.at[way], kv_far_recv.at[way]), (right, left)[way])

    def kv_near_copy(way):
        return remote(kv_near[way], kv_near_in.at[way], (kv_near_send.at[way], kv_near_recv.at[way]), (right, left)[way])

    def kv_move(kind):
        if kind in (RIGHT, LEFT, PART):
            src, dst = kv_sum, dkv_full.at[me]
        elif kind in (FAR_R, FAR_L):
            src = dst = dkv_full.at[left, pl.ds(0, kv_half)] if kind == FAR_R else dkv_full.at[right, pl.ds(kv_half, kv_half)]
        else:
            src = dst = dkv_full.at[{PASS_L: left, PASS_R: right, PASS_F: far_chip}[kind]]
        to = {RIGHT: right, FAR_R: right, LEFT: left, FAR_L: left}.get(kind, partner)
        return remote(src, dst, (kv_send.at[kind], kv_recv.at[kind]), to)

    def kv_keep():
        return pltpu.make_async_copy(kv_sum, dkv_full.at[me], kv_keep_sem.at[0])

    def kv_steps():
        def start():
            stored(batch - 1)
            for r in range(chips):
                kv_pair(r).start()
                kv_mine(r).start()

        def sum_chip():
            for r in range(chips):
                kv_mine(r).wait()
                kv_pair(r).wait_recv()
            chip = lambda r: (kv_ours[r][...].astype(F32) + kv_theirs[r].astype(F32)).astype(BF16)
            kv_far[...] = chip(chips // 2)
            for way in range(2):
                kv_far_copy(way).start()
            kv_near[0][...] = chip(1)
            kv_near[1][...] = chip(chips - 1)

        def relay_far():
            for way in range(2):
                kv_far_copy(way).wait_recv()
            for way in range(2):
                at = slice(way * kv_half, way * kv_half + kv_half)
                kv_near[way][at, :] = (kv_near[way][at, :].astype(F32) + kv_far_in[at, :].astype(F32)).astype(BF16)
            for way in range(2):
                kv_near_copy(way).start()

        def sum_all():
            for way in range(2):
                kv_near_copy(way).wait_recv()
            chip = kv_ours[0][...].astype(F32) + kv_theirs[0].astype(F32)
            kv_sum[...] = (chip + kv_near_in[0].astype(F32) + kv_near_in[1].astype(F32)).astype(BF16)
            for kind in (RIGHT, LEFT, PART):
                kv_move(kind).start()
            kv_keep().start()

        def spread():
            kv_move(RIGHT).wait_recv()
            kv_move(FAR_R).start()
            kv_move(LEFT).wait_recv()
            kv_move(FAR_L).start()
            kv_move(PASS_L).start()
            kv_move(PASS_R).start()

        def spread_far():
            kv_move(FAR_R).wait_recv()
            kv_move(FAR_L).wait_recv()
            kv_move(PASS_F).start()

        def settle_kv():
            for kind in (PART, PASS_L, PASS_R, PASS_F):
                kv_move(kind).wait_recv()
            kv_keep().wait()
            for kind in range(8):
                kv_move(kind).wait_send()
            for way in range(2):
                kv_far_copy(way).wait_send()
                kv_near_copy(way).wait_send()
            for r in range(chips):
                kv_pair(r).wait_send()

        return start, sum_chip, relay_far, sum_all, spread, spread_far, settle_kv

    load_x(0).start()
    load_dy(0).start()
    load_x(1).start()
    weights = (pltpu.make_async_copy(wq_hbm, w_buf.at[:, pl.ds(0, q_width)], w_sem.at[0]),
               pltpu.make_async_copy(wkv_hbm, w_buf.at[:, pl.ds(q_width, kv_width)], w_sem.at[1]),
               pltpu.make_async_copy(wo_hbm, wo_buf, w_sem.at[2]))
    launch(0)
    launch(1)
    for copy in weights:
        copy.start()
    for b in range(1, batch):
        load_dy(b).start()
    dbo[...] = jnp.zeros_like(dbo)
    dbq[...] = jnp.zeros_like(dbq)
    bias[:, pl.ds(0, q_width)] = b_q[...].reshape(1, q_width)
    bias[:, pl.ds(q_width, kv_width)] = b_kv[...].reshape(1, kv_width)
    for copy in weights:
        copy.wait()

    lead = units - 2

    @pl.loop(0, lead + scatters + 3)
    def _(s):
        t = s - lead
        when = lambda low, high: pl.when(jnp.logical_and(t >= low, t < high))

        @pl.when(s < units)
        def _():
            unit(s, forward)

        launch(s + 2)

        @pl.when(s < units)
        def _():
            unit(s, share)

        unit(s - 2, retire)

        @when(1, scatters + 1)
        def _():
            combine(t - 1)

        @when(2, scatters + 2)
        def _():
            relay(t - 2)

        @when(0, scatters)
        def _():
            fetch(t)

        turn(s - 2, attend_and_project, differentiate)
        unit(s - 1, share_far)
        unit(s - 1, complete)
        turn(s - 1, project, grad_attended)

        @when(3, scatters + 3)
        def _():
            finish(t - 3)

        @when(2, 3)
        def _():
            scatter_x(0).start()

        for n, act in enumerate(kv_steps()):
            @when(4 + n, 5 + n)
            def _():
                act()

        @when(5 + early, 5 + batch)
        def _():
            late_sum(t - 5 - early)

        @when(4, 4 + batch)
        def _():
            grad_part(t - 4)

        @when(4 + early, 4 + batch)
        def _():
            for chip in range(chips):
                late_pair(t - 4 - early, chip).start()

    late_store(batch - early - 1).wait()
    for chip in range(chips):
        for v in range(batch - early):
            late_pair(v, chip).wait_send()
    store_att(batch - 1).wait()
    store_y(y_out, 0).wait()
    for r in range(chips):
        pair(o_part.at[0], r).wait_send()
    for way in range(2):
        for u in (scatters - 2, scatters - 1):
            far(u, way).wait_send()
        for u in (scatters - 3, scatters - 2, scatters - 1):
            near(u, way).wait_send()


def attention_block(x_loc, dy_loc, gamma, beta, w_q, w_kv, b_q, b_kv, w_o, b_o, early, ring, dim):
    batch, rows, width = x_loc.shape
    q_width, kv_width = w_q.shape[1], w_kv.shape[1]
    qkv_width = q_width + kv_width
    seq = rows * ring
    units = 2 * batch
    chips = ring // 2
    heads = q_width // dim
    hbm = pl.BlockSpec(memory_space=pl.ANY)
    vmem = pl.BlockSpec(memory_space=pltpu.VMEM)
    dma = pltpu.SemaphoreType.DMA
    full = lambda n, w: jax.ShapeDtypeStruct((n, seq, w), BF16)
    at_home = lambda n: jax.ShapeDtypeStruct((n, rows, width), BF16)
    half_seq = jax.ShapeDtypeStruct((batch - early, chips * rows, width), BF16)
    owned = jax.ShapeDtypeStruct((ring, batch * rows, kv_width), BF16)
    lo, hi = (lambda *shape: pltpu.VMEM(shape, BF16)), (lambda *shape: pltpu.VMEM(shape, F32))
    return pl.pallas_call(
        functools.partial(block_kernel, heads, dim),
        name="attention_block",
        out_shape=(full(batch, width), full(batch, width), full(batch, q_width), full(batch, width), full(batch, q_width), owned, owned, at_home(batch),
                   full(early, width), full(batch - early, width), half_seq, half_seq, at_home(early),
                   jax.ShapeDtypeStruct((8, width), F32), jax.ShapeDtypeStruct((8, q_width), F32), jax.ShapeDtypeStruct((2, batch, rows, 128), F32)),
        in_specs=[hbm, hbm, vmem, vmem, hbm, hbm, vmem, vmem, hbm, vmem],
        out_specs=(hbm,) * 13 + (vmem, vmem, vmem),
        scratch_shapes=[
            lo(units + 2, rows, width), hi(1, qkv_width), lo(width, qkv_width), lo(q_width, width), lo(seq, width), lo(seq, qkv_width), lo(seq, q_width), lo(seq, q_width),
            lo(seq, q_width), lo(seq, kv_width), lo(2, seq, 512), hi(seq, kv_width), hi(heads, 8, seq),
            hi(seq, q_width), hi(seq, q_width), lo(seq, q_width), lo(seq, q_width), lo(q_width, dim), lo(q_width, dim),
            lo(chips, rows, width), lo(3, rows, width), lo(3, 2, rows, width),
            lo(chips, batch * rows, kv_width), lo(batch * rows, kv_width), lo(2, batch * rows, kv_width),
            dma((8, units)), dma((8, units)), dma((2,)), dma((batch,)), dma((units,)), dma((3,)), dma((1,)), dma((1,)), dma((1,)), dma((ring,)), dma((2,)),
            dma((ring + 3,)),
            dma((chips,)), dma((chips,)), dma((chips,)), dma((2, 2)), dma((3, 2)), dma((3, 2)), dma((3, 2)), pltpu.SemaphoreType.REGULAR,
            dma((chips,)), dma((chips,)), dma((chips,)), dma((2,)), dma((2,)), dma((2,)), dma((2,)), dma((8,)), dma((8,)), dma((1,)),
            dma((batch - early, chips)), dma((batch - early, chips)), dma((chips + 2,))],
        compiler_params=pltpu.CompilerParams(collective_id=0, has_side_effects=True, vmem_limit_bytes=VMEM_LIMIT),
        cost_estimate=pl.CostEstimate(flops=8 * batch * seq * width * qkv_width, bytes_accessed=12 * batch * seq * width, transcendentals=0),
    )(x_loc, dy_loc, gamma, beta, w_q, w_kv, b_q, b_kv, w_o, b_o)


def norm_backward_kernel(dh, x, dy, ln_stats, gamma, *refs):
    dx, sums, x_hat_s, scaled_s = refs[-4:]
    rows, width = x.shape[1:]
    tile = 512

    @pl.when(pl.program_id(0) == 0)
    def _():
        sums[...] = jnp.zeros_like(sums)

    mean, inv_std = ln_stats[0, 0, :, :1], ln_stats[1, 0, :, :1]
    by_lane = lambda v: v[:, :128] + v[:, 128:256] + v[:, 256:384] + v[:, 384:]
    by_sublane = lambda v: jnp.sum(v.reshape(-1, 8, tile), axis=0)

    def gather_sums(n, carry):
        plain, along = carry
        at = pl.ds(pl.multiple_of(n * tile, tile), tile)
        grad_h = dh[0, :, at].astype(F32)
        x_hat = (x[0, :, at].astype(F32) - mean) * inv_std
        scaled = grad_h * gamma[:, at]
        x_hat_s[:, at] = x_hat
        scaled_s[:, at] = scaled
        sums[0, :, at] += by_sublane(grad_h * x_hat)
        sums[1, :, at] += by_sublane(grad_h)
        return plain + by_lane(scaled), along + by_lane(scaled * x_hat)

    zero = jnp.zeros((rows, 128), F32)
    plain, along = lax.fori_loop(0, width // tile, gather_sums, (zero, zero), unroll=2)
    plain = jnp.sum(plain, axis=-1, keepdims=True) / width
    along = jnp.sum(along, axis=-1, keepdims=True) / width

    @pl.loop(0, width // tile, unroll=2)
    def _(n):
        at = pl.ds(pl.multiple_of(n * tile, tile), tile)
        grad_in = inv_std * (scaled_s[:, at] - plain - x_hat_s[:, at] * along)
        dx[0, :, at] = (dy[0, :, at].astype(F32) + grad_in).astype(BF16)


def norm_backward(grad_h, x_loc, dy_loc, ln_stats, gamma, first, started):
    rows, width = x_loc.shape[1:]
    count = grad_h.shape[0]
    block = lambda skip: pl.BlockSpec((1, rows, width), lambda b: (b + skip, 0, 0))
    still = lambda shape: pl.BlockSpec(shape, lambda b: (0,) * len(shape))
    extra = [] if started is None else [started]
    return pl.pallas_call(
        norm_backward_kernel,
        name="norm_backward",
        grid=(count,),
        out_shape=(jax.ShapeDtypeStruct(x_loc.shape, BF16), jax.ShapeDtypeStruct((2, 8, width), F32)),
        in_specs=[block(0), block(first), block(first), pl.BlockSpec((2, 1, rows, 128), lambda b: (0, b + first, 0, 0)), still(gamma.shape)]
        + [pl.BlockSpec(memory_space=pl.ANY)] * len(extra),
        out_specs=(block(first), still((2, 8, width))),
        scratch_shapes=[pltpu.VMEM((rows, width), F32), pltpu.VMEM((rows, width), F32)],
        input_output_aliases={5: 0} if extra else {},
        compiler_params=pltpu.CompilerParams(vmem_limit_bytes=VMEM_LIMIT),
        cost_estimate=pl.CostEstimate(flops=60 * count * rows * width, bytes_accessed=8 * count * rows * width, transcendentals=0),
    )(grad_h, x_loc, dy_loc, ln_stats, gamma, *extra)


def settle(values):
    block = pl.BlockSpec((2,) + values.shape[1:], lambda b: (b, 0, 0))

    def body(src, dst):
        dst[...] = src[...]

    return pl.pallas_call(
        body, name="settle", grid=(values.shape[0] // 2,), out_shape=jax.ShapeDtypeStruct(values.shape, values.dtype), in_specs=[block], out_specs=block,
        compiler_params=pltpu.CompilerParams(vmem_limit_bytes=VMEM_LIMIT),
        cost_estimate=pl.CostEstimate(flops=values.size * 100, bytes_accessed=values.size * 4, transcendentals=0))(values)


def sum_kernel(ring, first, second, out, parts, gathered, send, recv):
    me = lax.axis_index("tp")
    barrier = pltpu.get_barrier_semaphore()
    others = [lax.rem(me + k, ring) for k in range(1, ring)]
    for other in others:
        pl.semaphore_signal(barrier, inc=1, device_id={"tp": other}, device_id_type=pl.DeviceIdType.MESH)
    groups = first.shape[2] // 128
    for kind in range(2):
        row = jnp.sum(first[kind] + second[kind], axis=0, keepdims=True)
        for n in range(groups):
            parts[kind * groups + n : kind * groups + n + 1, :] = row[:, n * 128 : (n + 1) * 128]
    pl.semaphore_wait(barrier, ring - 1)

    def copy(k):
        return pltpu.make_async_remote_copy(
            src_ref=parts, dst_ref=gathered.at[me], send_sem=send.at[k], recv_sem=recv.at[k],
            device_id={"tp": lax.rem(me + k, ring)}, device_id_type=pl.DeviceIdType.MESH)

    for k in range(1, ring):
        copy(k).start()
    gathered[me] = parts[...]
    for k in range(1, ring):
        copy(k).wait_recv()
    total = gathered[0]
    for k in range(1, ring):
        total = total + gathered[k]
    out[...] = total
    for k in range(1, ring):
        copy(k).wait_send()


def sum_over_ring(first, second, ring):
    vmem = pl.BlockSpec(memory_space=pltpu.VMEM)
    shape = (2 * first.shape[2] // 128, 128)
    return pl.pallas_call(
        functools.partial(sum_kernel, ring),
        name="sum_over_ring",
        out_shape=jax.ShapeDtypeStruct(shape, F32),
        in_specs=[vmem, vmem],
        out_specs=vmem,
        scratch_shapes=[pltpu.VMEM(shape, F32), pltpu.VMEM((ring,) + shape, F32), pltpu.SemaphoreType.DMA((ring,)), pltpu.SemaphoreType.DMA((ring,))],
        compiler_params=pltpu.CompilerParams(collective_id=2, has_side_effects=True),
    )(first, second)


def solution(mesh):
    ring = mesh.shape["tp"]

    def device_block(x_loc, ln_gamma, ln_beta, w_q, b_q, w_kv, b_kv, w_o, b_o, dy_loc):
        head_dim = w_kv.shape[1] // 2
        batch, own_rows, width = x_loc.shape
        early = 3 * batch // 8
        normed_full, dy_full, merged, _, grad_q, _, kv_owned, y_loc, _, _, _, dh_chip, dh_early, bo_rows, bq_rows, ln_stats = attention_block(
            x_loc, dy_loc, ln_gamma[None, :], ln_beta[None, :], w_q, w_kv, b_q, b_kv, w_o, b_o[None, :], early, ring, head_dim)
        lines = [[i for i in range(ring) if i % 2 == core] for core in range(2)]
        dh_late = lax.psum_scatter(dh_chip, "tp", scatter_dimension=1, tiled=True, axis_index_groups=lines)
        kv_owned = kv_owned.reshape(ring, batch, own_rows, 2 * head_dim)
        grad_kv = jnp.moveaxis(kv_owned, 0, 1).reshape(batch, ring * own_rows, 2 * head_dim)

        grad_q, merged, y_loc = lax.optimization_barrier((grad_q, merged, y_loc))
        y_loc = settle(y_loc)
        grad_bo = jnp.sum(bo_rows, axis=0)
        grad_wo = jnp.einsum("bse,bsd->ed", merged, dy_full, preferred_element_type=jnp.float32)
        grad_wq = jnp.einsum("bsd,bse->de", normed_full, grad_q, preferred_element_type=jnp.float32)
        grad_bq = jnp.sum(bq_rows, axis=0)
        grad_wkv = jnp.einsum("bsd,bsc->dc", normed_full, grad_kv, preferred_element_type=jnp.float32)
        grad_bkv = jnp.sum(grad_kv, axis=(0, 1), dtype=jnp.float32)
        gamma = ln_gamma[None, :]
        started, parts_early = norm_backward(dh_early, x_loc, dy_loc, ln_stats, gamma, 0, None)
        grad_x, parts_late = norm_backward(dh_late, x_loc, dy_loc, ln_stats, gamma, early, started)
        sums = sum_over_ring(parts_early, parts_late, ring).reshape(2, width)
        return (y_loc, grad_x, sums[0], sums[1], grad_wq, grad_bq, grad_wkv, grad_bkv, grad_wo, grad_bo)

    return jax.shard_map(
        device_block,
        mesh=mesh,
        in_specs=(P("dp", "tp", None), P(None), P(None), P(None, "tp"), P("tp"), P(None, None), P(None), P("tp", None), P(None), P("dp", "tp", None)),
        out_specs=(P("dp", "tp", None), P("dp", "tp", None), P("dp"), P("dp"), P("dp", "tp"), P(("dp", "tp")), P("dp", None), P("dp"), P(("dp", "tp"), None), P("dp")),
        check_vma=False,
    )
```

```python
import functools

import jax
import jax.numpy as jnp
from jax import lax
from jax.experimental import pallas as pl
from jax.experimental.pallas import tpu as pltpu
from jax.sharding import PartitionSpec as P

LN_EPS = 1e-5
VMEM_LIMIT = 64 * 1024 * 1024 - 65536
BF16 = jnp.bfloat16
F32 = jnp.float32

RIGHT, LEFT, PART, FAR_R, FAR_L, PASS_L, PASS_R, PASS_F = range(8)


def stack_heads(rows, dst, first, heads, dim):
    for h in range(heads):
        dst[h * dim : (h + 1) * dim, :] = rows[first : first + dim, h * dim : (h + 1) * dim]


def scaled_scores(scores_s, lanes, first, dim):
    scores = scores_s[: first + dim, lanes] * dim**-0.5
    keys = lax.broadcasted_iota(jnp.int32, scores.shape, 0)
    queries = lax.broadcasted_iota(jnp.int32, scores.shape, 1) + first
    return jnp.where(keys <= queries, scores, -1e30)


ACROSS = (((1,), (1,)), ((), ()))
DOWN = (((0,), (0,)), ((), ()))


def attend(qkv, out, stats, scores_s, probs_s, q_s, heads, dim):
    rows = qkv.shape[0]
    width = heads * dim
    for first in range(0, rows, dim):
        last = first + dim
        stack_heads(qkv, q_s, first, heads, dim)
        scores_s[:last, :] = lax.dot_general(qkv[:last, width : width + dim], q_s[...], ACROSS, preferred_element_type=F32)

        @pl.loop(0, heads, unroll=2)
        def _(h):
            lanes = pl.ds(pl.multiple_of(h * dim, dim), dim)
            scores = scaled_scores(scores_s, lanes, first, dim)
            top = jnp.max(scores, axis=0, keepdims=True)
            weights = jnp.exp(scores - top)
            share = 1.0 / jnp.sum(weights, axis=0, keepdims=True)
            probs_s[:last, lanes] = (weights * share).astype(BF16)
            stats[h, 0:1, first:last] = top
            stats[h, 1:2, first:last] = share

        turned = lax.dot_general(qkv[:last, width + dim :], probs_s[:last, :], DOWN, preferred_element_type=F32)
        for h in range(heads):
            out[first:last, h * dim : (h + 1) * dim] = turned[:, h * dim : (h + 1) * dim].T.astype(BF16)


def attend_backward(qkv, grad_att, grad_q, grad_kv, stats, scores_s, grad_p_s, probs_s, grad_s_s, q_s, att_s, heads, dim):
    rows = qkv.shape[0]
    width = heads * dim
    grad_kv[...] = jnp.zeros_like(grad_kv)
    for first in range(0, rows, dim):
        last = first + dim
        stack_heads(qkv, q_s, first, heads, dim)
        stack_heads(grad_att, att_s, first, heads, dim)
        scores_s[:last, :] = lax.dot_general(qkv[:last, width : width + dim], q_s[...], ACROSS, preferred_element_type=F32)
        grad_p_s[:last, :] = lax.dot_general(qkv[:last, width + dim :], att_s[...], ACROSS, preferred_element_type=F32)

        @pl.loop(0, heads, unroll=2)
        def _(h):
            lanes = pl.ds(pl.multiple_of(h * dim, dim), dim)
            scores = scaled_scores(scores_s, lanes, first, dim)
            probs = jnp.exp(scores - stats[h, 0:1, first:last]) * stats[h, 1:2, first:last]
            grad_p = grad_p_s[:last, lanes].astype(BF16).astype(F32)
            row_dot = jnp.sum(probs * grad_p, axis=0, keepdims=True)
            grad_s_s[:last, lanes] = (probs * (grad_p - row_dot) * dim**-0.5).astype(BF16)
            probs_s[:last, lanes] = probs.astype(BF16)

        turned = lax.dot_general(qkv[:last, width : width + dim], grad_s_s[:last, :], DOWN, preferred_element_type=F32)
        for h in range(heads):
            grad_q[first:last, h * dim : (h + 1) * dim] = turned[:, h * dim : (h + 1) * dim].T.astype(BF16)
        grad_kv[:last, :dim] += jnp.dot(grad_s_s[:last, :], q_s[...], preferred_element_type=F32)
        grad_kv[:last, dim:] += jnp.dot(probs_s[:last, :], att_s[...], preferred_element_type=F32)


def block_kernel(heads, dim, x_hbm, dy_hbm, gamma, beta, wq_hbm, wkv_hbm, b_q, b_kv, wo_hbm, b_o,
                 h_full, dy_full, att_out, o_part, dq_out, dkv_part, dkv_full, y_out, dh_part, o_theirs, o_chip, dh_sum, dbo, dbq, ln_stats,
                 own, bias, w_buf, wo_buf, h_buf, qkv_buf, att_buf, da_buf, dq_buf, dkv_buf, part_buf, total, stats,
                 scores_s, grad_p_s, probs_s, grad_s_s, q_s, att_s, theirs, far_in, near_in, kv_theirs, kv_far_in, kv_near_in,
                 send, recv, x_sem, dy_sem, keep_sem, w_sem, h_sem, att_sem, dq_sem, dkv_sem, part_sem, load_sem,
                 ours_sem, pair_send, pair_recv, far_send, far_recv, near_send, near_recv, free,
                 kv_ours_sem, kv_pair_send, kv_pair_recv, kv_far_send, kv_far_recv, kv_near_send, kv_near_recv, kv_send, kv_recv, kv_keep_sem, late_send, late_recv, late_sem):
    batch, rows, width = x_hbm.shape
    early = y_out.shape[0]
    half = rows // 2
    wide = width // 2
    units = 2 * batch
    scatters = batch + early
    ring = h_full.shape[1] // rows
    chips = ring // 2
    q_width = heads * dim
    kv_width = 2 * dim
    tile = 512
    me = lax.axis_index("tp")
    partner = me + 1 - 2 * lax.rem(me, 2)
    right, left, far_chip = lax.rem(me + 2, ring), lax.rem(me + ring - 2, ring), lax.rem(me + ring // 2, ring)
    OURS, NEAR, SUM, FAR, X, Y = 0, 4, 10, 13, units, units + 1

    barrier = pltpu.get_barrier_semaphore()
    for other in (left, right, partner):
        pl.semaphore_signal(barrier, inc=1, device_id={"tp": other}, device_id_type=pl.DeviceIdType.MESH)
    pl.semaphore_wait(barrier, 3)

    def remote(src, dst, sems, to):
        return pltpu.make_async_remote_copy(
            src_ref=src, dst_ref=dst, send_sem=sems[0], recv_sem=sems[1], device_id={"tp": to}, device_id_type=pl.DeviceIdType.MESH)

    def columns(low, high, act, step=tile):
        @pl.loop(low, high, step=step)
        def _(n):
            act(pl.ds(pl.multiple_of(n, step), step))

    def block(full, b, owner, first=0, count=rows):
        return full.at[b, pl.ds(pl.multiple_of(owner * rows + first, half), count)]

    def move(kind, full, b, u):
        if kind in (RIGHT, LEFT, PART):
            src, dst = own.at[u], block(full, b, me)
        elif kind in (FAR_R, FAR_L):
            src = dst = block(full, b, left, 0, half) if kind == FAR_R else block(full, b, right, half, half)
        else:
            src = dst = block(full, b, {PASS_L: left, PASS_R: right, PASS_F: far_chip}[kind])
        to = {RIGHT: right, FAR_R: right, LEFT: left, FAR_L: left}.get(kind, partner)
        return remote(src, dst, (send.at[kind, u], recv.at[kind, u]), to)

    def keep(full, b, u):
        return pltpu.make_async_copy(own.at[u], block(full, b, me), keep_sem.at[u])

    def load_x(b):
        return pltpu.make_async_copy(x_hbm.at[b], own.at[units + lax.rem(b, 2)], x_sem.at[lax.rem(b, 2)])

    def load_dy(b):
        return pltpu.make_async_copy(dy_hbm.at[b], own.at[2 * b + 1], dy_sem.at[b])

    def turn(u, h_act, dy_act):
        b = lax.div(u, 2)
        inside = jnp.logical_and(u >= 0, u < units)

        @pl.when(jnp.logical_and(inside, lax.rem(u, 2) == 0))
        def _():
            h_act(b)

        @pl.when(jnp.logical_and(inside, lax.rem(u, 2) == 1))
        def _():
            dy_act(b)

    def unit(u, act):
        turn(u, lambda b: act(h_full, b, u), lambda b: act(dy_full, b, u))

    def normalise(b):
        load_x(b).wait()
        slot = units + lax.rem(b, 2)

        @pl.loop(0, rows, step=16)
        def _(r):
            at = pl.ds(pl.multiple_of(r, 16), 16)
            x_wide = own[slot, at, :].astype(F32)
            mean = jnp.mean(x_wide, axis=-1, keepdims=True)
            centred = x_wide - mean
            inv_std = lax.rsqrt(jnp.mean(centred * centred, axis=-1, keepdims=True) + LN_EPS)
            own[2 * b, at, :] = (centred * inv_std * gamma[...] + beta[...]).astype(BF16)
            ln_stats[0, b, at, :] = jnp.broadcast_to(mean, (16, 128))
            ln_stats[1, b, at, :] = jnp.broadcast_to(inv_std, (16, 128))

        @pl.when(b + 2 < batch)
        def _():
            load_x(b + 2).start()

    def launch(u):
        turn(u, normalise, lambda b: load_dy(b).wait())

        def act(full, b, u):
            for kind in (RIGHT, LEFT, PART):
                move(kind, full, b, u).start()
            keep(full, b, u).start()

        unit(u, act)

    def forward(full, b, u):
        move(RIGHT, full, b, u).wait_recv()
        move(FAR_R, full, b, u).start()
        move(LEFT, full, b, u).wait_recv()
        move(FAR_L, full, b, u).start()

    def share(full, b, u):
        move(PASS_L, full, b, u).start()
        move(PASS_R, full, b, u).start()

    def share_far(full, b, u):
        move(FAR_R, full, b, u).wait_recv()
        move(FAR_L, full, b, u).wait_recv()
        move(PASS_F, full, b, u).start()

    def complete(full, b, u):
        for kind in (PART, PASS_L, PASS_R, PASS_F):
            move(kind, full, b, u).wait_recv()
        keep(full, b, u).wait()

    def retire(full, b, u):
        for kind in range(8):
            move(kind, full, b, u).wait_send()

    def load_block(full, b):
        load = pltpu.make_async_copy(full.at[b], h_buf, h_sem.at[0])
        load.start()
        load.wait()

    def project(b):
        load_block(h_full, b)

        def act(at):
            qkv_buf[:, at] = (jnp.dot(h_buf[...], w_buf[:, at], preferred_element_type=F32) + bias[:, at]).astype(BF16)

        columns(0, q_width + kv_width, act, 256)

    def store_att(b):
        return pltpu.make_async_copy(att_buf, att_out.at[b], att_sem.at[0])

    def store_part(out, b, n):
        at = pl.ds(pl.multiple_of(n, tile), tile)
        slot = lax.rem(lax.div(n, tile), 2)
        return pltpu.make_async_copy(part_buf.at[slot], out.at[b, :, at], part_sem.at[slot])

    def make_part(product, store):
        @pl.loop(0, width, step=tile)
        def _(n):
            @pl.when(n >= 2 * tile)
            def _():
                store_part(o_part, 0, n - 2 * tile).wait()

            part_buf[lax.rem(lax.div(n, tile), 2)] = product(pl.ds(pl.multiple_of(n, tile), tile)).astype(BF16)
            store(n)

        for n in (width - 2 * tile, width - tile):
            store_part(o_part, 0, n).wait()

    def attend_and_project(b):
        @pl.when(b > 0)
        def _():
            store_att(b - 1).wait()

        attend(qkv_buf, att_buf, stats, scores_s, probs_s, q_s, heads, dim)
        store_att(b).start()
        make_part(lambda at: jnp.dot(att_buf[...], wo_buf[:, at], preferred_element_type=F32), lambda n: store_part(o_part, b, n).start())

    def grad_attended(b):
        load_block(dy_full, b)

        def act(at):
            da_buf[:, at] = lax.dot_general(h_buf[...], wo_buf[at, :], ACROSS, preferred_element_type=F32).astype(BF16)

        columns(0, q_width, act, 256)

        def add(at):
            dbo[:, at] += jnp.sum(h_buf[:, at].astype(F32).reshape(-1, 8, tile), axis=0)

        columns(0, width, add)

    def store_dq(b):
        return pltpu.make_async_copy(dq_buf, dq_out.at[b], dq_sem.at[0])

    def store_dkv(b, owner):
        return pltpu.make_async_copy(dkv_buf.at[pl.ds(owner * rows, rows)], dkv_part.at[owner, pl.ds(pl.multiple_of(b * rows, rows), rows)], dkv_sem.at[owner])

    def stored(b):
        store_dq(b).wait()
        for owner in range(ring):
            store_dkv(b, owner).wait()

    def differentiate(b):
        @pl.when(b > 0)
        def _():
            stored(b - 1)

        attend_backward(qkv_buf, da_buf, dq_buf, total, stats, scores_s, grad_p_s, probs_s, grad_s_s, q_s, att_s, heads, dim)
        dkv_buf[...] = total[...].astype(BF16)

        def add(at):
            dbq[:, at] += jnp.sum(dq_buf[:, at].astype(F32).reshape(-1, 8, 256), axis=0)

        columns(0, q_width, add, 256)
        store_dq(b).start()
        for owner in range(ring):
            store_dkv(b, owner).start()

    def grad_part(b):
        def product(at):
            from_q = lax.dot_general(dq_buf[...], w_buf[at, :q_width], ACROSS, preferred_element_type=F32)
            return from_q + lax.dot_general(dkv_buf[...], w_buf[at, q_width:], ACROSS, preferred_element_type=F32)

        make_part(product, lambda n: store_part(dh_part, b, n).start())

    def line(owner):
        return pl.ds(pl.multiple_of(owner * rows, rows), rows)

    def sourced(u, act):
        @pl.when(u < early)
        def _():
            act(o_part.at[u])

        @pl.when(u >= early)
        def _():
            act(dh_part.at[u - early])

    def mine(part, r):
        return pltpu.make_async_copy(part.at[line(lax.rem(me + 2 * r, ring))], own.at[OURS + r], ours_sem.at[r])

    def pair(part, r):
        return remote(part.at[line(lax.rem(partner + 2 * r, ring))], theirs.at[r], (pair_send.at[r], pair_recv.at[r]), partner)

    def far(u, way):
        cols = pl.ds(way * wide, wide)
        return remote(own.at[FAR + lax.rem(u, 2), :, cols], far_in.at[lax.rem(u, 3), :, cols],
                      (far_send.at[lax.rem(u, 2), way], far_recv.at[lax.rem(u, 3), way]), (right, left)[way])

    def near(u, way):
        slot = lax.rem(u, 3)
        return remote(own.at[NEAR + 2 * slot + way], near_in.at[slot, way], (near_send.at[slot, way], near_recv.at[slot, way]), (right, left)[way])

    def fetch(u):
        @pl.when(u >= 1)
        def _():
            pl.semaphore_wait(free, 1)
            for r in range(chips):
                pair(o_part.at[0], r).wait_send()

        def act(part):
            for r in range(chips):
                pair(part, r).start()
            for r in range(chips):
                mine(part, r).start()

        sourced(u, act)

    def combine(u):
        slot2, slot3 = lax.rem(u, 2), lax.rem(u, 3)
        for r in range(chips):
            mine(o_part.at[0], r).wait()
            pair(o_part.at[0], r).wait_recv()

        @pl.when(u >= 2)
        def _():
            for way in range(2):
                far(u - 2, way).wait_send()

        @pl.when(u >= 3)
        def _():
            for way in range(2):
                near(u - 3, way).wait_send()

        def chip_sum(r, at):
            return (own[OURS + r, :, at].astype(F32) + theirs[r, :, at].astype(F32)).astype(BF16)

        def act_far(at):
            own[FAR + slot2, :, at] = chip_sum(chips // 2, at)

        columns(0, width, act_far)
        for way in range(2):
            far(u, way).start()

        def act(at):
            own[NEAR + 2 * slot3, :, at] = chip_sum(1, at)
            own[NEAR + 2 * slot3 + 1, :, at] = chip_sum(chips - 1, at)
            own[SUM + slot3, :, at] = chip_sum(0, at)

        columns(0, width, act)

        @pl.when(u + 1 < scatters)
        def _():
            pl.semaphore_signal(free, inc=1, device_id={"tp": partner}, device_id_type=pl.DeviceIdType.MESH)

    def relay(u):
        slot = lax.rem(u, 3)
        for way in range(2):
            far(u, way).wait_recv()
        for way in range(2):
            def act(at):
                place = NEAR + 2 * slot + way
                own[place, :, at] = (own[place, :, at].astype(F32) + far_in[slot, :, at].astype(F32)).astype(BF16)

            columns(way * wide, way * wide + wide, act)
        for way in range(2):
            near(u, way).start()

    def scatter_x(u):
        return pltpu.make_async_copy(x_hbm.at[u], own.at[X], load_sem.at[ring + 1])

    def store_y(out, b):
        return pltpu.make_async_copy(own.at[Y], out.at[b], load_sem.at[ring + 2])

    def finish(u):
        slot = lax.rem(u, 3)
        for way in range(2):
            near(u, way).wait_recv()

        @pl.when(u > 0)
        def _():
            store_y(y_out, 0).wait()

        def whole(at):
            return own[SUM + slot, :, at].astype(F32) + near_in[slot, 0, :, at].astype(F32) + near_in[slot, 1, :, at].astype(F32)

        @pl.when(u < early)
        def _():
            scatter_x(u).wait()

            def act(at):
                own[Y, :, at] = (own[X, :, at].astype(F32) + whole(at) + b_o[:, at]).astype(BF16)

            columns(0, width, act)
            store_y(y_out, u).start()

        @pl.when(u >= early)
        def _():
            def act(at):
                own[Y, :, at] = whole(at).astype(BF16)

            columns(0, width, act)
            store_y(dh_sum, u - early).start()

        @pl.when(u + 1 < early)
        def _():
            scatter_x(u + 1).start()

    core = lax.rem(me, 2)

    def late_pair(v, chip):
        return remote(o_part.at[early + v, line(2 * chip + 1 - core)], o_theirs.at[v, pl.ds(chip * rows, rows)], (late_send.at[v, chip], late_recv.at[v, chip]), partner)

    def late_loads(v):
        copies = [pltpu.make_async_copy(o_part.at[early + v, line(2 * chip + core)], h_buf.at[pl.ds(chip * rows, rows)], late_sem.at[chip]) for chip in range(chips)]
        return copies + [pltpu.make_async_copy(o_theirs.at[v], h_buf.at[pl.ds(chips * rows, chips * rows)], late_sem.at[chips])]

    def late_store(v):
        return pltpu.make_async_copy(h_buf.at[pl.ds(0, chips * rows)], o_chip.at[v], late_sem.at[chips + 1])

    def late_sum(v):
        for chip in range(chips):
            late_pair(v, chip).wait_recv()

        @pl.when(v > 0)
        def _():
            late_store(v - 1).wait()

        for copy in late_loads(v):
            copy.start()
        for copy in late_loads(v):
            copy.wait()

        def act(at):
            mine_, theirs_ = h_buf[: chips * rows, at].astype(F32), h_buf[chips * rows :, at].astype(F32)
            h_buf[: chips * rows, at] = (mine_ + theirs_).astype(BF16)

        columns(0, width, act)
        late_store(v).start()

    pick = lambda ref, n: ref.at[:, pl.ds(n * kv_width, kv_width)]
    kv_ours = [pick(probs_s, 0), pick(probs_s, 1), pick(probs_s, 2), pick(grad_s_s, 0)]
    kv_far, kv_sum = pick(grad_s_s, 1), pick(da_buf, 2)
    kv_near = [pick(da_buf, 0), pick(da_buf, 1)]
    kv_rows = batch * rows
    kv_half = kv_rows // 2

    def kv_mine(r):
        return pltpu.make_async_copy(dkv_part.at[lax.rem(me + 2 * r, ring)], kv_ours[r], kv_ours_sem.at[r])

    def kv_pair(r):
        return remote(dkv_part.at[lax.rem(partner + 2 * r, ring)], kv_theirs.at[r], (kv_pair_send.at[r], kv_pair_recv.at[r]), partner)

    def kv_far_copy(way):
        at = pl.ds(way * kv_half, kv_half)
        return remote(kv_far.at[at], kv_far_in.at[at], (kv_far_send.at[way], kv_far_recv.at[way]), (right, left)[way])

    def kv_near_copy(way):
        return remote(kv_near[way], kv_near_in.at[way], (kv_near_send.at[way], kv_near_recv.at[way]), (right, left)[way])

    def kv_move(kind):
        if kind in (RIGHT, LEFT, PART):
            src, dst = kv_sum, dkv_full.at[me]
        elif kind in (FAR_R, FAR_L):
            src = dst = dkv_full.at[left, pl.ds(0, kv_half)] if kind == FAR_R else dkv_full.at[right, pl.ds(kv_half, kv_half)]
        else:
            src = dst = dkv_full.at[{PASS_L: left, PASS_R: right, PASS_F: far_chip}[kind]]
        to = {RIGHT: right, FAR_R: right, LEFT: left, FAR_L: left}.get(kind, partner)
        return remote(src, dst, (kv_send.at[kind], kv_recv.at[kind]), to)

    def kv_keep():
        return pltpu.make_async_copy(kv_sum, dkv_full.at[me], kv_keep_sem.at[0])

    def kv_steps():
        def start():
            stored(batch - 1)
            for r in range(chips):
                kv_pair(r).start()
                kv_mine(r).start()

        def sum_chip():
            for r in range(chips):
                kv_mine(r).wait()
                kv_pair(r).wait_recv()
            chip = lambda r: (kv_ours[r][...].astype(F32) + kv_theirs[r].astype(F32)).astype(BF16)
            kv_far[...] = chip(chips // 2)
            for way in range(2):
                kv_far_copy(way).start()
            kv_near[0][...] = chip(1)
            kv_near[1][...] = chip(chips - 1)

        def relay_far():
            for way in range(2):
                kv_far_copy(way).wait_recv()
            for way in range(2):
                at = slice(way * kv_half, way * kv_half + kv_half)
                kv_near[way][at, :] = (kv_near[way][at, :].astype(F32) + kv_far_in[at, :].astype(F32)).astype(BF16)
            for way in range(2):
                kv_near_copy(way).start()

        def sum_all():
            for way in range(2):
                kv_near_copy(way).wait_recv()
            chip = kv_ours[0][...].astype(F32) + kv_theirs[0].astype(F32)
            kv_sum[...] = (chip + kv_near_in[0].astype(F32) + kv_near_in[1].astype(F32)).astype(BF16)
            for kind in (RIGHT, LEFT, PART):
                kv_move(kind).start()
            kv_keep().start()

        def spread():
            kv_move(RIGHT).wait_recv()
            kv_move(FAR_R).start()
            kv_move(LEFT).wait_recv()
            kv_move(FAR_L).start()
            kv_move(PASS_L).start()
            kv_move(PASS_R).start()

        def spread_far():
            kv_move(FAR_R).wait_recv()
            kv_move(FAR_L).wait_recv()
            kv_move(PASS_F).start()

        def settle_kv():
            for kind in (PART, PASS_L, PASS_R, PASS_F):
                kv_move(kind).wait_recv()
            kv_keep().wait()
            for kind in range(8):
                kv_move(kind).wait_send()
            for way in range(2):
                kv_far_copy(way).wait_send()
                kv_near_copy(way).wait_send()
            for r in range(chips):
                kv_pair(r).wait_send()

        return start, sum_chip, relay_far, sum_all, spread, spread_far, settle_kv

    load_x(0).start()
    load_dy(0).start()
    load_x(1).start()
    weights = (pltpu.make_async_copy(wq_hbm, w_buf.at[:, pl.ds(0, q_width)], w_sem.at[0]),
               pltpu.make_async_copy(wkv_hbm, w_buf.at[:, pl.ds(q_width, kv_width)], w_sem.at[1]),
               pltpu.make_async_copy(wo_hbm, wo_buf, w_sem.at[2]))
    launch(0)
    launch(1)
    for copy in weights:
        copy.start()
    for b in range(1, batch):
        load_dy(b).start()
    dbo[...] = jnp.zeros_like(dbo)
    dbq[...] = jnp.zeros_like(dbq)
    bias[:, pl.ds(0, q_width)] = b_q[...].reshape(1, q_width)
    bias[:, pl.ds(q_width, kv_width)] = b_kv[...].reshape(1, kv_width)
    for copy in weights:
        copy.wait()

    lead = units - 2

    @pl.loop(0, lead + scatters + 3)
    def _(s):
        t = s - lead
        when = lambda low, high: pl.when(jnp.logical_and(t >= low, t < high))

        @pl.when(s < units)
        def _():
            unit(s, forward)

        launch(s + 2)

        @pl.when(s < units)
        def _():
            unit(s, share)

        unit(s - 2, retire)

        @when(1, scatters + 1)
        def _():
            combine(t - 1)

        @when(2, scatters + 2)
        def _():
            relay(t - 2)

        @when(0, scatters)
        def _():
            fetch(t)

        @when(3, 5)
        def _():
            grad_part(batch - 5 + t)

        turn(s - 2, attend_and_project, differentiate)

        @pl.when(jnp.logical_and(s < units - 1, lax.rem(s, 2) == 1))
        def _():
            @pl.when(s >= 3)
            def _():
                grad_part(lax.div(s - 3, 2))

        unit(s - 1, share_far)
        unit(s - 1, complete)
        turn(s - 1, project, grad_attended)

        @when(3, scatters + 3)
        def _():
            finish(t - 3)

        @when(2, 3)
        def _():
            scatter_x(0).start()

        for n, act in enumerate(kv_steps()):
            @when(4 + n, 5 + n)
            def _():
                act()

        @when(6, 6 + batch - early)
        def _():
            late_sum(t - 6)

        @when(5, 5 + batch - early)
        def _():
            for chip in range(chips):
                late_pair(t - 5, chip).start()

    late_store(batch - early - 1).wait()
    for chip in range(chips):
        for v in range(batch - early):
            late_pair(v, chip).wait_send()
    store_att(batch - 1).wait()
    store_y(y_out, 0).wait()
    for r in range(chips):
        pair(o_part.at[0], r).wait_send()
    for way in range(2):
        for u in (scatters - 2, scatters - 1):
            far(u, way).wait_send()
        for u in (scatters - 3, scatters - 2, scatters - 1):
            near(u, way).wait_send()


def attention_block(x_loc, dy_loc, gamma, beta, w_q, w_kv, b_q, b_kv, w_o, b_o, early, ring, dim):
    batch, rows, width = x_loc.shape
    q_width, kv_width = w_q.shape[1], w_kv.shape[1]
    qkv_width = q_width + kv_width
    seq = rows * ring
    units = 2 * batch
    chips = ring // 2
    heads = q_width // dim
    hbm = pl.BlockSpec(memory_space=pl.ANY)
    vmem = pl.BlockSpec(memory_space=pltpu.VMEM)
    dma = pltpu.SemaphoreType.DMA
    full = lambda n, w: jax.ShapeDtypeStruct((n, seq, w), BF16)
    at_home = lambda n: jax.ShapeDtypeStruct((n, rows, width), BF16)
    half_seq = jax.ShapeDtypeStruct((batch - early, chips * rows, width), BF16)
    owned = jax.ShapeDtypeStruct((ring, batch * rows, kv_width), BF16)
    lo, hi = (lambda *shape: pltpu.VMEM(shape, BF16)), (lambda *shape: pltpu.VMEM(shape, F32))
    return pl.pallas_call(
        functools.partial(block_kernel, heads, dim),
        name="attention_block",
        out_shape=(full(batch, width), full(batch, width), full(batch, q_width), full(batch, width), full(batch, q_width), owned, owned, at_home(early),
                   full(batch, width), half_seq, half_seq, at_home(batch),
                   jax.ShapeDtypeStruct((8, width), F32), jax.ShapeDtypeStruct((8, q_width), F32), jax.ShapeDtypeStruct((2, batch, rows, 128), F32)),
        in_specs=[hbm, hbm, vmem, vmem, hbm, hbm, vmem, vmem, hbm, vmem],
        out_specs=(hbm,) * 12 + (vmem, vmem, vmem),
        scratch_shapes=[
            lo(units + 2, rows, width), hi(1, qkv_width), lo(width, qkv_width), lo(q_width, width), lo(seq, width), lo(seq, qkv_width), lo(seq, q_width), lo(seq, q_width),
            lo(seq, q_width), lo(seq, kv_width), lo(2, seq, 512), hi(seq, kv_width), hi(heads, 8, seq),
            hi(seq, q_width), hi(seq, q_width), lo(seq, q_width), lo(seq, q_width), lo(q_width, dim), lo(q_width, dim),
            lo(chips, rows, width), lo(3, rows, width), lo(3, 2, rows, width),
            lo(chips, batch * rows, kv_width), lo(batch * rows, kv_width), lo(2, batch * rows, kv_width),
            dma((8, units)), dma((8, units)), dma((2,)), dma((batch,)), dma((units,)), dma((3,)), dma((1,)), dma((1,)), dma((1,)), dma((ring,)), dma((2,)),
            dma((ring + 3,)),
            dma((chips,)), dma((chips,)), dma((chips,)), dma((2, 2)), dma((3, 2)), dma((3, 2)), dma((3, 2)), pltpu.SemaphoreType.REGULAR,
            dma((chips,)), dma((chips,)), dma((chips,)), dma((2,)), dma((2,)), dma((2,)), dma((2,)), dma((8,)), dma((8,)), dma((1,)),
            dma((batch - early, chips)), dma((batch - early, chips)), dma((chips + 2,))],
        compiler_params=pltpu.CompilerParams(collective_id=0, has_side_effects=True, vmem_limit_bytes=VMEM_LIMIT),
        cost_estimate=pl.CostEstimate(flops=8 * batch * seq * width * qkv_width, bytes_accessed=12 * batch * seq * width, transcendentals=0),
    )(x_loc, dy_loc, gamma, beta, w_q, w_kv, b_q, b_kv, w_o, b_o)


def norm_backward_kernel(dh, x, dy, ln_stats, gamma, dx, sums, x_hat_s, scaled_s):
    rows, width = x.shape[1:]
    tile = 512

    @pl.when(pl.program_id(0) == 0)
    def _():
        sums[...] = jnp.zeros_like(sums)

    mean, inv_std = ln_stats[0, 0, :, :1], ln_stats[1, 0, :, :1]
    by_lane = lambda v: v[:, :128] + v[:, 128:256] + v[:, 256:384] + v[:, 384:]
    by_sublane = lambda v: jnp.sum(v.reshape(-1, 8, tile), axis=0)

    def gather_sums(n, carry):
        plain, along = carry
        at = pl.ds(pl.multiple_of(n * tile, tile), tile)
        grad_h = dh[0, :, at].astype(F32)
        x_hat = (x[0, :, at].astype(F32) - mean) * inv_std
        scaled = grad_h * gamma[:, at]
        x_hat_s[:, at] = x_hat
        scaled_s[:, at] = scaled
        sums[0, :, at] += by_sublane(grad_h * x_hat)
        sums[1, :, at] += by_sublane(grad_h)
        return plain + by_lane(scaled), along + by_lane(scaled * x_hat)

    zero = jnp.zeros((rows, 128), F32)
    plain, along = lax.fori_loop(0, width // tile, gather_sums, (zero, zero), unroll=2)
    plain = jnp.sum(plain, axis=-1, keepdims=True) / width
    along = jnp.sum(along, axis=-1, keepdims=True) / width

    @pl.loop(0, width // tile, unroll=2)
    def _(n):
        at = pl.ds(pl.multiple_of(n * tile, tile), tile)
        grad_in = inv_std * (scaled_s[:, at] - plain - x_hat_s[:, at] * along)
        dx[0, :, at] = (dy[0, :, at].astype(F32) + grad_in).astype(BF16)


def norm_backward(grad_h, x_loc, dy_loc, ln_stats, gamma):
    batch, rows, width = x_loc.shape
    block = pl.BlockSpec((1, rows, width), lambda b: (b, 0, 0))
    still = lambda shape: pl.BlockSpec(shape, lambda b: (0,) * len(shape))
    return pl.pallas_call(
        norm_backward_kernel,
        name="norm_backward",
        grid=(batch,),
        out_shape=(jax.ShapeDtypeStruct(x_loc.shape, BF16), jax.ShapeDtypeStruct((2, 8, width), F32)),
        in_specs=[block, block, block, pl.BlockSpec((2, 1, rows, 128), lambda b: (0, b, 0, 0)), still(gamma.shape)],
        out_specs=(block, still((2, 8, width))),
        scratch_shapes=[pltpu.VMEM((rows, width), F32), pltpu.VMEM((rows, width), F32)],
        compiler_params=pltpu.CompilerParams(vmem_limit_bytes=VMEM_LIMIT),
        cost_estimate=pl.CostEstimate(flops=60 * batch * rows * width, bytes_accessed=8 * batch * rows * width, transcendentals=0),
    )(grad_h, x_loc, dy_loc, ln_stats, gamma)


def turn_rows(rows, dst, place):
    count, cols = rows.shape
    chunk = 512

    @pl.loop(0, count, step=chunk)
    def _(k):
        at = pl.ds(pl.multiple_of(k, chunk), chunk)
        dst[place : place + cols, at] = rows[at, :].T


def grad_wo_kernel(att, dy, out, turned):
    @pl.when(pl.program_id(0) == 0)
    def _():
        turn_rows(att, turned, 0)

    @pl.loop(0, out.shape[1], step=256)
    def _(n):
        at = pl.ds(pl.multiple_of(n, 256), 256)
        out[:, at] = jnp.dot(turned[...], dy[:, at], preferred_element_type=F32)


def whole(shape):
    return pl.BlockSpec(shape, lambda n: (0,) * len(shape), pipeline_mode=pl.Buffered(1))


def grad_wo(att, dy):
    tokens, q_width = att.shape
    width = dy.shape[1]
    tile = 512
    return pl.pallas_call(
        grad_wo_kernel,
        name="grad_wo",
        grid=(width // tile,),
        out_shape=jax.ShapeDtypeStruct((q_width, width), F32),
        in_specs=[whole(att.shape), pl.BlockSpec((tokens, tile), lambda n: (0, n))],
        out_specs=pl.BlockSpec((q_width, tile), lambda n: (0, n)),
        scratch_shapes=[pltpu.VMEM((q_width, tokens), BF16)],
        compiler_params=pltpu.CompilerParams(vmem_limit_bytes=VMEM_LIMIT),
        cost_estimate=pl.CostEstimate(flops=2 * tokens * q_width * width, bytes_accessed=2 * tokens * width + 4 * q_width * width, transcendentals=0),
    )(att, dy)


def grad_wq_kernel(rows, grad_q, kv_owned, h, out_q, out_kv, kv_sums, turned, kv_lines):
    tokens, q_width = grad_q.shape
    ring, owned, kv_width = kv_owned.shape
    first = q_width - kv_width

    @pl.when(pl.program_id(0) == 0)
    def _():
        turn_rows(grad_q, turned, 0)

        @pl.loop(0, owned, step=rows)
        def _(r):
            for owner in range(ring):
                place = pl.multiple_of(r * ring + owner * rows, rows)
                kv_lines[pl.ds(place, rows), :] = kv_owned[owner, pl.ds(pl.multiple_of(r, rows), rows), :]

        turn_rows(kv_lines, turned, q_width)
        kv_sums[...] = jnp.zeros_like(kv_sums)

        @pl.loop(0, tokens, step=512)
        def _(k):
            kv_sums[...] += jnp.sum(kv_lines[pl.ds(pl.multiple_of(k, 512), 512), :].astype(F32).reshape(-1, 8, kv_width), axis=0)

    @pl.loop(0, out_q.shape[0], step=256)
    def _(n):
        at = pl.ds(pl.multiple_of(n, 256), 256)
        out_q[at, :first] = jnp.dot(turned[:first, :], h[:, at], preferred_element_type=F32).T
        late = jnp.dot(turned[first:, :], h[:, at], preferred_element_type=F32).T
        out_q[at, first:] = late[:, :kv_width]
        out_kv[at, :] = late[:, kv_width:]


def grad_wq(grad_q, kv_owned, h, rows):
    tokens, q_width = grad_q.shape
    kv_width = kv_owned.shape[2]
    width = h.shape[1]
    tile = 512
    return pl.pallas_call(
        functools.partial(grad_wq_kernel, rows),
        name="grad_wq",
        grid=(width // tile,),
        out_shape=(jax.ShapeDtypeStruct((width, q_width), F32), jax.ShapeDtypeStruct((width, kv_width), F32), jax.ShapeDtypeStruct((8, kv_width), F32)),
        in_specs=[whole(grad_q.shape), whole(kv_owned.shape), pl.BlockSpec((tokens, tile), lambda n: (0, n))],
        out_specs=(pl.BlockSpec((tile, q_width), lambda n: (n, 0)), pl.BlockSpec((tile, kv_width), lambda n: (n, 0)), pl.BlockSpec((8, kv_width), lambda n: (0, 0))),
        scratch_shapes=[pltpu.VMEM((q_width + kv_width, tokens), BF16), pltpu.VMEM((tokens, kv_width), BF16)],
        compiler_params=pltpu.CompilerParams(vmem_limit_bytes=VMEM_LIMIT),
        cost_estimate=pl.CostEstimate(flops=2 * tokens * (q_width + kv_width) * width, bytes_accessed=2 * tokens * width + 4 * (q_width + kv_width) * width, transcendentals=0),
    )(grad_q, kv_owned, h)


def settle(values, count):
    block = pl.BlockSpec((1,) + values.shape[1:], lambda b: (b, 0, 0))

    def body(src, dst):
        dst[...] = src[...]

    return pl.pallas_call(
        body, name="settle", grid=(values.shape[0],), out_shape=jax.ShapeDtypeStruct((count,) + values.shape[1:], values.dtype), in_specs=[block], out_specs=block,
        compiler_params=pltpu.CompilerParams(vmem_limit_bytes=VMEM_LIMIT),
        cost_estimate=pl.CostEstimate(flops=values.size * 100, bytes_accessed=values.size * 4, transcendentals=0))(values)


def finish_y(o_late, x_loc, b_o, started):
    count, rows, width = o_late.shape
    first = x_loc.shape[0] - count
    late = pl.BlockSpec((1, rows, width), lambda b: (b + first, 0, 0))

    def body(o, x, b_o, _, y):
        y[...] = (x[...].astype(F32) + o[...].astype(F32) + b_o[...][None]).astype(BF16)

    return pl.pallas_call(
        body, name="finish_y", grid=(count,), out_shape=jax.ShapeDtypeStruct(x_loc.shape, BF16),
        in_specs=[pl.BlockSpec((1, rows, width), lambda b: (b, 0, 0)), late, pl.BlockSpec((1, width), lambda b: (0, 0)), pl.BlockSpec(memory_space=pl.ANY)],
        out_specs=late, input_output_aliases={3: 0}, compiler_params=pltpu.CompilerParams(vmem_limit_bytes=VMEM_LIMIT),
        cost_estimate=pl.CostEstimate(flops=o_late.size * 100, bytes_accessed=o_late.size * 6, transcendentals=0))(o_late, x_loc, b_o, started)


def sum_kernel(ring, rows, out, parts, gathered, send, recv):
    me = lax.axis_index("tp")
    barrier = pltpu.get_barrier_semaphore()
    others = [lax.rem(me + k, ring) for k in range(1, ring)]
    for other in others:
        pl.semaphore_signal(barrier, inc=1, device_id={"tp": other}, device_id_type=pl.DeviceIdType.MESH)
    groups = rows.shape[2] // 128
    for kind in range(2):
        row = jnp.sum(rows[kind], axis=0, keepdims=True)
        for n in range(groups):
            parts[kind * groups + n : kind * groups + n + 1, :] = row[:, n * 128 : (n + 1) * 128]
    pl.semaphore_wait(barrier, ring - 1)

    def copy(k):
        return pltpu.make_async_remote_copy(
            src_ref=parts, dst_ref=gathered.at[me], send_sem=send.at[k], recv_sem=recv.at[k],
            device_id={"tp": lax.rem(me + k, ring)}, device_id_type=pl.DeviceIdType.MESH)

    for k in range(1, ring):
        copy(k).start()
    gathered[me] = parts[...]
    for k in range(1, ring):
        copy(k).wait_recv()
    total = gathered[0]
    for k in range(1, ring):
        total = total + gathered[k]
    out[...] = total
    for k in range(1, ring):
        copy(k).wait_send()


def sum_over_ring(rows, ring):
    vmem = pl.BlockSpec(memory_space=pltpu.VMEM)
    shape = (2 * rows.shape[2] // 128, 128)
    return pl.pallas_call(
        functools.partial(sum_kernel, ring),
        name="sum_over_ring",
        out_shape=jax.ShapeDtypeStruct(shape, F32),
        in_specs=[vmem],
        out_specs=vmem,
        scratch_shapes=[pltpu.VMEM(shape, F32), pltpu.VMEM((ring,) + shape, F32), pltpu.SemaphoreType.DMA((ring,)), pltpu.SemaphoreType.DMA((ring,))],
        compiler_params=pltpu.CompilerParams(collective_id=2, has_side_effects=True),
    )(rows)


def solution(mesh):
    ring = mesh.shape["tp"]

    def device_block(x_loc, ln_gamma, ln_beta, w_q, b_q, w_kv, b_kv, w_o, b_o, dy_loc):
        head_dim = w_kv.shape[1] // 2
        batch, own_rows, width = x_loc.shape
        early = 3 * batch // 8
        normed_full, dy_full, merged, _, grad_q, _, kv_owned, y_early, _, _, o_chip, grad_h, bo_rows, bq_rows, ln_stats = attention_block(
            x_loc, dy_loc, ln_gamma[None, :], ln_beta[None, :], w_q, w_kv, b_q, b_kv, w_o, b_o[None, :], early, ring, head_dim)
        lines = [[i for i in range(ring) if i % 2 == core] for core in range(2)]
        o_late = lax.psum_scatter(o_chip, "tp", scatter_dimension=1, tiled=True, axis_index_groups=lines)

        flat = lambda v: v.reshape(-1, v.shape[-1])
        grad_x, parts = norm_backward(grad_h, x_loc, dy_loc, ln_stats, ln_gamma[None, :])
        sums = sum_over_ring(parts, ring).reshape(2, width)
        wo_grad = grad_wo(flat(merged), flat(dy_full))
        wq_grad, wkv_grad, kv_sums = grad_wq(flat(grad_q), kv_owned, flat(normed_full), own_rows)
        grad_bq, grad_bkv, grad_bo = jnp.sum(bq_rows, axis=0), jnp.sum(kv_sums, axis=0), jnp.sum(bo_rows, axis=0)
        y_loc = finish_y(o_late, x_loc, b_o[None, :], settle(y_early, batch))
        return (y_loc, grad_x, sums[0], sums[1], wq_grad, grad_bq, wkv_grad, grad_bkv, wo_grad, grad_bo)

    return jax.shard_map(
        device_block,
        mesh=mesh,
        in_specs=(P("dp", "tp", None), P(None), P(None), P(None, "tp"), P("tp"), P(None, None), P(None), P("tp", None), P(None), P("dp", "tp", None)),
        out_specs=(P("dp", "tp", None), P("dp", "tp", None), P("dp"), P("dp"), P("dp", "tp"), P(("dp", "tp")), P("dp", None), P("dp"), P(("dp", "tp"), None), P("dp")),
        check_vma=False,
    )
```

```python
import functools

import jax
import jax.numpy as jnp
from jax import lax
from jax.experimental import pallas as pl
from jax.experimental.pallas import tpu as pltpu
from jax.sharding import PartitionSpec as P

LN_EPS = 1e-5
VMEM_LIMIT = 64 * 1024 * 1024 - 65536
BF16 = jnp.bfloat16
F32 = jnp.float32

RIGHT, LEFT, PART, FAR_R, FAR_L, PASS_L, PASS_R, PASS_F = range(8)


def stack_heads(rows, dst, first, heads, dim):
    for h in range(heads):
        dst[h * dim : (h + 1) * dim, :] = rows[first : first + dim, h * dim : (h + 1) * dim]


def scaled_scores(scores_s, lanes, first, dim):
    scores = scores_s[: first + dim, lanes] * dim**-0.5
    keys = lax.broadcasted_iota(jnp.int32, scores.shape, 0)
    queries = lax.broadcasted_iota(jnp.int32, scores.shape, 1) + first
    return jnp.where(keys <= queries, scores, -1e30)


ACROSS = (((1,), (1,)), ((), ()))
DOWN = (((0,), (0,)), ((), ()))


def attend(qkv, out, stats, scores_s, probs_s, q_s, heads, dim):
    rows = qkv.shape[0]
    width = heads * dim
    for first in range(0, rows, dim):
        last = first + dim
        stack_heads(qkv, q_s, first, heads, dim)
        scores_s[:last, :] = lax.dot_general(qkv[:last, width : width + dim], q_s[...], ACROSS, preferred_element_type=F32)

        @pl.loop(0, heads, unroll=2)
        def _(h):
            lanes = pl.ds(pl.multiple_of(h * dim, dim), dim)
            scores = scaled_scores(scores_s, lanes, first, dim)
            top = jnp.max(scores, axis=0, keepdims=True)
            weights = jnp.exp(scores - top)
            share = 1.0 / jnp.sum(weights, axis=0, keepdims=True)
            probs_s[:last, lanes] = (weights * share).astype(BF16)
            stats[h, 0:1, first:last] = top
            stats[h, 1:2, first:last] = share

        turned = lax.dot_general(qkv[:last, width + dim :], probs_s[:last, :], DOWN, preferred_element_type=F32)
        for h in range(heads):
            out[first:last, h * dim : (h + 1) * dim] = turned[:, h * dim : (h + 1) * dim].T.astype(BF16)


def attend_backward(qkv, grad_att, grad_q, grad_kv, stats, scores_s, grad_p_s, probs_s, grad_s_s, q_s, att_s, heads, dim):
    rows = qkv.shape[0]
    width = heads * dim
    grad_kv[...] = jnp.zeros_like(grad_kv)
    for first in range(0, rows, dim):
        last = first + dim
        stack_heads(qkv, q_s, first, heads, dim)
        stack_heads(grad_att, att_s, first, heads, dim)
        scores_s[:last, :] = lax.dot_general(qkv[:last, width : width + dim], q_s[...], ACROSS, preferred_element_type=F32)
        grad_p_s[:last, :] = lax.dot_general(qkv[:last, width + dim :], att_s[...], ACROSS, preferred_element_type=F32)

        @pl.loop(0, heads, unroll=2)
        def _(h):
            lanes = pl.ds(pl.multiple_of(h * dim, dim), dim)
            scores = scaled_scores(scores_s, lanes, first, dim)
            probs = jnp.exp(scores - stats[h, 0:1, first:last]) * stats[h, 1:2, first:last]
            grad_p = grad_p_s[:last, lanes].astype(BF16).astype(F32)
            row_dot = jnp.sum(probs * grad_p, axis=0, keepdims=True)
            grad_s_s[:last, lanes] = (probs * (grad_p - row_dot) * dim**-0.5).astype(BF16)
            probs_s[:last, lanes] = probs.astype(BF16)

        turned = lax.dot_general(qkv[:last, width : width + dim], grad_s_s[:last, :], DOWN, preferred_element_type=F32)
        for h in range(heads):
            grad_q[first:last, h * dim : (h + 1) * dim] = turned[:, h * dim : (h + 1) * dim].T.astype(BF16)
        grad_kv[:last, :dim] += jnp.dot(grad_s_s[:last, :], q_s[...], preferred_element_type=F32)
        grad_kv[:last, dim:] += jnp.dot(probs_s[:last, :], att_s[...], preferred_element_type=F32)


def block_kernel(heads, dim, x_hbm, dy_hbm, gamma, beta, wq_hbm, wkv_hbm, b_q, b_kv, wo_hbm, b_o,
                 h_full, dy_full, att_out, o_part, dq_out, dkv_part, dkv_full, y_out, dh_part, o_theirs, o_chip, dh_sum, dbo, dbq, ln_stats,
                 own, bias, w_buf, wo_buf, h_buf, qkv_buf, att_buf, da_buf, dq_buf, dkv_buf, part_buf, total, stats,
                 scores_s, grad_p_s, probs_s, grad_s_s, q_s, att_s, theirs, far_in, near_in, kv_theirs, kv_far_in, kv_near_in,
                 send, recv, x_sem, dy_sem, keep_sem, w_sem, h_sem, att_sem, dq_sem, dkv_sem, part_sem, load_sem,
                 ours_sem, pair_send, pair_recv, far_send, far_recv, near_send, near_recv, free,
                 kv_ours_sem, kv_pair_send, kv_pair_recv, kv_far_send, kv_far_recv, kv_near_send, kv_near_recv, kv_send, kv_recv, kv_keep_sem, late_send, late_recv, late_sem):
    batch, rows, width = x_hbm.shape
    early = y_out.shape[0]
    half = rows // 2
    wide = width // 2
    units = 2 * batch
    scatters = batch + early
    ring = h_full.shape[1] // rows
    chips = ring // 2
    q_width = heads * dim
    kv_width = 2 * dim
    tile = 512
    me = lax.axis_index("tp")
    partner = me + 1 - 2 * lax.rem(me, 2)
    right, left, far_chip = lax.rem(me + 2, ring), lax.rem(me + ring - 2, ring), lax.rem(me + ring // 2, ring)
    OURS, NEAR, SUM, FAR, X, Y = 0, 4, 10, 13, units, units + 1

    barrier = pltpu.get_barrier_semaphore()
    for other in (left, right, partner):
        pl.semaphore_signal(barrier, inc=1, device_id={"tp": other}, device_id_type=pl.DeviceIdType.MESH)
    pl.semaphore_wait(barrier, 3)

    def remote(src, dst, sems, to):
        return pltpu.make_async_remote_copy(
            src_ref=src, dst_ref=dst, send_sem=sems[0], recv_sem=sems[1], device_id={"tp": to}, device_id_type=pl.DeviceIdType.MESH)

    def columns(low, high, act, step=tile):
        @pl.loop(low, high, step=step)
        def _(n):
            act(pl.ds(pl.multiple_of(n, step), step))

    def block(full, b, owner, first=0, count=rows):
        return full.at[b, pl.ds(pl.multiple_of(owner * rows + first, half), count)]

    def move(kind, full, b, u):
        if kind in (RIGHT, LEFT, PART):
            src, dst = own.at[u], block(full, b, me)
        elif kind in (FAR_R, FAR_L):
            src = dst = block(full, b, left, 0, half) if kind == FAR_R else block(full, b, right, half, half)
        else:
            src = dst = block(full, b, {PASS_L: left, PASS_R: right, PASS_F: far_chip}[kind])
        to = {RIGHT: right, FAR_R: right, LEFT: left, FAR_L: left}.get(kind, partner)
        return remote(src, dst, (send.at[kind, u], recv.at[kind, u]), to)

    def keep(full, b, u):
        return pltpu.make_async_copy(own.at[u], block(full, b, me), keep_sem.at[u])

    def load_x(b):
        return pltpu.make_async_copy(x_hbm.at[b], own.at[units + lax.rem(b, 2)], x_sem.at[lax.rem(b, 2)])

    def load_dy(b):
        return pltpu.make_async_copy(dy_hbm.at[b], own.at[2 * b + 1], dy_sem.at[b])

    def turn(u, h_act, dy_act):
        b = lax.div(u, 2)
        inside = jnp.logical_and(u >= 0, u < units)

        @pl.when(jnp.logical_and(inside, lax.rem(u, 2) == 0))
        def _():
            h_act(b)

        @pl.when(jnp.logical_and(inside, lax.rem(u, 2) == 1))
        def _():
            dy_act(b)

    def unit(u, act):
        turn(u, lambda b: act(h_full, b, u), lambda b: act(dy_full, b, u))

    def normalise(b):
        load_x(b).wait()
        slot = units + lax.rem(b, 2)

        @pl.loop(0, rows, step=16)
        def _(r):
            at = pl.ds(pl.multiple_of(r, 16), 16)
            x_wide = own[slot, at, :].astype(F32)
            mean = jnp.mean(x_wide, axis=-1, keepdims=True)
            centred = x_wide - mean
            inv_std = lax.rsqrt(jnp.mean(centred * centred, axis=-1, keepdims=True) + LN_EPS)
            own[2 * b, at, :] = (centred * inv_std * gamma[...] + beta[...]).astype(BF16)
            ln_stats[0, b, at, :] = jnp.broadcast_to(mean, (16, 128))
            ln_stats[1, b, at, :] = jnp.broadcast_to(inv_std, (16, 128))

        @pl.when(b + 2 < batch)
        def _():
            load_x(b + 2).start()

    def launch(u):
        turn(u, normalise, lambda b: load_dy(b).wait())

        def act(full, b, u):
            for kind in (RIGHT, LEFT, PART):
                move(kind, full, b, u).start()
            keep(full, b, u).start()

        unit(u, act)

    def forward(full, b, u):
        move(RIGHT, full, b, u).wait_recv()
        move(FAR_R, full, b, u).start()
        move(LEFT, full, b, u).wait_recv()
        move(FAR_L, full, b, u).start()

    def share(full, b, u):
        move(PASS_L, full, b, u).start()
        move(PASS_R, full, b, u).start()

    def share_far(full, b, u):
        move(FAR_R, full, b, u).wait_recv()
        move(FAR_L, full, b, u).wait_recv()
        move(PASS_F, full, b, u).start()

    def complete(full, b, u):
        for kind in (PART, PASS_L, PASS_R, PASS_F):
            move(kind, full, b, u).wait_recv()
        keep(full, b, u).wait()

    def retire(full, b, u):
        for kind in range(8):
            move(kind, full, b, u).wait_send()

    def load_block(full, b):
        load = pltpu.make_async_copy(full.at[b], h_buf, h_sem.at[0])
        load.start()
        load.wait()

    def project(b):
        load_block(h_full, b)

        def act(at):
            qkv_buf[:, at] = (jnp.dot(h_buf[...], w_buf[:, at], preferred_element_type=F32) + bias[:, at]).astype(BF16)

        columns(0, q_width + kv_width, act, 256)

    def store_att(b):
        return pltpu.make_async_copy(att_buf, att_out.at[b], att_sem.at[0])

    def store_part(out, b, n):
        at = pl.ds(pl.multiple_of(n, tile), tile)
        slot = lax.rem(lax.div(n, tile), 2)
        return pltpu.make_async_copy(part_buf.at[slot], out.at[b, :, at], part_sem.at[slot])

    def make_part(product, store):
        @pl.loop(0, width, step=tile)
        def _(n):
            @pl.when(n >= 2 * tile)
            def _():
                store_part(o_part, 0, n - 2 * tile).wait()

            part_buf[lax.rem(lax.div(n, tile), 2)] = product(pl.ds(pl.multiple_of(n, tile), tile)).astype(BF16)
            store(n)

        for n in (width - 2 * tile, width - tile):
            store_part(o_part, 0, n).wait()

    def project_out(b):
        make_part(lambda at: jnp.dot(att_buf[...], wo_buf[:, at], preferred_element_type=F32), lambda n: store_part(o_part, b, n).start())

    def project_out_late(b):
        again = pltpu.make_async_copy(att_out.at[b], att_buf, load_sem.at[ring])
        again.start()
        again.wait()
        project_out(b)

    def attend_and_project(b):
        @pl.when(b > 0)
        def _():
            store_att(b - 1).wait()

        attend(qkv_buf, att_buf, stats, scores_s, probs_s, q_s, heads, dim)
        store_att(b).start()

        @pl.when(b < early)
        def _():
            project_out(b)

    def grad_attended(b):
        load_block(dy_full, b)

        def act(at):
            da_buf[:, at] = lax.dot_general(h_buf[...], wo_buf[at, :], ACROSS, preferred_element_type=F32).astype(BF16)

        columns(0, q_width, act, 256)

        def add(at):
            dbo[:, at] += jnp.sum(h_buf[:, at].astype(F32).reshape(-1, 8, tile), axis=0)

        columns(0, width, add)

    def store_dq(b):
        return pltpu.make_async_copy(dq_buf, dq_out.at[b], dq_sem.at[0])

    def store_dkv(b, owner):
        return pltpu.make_async_copy(dkv_buf.at[pl.ds(owner * rows, rows)], dkv_part.at[owner, pl.ds(pl.multiple_of(b * rows, rows), rows)], dkv_sem.at[owner])

    def stored(b):
        store_dq(b).wait()
        for owner in range(ring):
            store_dkv(b, owner).wait()

    def differentiate(b):
        @pl.when(b > 0)
        def _():
            stored(b - 1)

        attend_backward(qkv_buf, da_buf, dq_buf, total, stats, scores_s, grad_p_s, probs_s, grad_s_s, q_s, att_s, heads, dim)
        dkv_buf[...] = total[...].astype(BF16)

        def add(at):
            dbq[:, at] += jnp.sum(dq_buf[:, at].astype(F32).reshape(-1, 8, 256), axis=0)

        columns(0, q_width, add, 256)
        store_dq(b).start()
        for owner in range(ring):
            store_dkv(b, owner).start()

    def grad_part(b):
        def product(at):
            from_q = lax.dot_general(dq_buf[...], w_buf[at, :q_width], ACROSS, preferred_element_type=F32)
            return from_q + lax.dot_general(dkv_buf[...], w_buf[at, q_width:], ACROSS, preferred_element_type=F32)

        make_part(product, lambda n: store_part(dh_part, b, n).start())

    def line(owner):
        return pl.ds(pl.multiple_of(owner * rows, rows), rows)

    def sourced(u, act):
        @pl.when(u < early)
        def _():
            act(o_part.at[u])

        @pl.when(u >= early)
        def _():
            act(dh_part.at[u - early])

    def mine(part, r):
        return pltpu.make_async_copy(part.at[line(lax.rem(me + 2 * r, ring))], own.at[OURS + r], ours_sem.at[r])

    def pair(part, r):
        return remote(part.at[line(lax.rem(partner + 2 * r, ring))], theirs.at[r], (pair_send.at[r], pair_recv.at[r]), partner)

    def far(u, way):
        cols = pl.ds(way * wide, wide)
        return remote(own.at[FAR + lax.rem(u, 2), :, cols], far_in.at[lax.rem(u, 3), :, cols],
                      (far_send.at[lax.rem(u, 2), way], far_recv.at[lax.rem(u, 3), way]), (right, left)[way])

    def near(u, way):
        slot = lax.rem(u, 3)
        return remote(own.at[NEAR + 2 * slot + way], near_in.at[slot, way], (near_send.at[slot, way], near_recv.at[slot, way]), (right, left)[way])

    def fetch(u):
        @pl.when(u >= 1)
        def _():
            pl.semaphore_wait(free, 1)
            for r in range(chips):
                pair(o_part.at[0], r).wait_send()

        def act(part):
            for r in range(chips):
                pair(part, r).start()
            for r in range(chips):
                mine(part, r).start()

        sourced(u, act)

    def combine(u):
        slot2, slot3 = lax.rem(u, 2), lax.rem(u, 3)
        for r in range(chips):
            mine(o_part.at[0], r).wait()
            pair(o_part.at[0], r).wait_recv()

        @pl.when(u >= 2)
        def _():
            for way in range(2):
                far(u - 2, way).wait_send()

        @pl.when(u >= 3)
        def _():
            for way in range(2):
                near(u - 3, way).wait_send()

        def chip_sum(r, at):
            return (own[OURS + r, :, at].astype(F32) + theirs[r, :, at].astype(F32)).astype(BF16)

        def act_far(at):
            own[FAR + slot2, :, at] = chip_sum(chips // 2, at)

        columns(0, width, act_far)
        for way in range(2):
            far(u, way).start()

        def act(at):
            own[NEAR + 2 * slot3, :, at] = chip_sum(1, at)
            own[NEAR + 2 * slot3 + 1, :, at] = chip_sum(chips - 1, at)
            own[SUM + slot3, :, at] = chip_sum(0, at)

        columns(0, width, act)

        @pl.when(u + 1 < scatters)
        def _():
            pl.semaphore_signal(free, inc=1, device_id={"tp": partner}, device_id_type=pl.DeviceIdType.MESH)

    def relay(u):
        slot = lax.rem(u, 3)
        for way in range(2):
            far(u, way).wait_recv()
        for way in range(2):
            def act(at):
                place = NEAR + 2 * slot + way
                own[place, :, at] = (own[place, :, at].astype(F32) + far_in[slot, :, at].astype(F32)).astype(BF16)

            columns(way * wide, way * wide + wide, act)
        for way in range(2):
            near(u, way).start()

    def scatter_x(u):
        return pltpu.make_async_copy(x_hbm.at[u], own.at[X], load_sem.at[ring + 1])

    def store_y(out, b):
        return pltpu.make_async_copy(own.at[Y], out.at[b], load_sem.at[ring + 2])

    def finish(u):
        slot = lax.rem(u, 3)
        for way in range(2):
            near(u, way).wait_recv()

        @pl.when(u > 0)
        def _():
            store_y(y_out, 0).wait()

        def whole(at):
            return own[SUM + slot, :, at].astype(F32) + near_in[slot, 0, :, at].astype(F32) + near_in[slot, 1, :, at].astype(F32)

        @pl.when(u < early)
        def _():
            scatter_x(u).wait()

            def act(at):
                own[Y, :, at] = (own[X, :, at].astype(F32) + whole(at) + b_o[:, at]).astype(BF16)

            columns(0, width, act)
            store_y(y_out, u).start()

        @pl.when(u >= early)
        def _():
            def act(at):
                own[Y, :, at] = whole(at).astype(BF16)

            columns(0, width, act)
            store_y(dh_sum, u - early).start()

        @pl.when(u + 1 < early)
        def _():
            scatter_x(u + 1).start()

    core = lax.rem(me, 2)

    def late_pair(v, chip):
        return remote(o_part.at[early + v, line(2 * chip + 1 - core)], o_theirs.at[v, pl.ds(chip * rows, rows)], (late_send.at[v, chip], late_recv.at[v, chip]), partner)

    def late_loads(v):
        copies = [pltpu.make_async_copy(o_part.at[early + v, line(2 * chip + core)], h_buf.at[pl.ds(chip * rows, rows)], late_sem.at[chip]) for chip in range(chips)]
        return copies + [pltpu.make_async_copy(o_theirs.at[v], h_buf.at[pl.ds(chips * rows, chips * rows)], late_sem.at[chips])]

    def late_store(v):
        return pltpu.make_async_copy(h_buf.at[pl.ds(0, chips * rows)], o_chip.at[v], late_sem.at[chips + 1])

    def late_sum(v):
        for chip in range(chips):
            late_pair(v, chip).wait_recv()

        @pl.when(v > 0)
        def _():
            late_store(v - 1).wait()

        for copy in late_loads(v):
            copy.start()
        for copy in late_loads(v):
            copy.wait()

        def act(at):
            mine_, theirs_ = h_buf[: chips * rows, at].astype(F32), h_buf[chips * rows :, at].astype(F32)
            h_buf[: chips * rows, at] = (mine_ + theirs_).astype(BF16)

        columns(0, width, act)
        late_store(v).start()

    pick = lambda ref, n: ref.at[:, pl.ds(n * kv_width, kv_width)]
    kv_ours = [pick(probs_s, 0), pick(probs_s, 1), pick(probs_s, 2), pick(grad_s_s, 0)]
    kv_far, kv_sum = pick(grad_s_s, 1), pick(da_buf, 2)
    kv_near = [pick(da_buf, 0), pick(da_buf, 1)]
    kv_rows = batch * rows
    kv_half = kv_rows // 2

    def kv_mine(r):
        return pltpu.make_async_copy(dkv_part.at[lax.rem(me + 2 * r, ring)], kv_ours[r], kv_ours_sem.at[r])

    def kv_pair(r):
        return remote(dkv_part.at[lax.rem(partner + 2 * r, ring)], kv_theirs.at[r], (kv_pair_send.at[r], kv_pair_recv.at[r]), partner)

    def kv_far_copy(way):
        at = pl.ds(way * kv_half, kv_half)
        return remote(kv_far.at[at], kv_far_in.at[at], (kv_far_send.at[way], kv_far_recv.at[way]), (right, left)[way])

    def kv_near_copy(way):
        return remote(kv_near[way], kv_near_in.at[way], (kv_near_send.at[way], kv_near_recv.at[way]), (right, left)[way])

    def kv_move(kind):
        if kind in (RIGHT, LEFT, PART):
            src, dst = kv_sum, dkv_full.at[me]
        elif kind in (FAR_R, FAR_L):
            src = dst = dkv_full.at[left, pl.ds(0, kv_half)] if kind == FAR_R else dkv_full.at[right, pl.ds(kv_half, kv_half)]
        else:
            src = dst = dkv_full.at[{PASS_L: left, PASS_R: right, PASS_F: far_chip}[kind]]
        to = {RIGHT: right, FAR_R: right, LEFT: left, FAR_L: left}.get(kind, partner)
        return remote(src, dst, (kv_send.at[kind], kv_recv.at[kind]), to)

    def kv_keep():
        return pltpu.make_async_copy(kv_sum, dkv_full.at[me], kv_keep_sem.at[0])

    def kv_steps():
        def start():
            stored(batch - 1)
            for r in range(chips):
                kv_pair(r).start()
                kv_mine(r).start()

        def sum_chip():
            for r in range(chips):
                kv_mine(r).wait()
                kv_pair(r).wait_recv()
            chip = lambda r: (kv_ours[r][...].astype(F32) + kv_theirs[r].astype(F32)).astype(BF16)
            kv_far[...] = chip(chips // 2)
            for way in range(2):
                kv_far_copy(way).start()
            kv_near[0][...] = chip(1)
            kv_near[1][...] = chip(chips - 1)

        def relay_far():
            for way in range(2):
                kv_far_copy(way).wait_recv()
            for way in range(2):
                at = slice(way * kv_half, way * kv_half + kv_half)
                kv_near[way][at, :] = (kv_near[way][at, :].astype(F32) + kv_far_in[at, :].astype(F32)).astype(BF16)
            for way in range(2):
                kv_near_copy(way).start()

        def sum_all():
            for way in range(2):
                kv_near_copy(way).wait_recv()
            chip = kv_ours[0][...].astype(F32) + kv_theirs[0].astype(F32)
            kv_sum[...] = (chip + kv_near_in[0].astype(F32) + kv_near_in[1].astype(F32)).astype(BF16)
            for kind in (RIGHT, LEFT, PART):
                kv_move(kind).start()
            kv_keep().start()

        def spread():
            kv_move(RIGHT).wait_recv()
            kv_move(FAR_R).start()
            kv_move(LEFT).wait_recv()
            kv_move(FAR_L).start()
            kv_move(PASS_L).start()
            kv_move(PASS_R).start()

        def spread_far():
            kv_move(FAR_R).wait_recv()
            kv_move(FAR_L).wait_recv()
            kv_move(PASS_F).start()

        def settle_kv():
            for kind in (PART, PASS_L, PASS_R, PASS_F):
                kv_move(kind).wait_recv()
            kv_keep().wait()
            for kind in range(8):
                kv_move(kind).wait_send()
            for way in range(2):
                kv_far_copy(way).wait_send()
                kv_near_copy(way).wait_send()
            for r in range(chips):
                kv_pair(r).wait_send()

        return start, sum_chip, relay_far, sum_all, spread, spread_far, settle_kv

    load_x(0).start()
    load_dy(0).start()
    load_x(1).start()
    weights = (pltpu.make_async_copy(wq_hbm, w_buf.at[:, pl.ds(0, q_width)], w_sem.at[0]),
               pltpu.make_async_copy(wkv_hbm, w_buf.at[:, pl.ds(q_width, kv_width)], w_sem.at[1]),
               pltpu.make_async_copy(wo_hbm, wo_buf, w_sem.at[2]))
    launch(0)
    launch(1)
    for copy in weights:
        copy.start()
    for b in range(1, batch):
        load_dy(b).start()
    dbo[...] = jnp.zeros_like(dbo)
    dbq[...] = jnp.zeros_like(dbq)
    bias[:, pl.ds(0, q_width)] = b_q[...].reshape(1, q_width)
    bias[:, pl.ds(q_width, kv_width)] = b_kv[...].reshape(1, kv_width)
    for copy in weights:
        copy.wait()

    lead = units - 2

    @pl.loop(0, lead + scatters + 3)
    def _(s):
        t = s - lead
        when = lambda low, high: pl.when(jnp.logical_and(t >= low, t < high))

        @pl.when(s < units)
        def _():
            unit(s, forward)

        launch(s + 2)

        @pl.when(s < units)
        def _():
            unit(s, share)

        unit(s - 2, retire)

        @when(1, scatters + 1)
        def _():
            combine(t - 1)

        @when(2, scatters + 2)
        def _():
            relay(t - 2)

        @when(0, scatters)
        def _():
            fetch(t)

        @when(3, 5)
        def _():
            grad_part(batch - 5 + t)

        turn(s - 2, attend_and_project, differentiate)

        @pl.when(jnp.logical_and(s < units - 1, lax.rem(s, 2) == 1))
        def _():
            @pl.when(s >= 3)
            def _():
                grad_part(lax.div(s - 3, 2))

        unit(s - 1, share_far)
        unit(s - 1, complete)
        turn(s - 1, project, grad_attended)

        @when(3, scatters + 3)
        def _():
            finish(t - 3)

        @when(2, 3)
        def _():
            scatter_x(0).start()

        for n, act in enumerate(kv_steps()):
            @when(4 + n, 5 + n)
            def _():
                act()

        @when(6, 6 + batch - early)
        def _():
            late_sum(t - 6)

        @when(4, 5)
        def _():
            store_att(batch - 1).wait()

        @when(5, 5 + batch - early)
        def _():
            project_out_late(early + t - 5)
            for chip in range(chips):
                late_pair(t - 5, chip).start()

    late_store(batch - early - 1).wait()
    for chip in range(chips):
        for v in range(batch - early):
            late_pair(v, chip).wait_send()
    store_y(y_out, 0).wait()
    for r in range(chips):
        pair(o_part.at[0], r).wait_send()
    for way in range(2):
        for u in (scatters - 2, scatters - 1):
            far(u, way).wait_send()
        for u in (scatters - 3, scatters - 2, scatters - 1):
            near(u, way).wait_send()


def attention_block(x_loc, dy_loc, gamma, beta, w_q, w_kv, b_q, b_kv, w_o, b_o, early, ring, dim):
    batch, rows, width = x_loc.shape
    q_width, kv_width = w_q.shape[1], w_kv.shape[1]
    qkv_width = q_width + kv_width
    seq = rows * ring
    units = 2 * batch
    chips = ring // 2
    heads = q_width // dim
    hbm = pl.BlockSpec(memory_space=pl.ANY)
    vmem = pl.BlockSpec(memory_space=pltpu.VMEM)
    dma = pltpu.SemaphoreType.DMA
    full = lambda n, w: jax.ShapeDtypeStruct((n, seq, w), BF16)
    at_home = lambda n: jax.ShapeDtypeStruct((n, rows, width), BF16)
    half_seq = jax.ShapeDtypeStruct((batch - early, chips * rows, width), BF16)
    owned = jax.ShapeDtypeStruct((ring, batch * rows, kv_width), BF16)
    lo, hi = (lambda *shape: pltpu.VMEM(shape, BF16)), (lambda *shape: pltpu.VMEM(shape, F32))
    return pl.pallas_call(
        functools.partial(block_kernel, heads, dim),
        name="attention_block",
        out_shape=(full(batch, width), full(batch, width), full(batch, q_width), full(batch, width), full(batch, q_width), owned, owned, at_home(early),
                   full(batch, width), half_seq, half_seq, at_home(batch),
                   jax.ShapeDtypeStruct((8, width), F32), jax.ShapeDtypeStruct((8, q_width), F32), jax.ShapeDtypeStruct((2, batch, rows, 128), F32)),
        in_specs=[hbm, hbm, vmem, vmem, hbm, hbm, vmem, vmem, hbm, vmem],
        out_specs=(hbm,) * 12 + (vmem, vmem, vmem),
        scratch_shapes=[
            lo(units + 2, rows, width), hi(1, qkv_width), lo(width, qkv_width), lo(q_width, width), lo(seq, width), lo(seq, qkv_width), lo(seq, q_width), lo(seq, q_width),
            lo(seq, q_width), lo(seq, kv_width), lo(2, seq, 512), hi(seq, kv_width), hi(heads, 8, seq),
            hi(seq, q_width), hi(seq, q_width), lo(seq, q_width), lo(seq, q_width), lo(q_width, dim), lo(q_width, dim),
            lo(chips, rows, width), lo(3, rows, width), lo(3, 2, rows, width),
            lo(chips, batch * rows, kv_width), lo(batch * rows, kv_width), lo(2, batch * rows, kv_width),
            dma((8, units)), dma((8, units)), dma((2,)), dma((batch,)), dma((units,)), dma((3,)), dma((1,)), dma((1,)), dma((1,)), dma((ring,)), dma((2,)),
            dma((ring + 3,)),
            dma((chips,)), dma((chips,)), dma((chips,)), dma((2, 2)), dma((3, 2)), dma((3, 2)), dma((3, 2)), pltpu.SemaphoreType.REGULAR,
            dma((chips,)), dma((chips,)), dma((chips,)), dma((2,)), dma((2,)), dma((2,)), dma((2,)), dma((8,)), dma((8,)), dma((1,)),
            dma((batch - early, chips)), dma((batch - early, chips)), dma((chips + 2,))],
        compiler_params=pltpu.CompilerParams(collective_id=0, has_side_effects=True, vmem_limit_bytes=VMEM_LIMIT),
        cost_estimate=pl.CostEstimate(flops=8 * batch * seq * width * qkv_width, bytes_accessed=12 * batch * seq * width, transcendentals=0),
    )(x_loc, dy_loc, gamma, beta, w_q, w_kv, b_q, b_kv, w_o, b_o)


def norm_backward_kernel(dh, x, dy, ln_stats, gamma, dx, sums, x_hat_s, scaled_s):
    rows, width = x.shape[1:]
    tile = 512

    @pl.when(pl.program_id(0) == 0)
    def _():
        sums[...] = jnp.zeros_like(sums)

    mean, inv_std = ln_stats[0, 0, :, :1], ln_stats[1, 0, :, :1]
    by_lane = lambda v: v[:, :128] + v[:, 128:256] + v[:, 256:384] + v[:, 384:]
    by_sublane = lambda v: jnp.sum(v.reshape(-1, 8, tile), axis=0)

    def gather_sums(n, carry):
        plain, along = carry
        at = pl.ds(pl.multiple_of(n * tile, tile), tile)
        grad_h = dh[0, :, at].astype(F32)
        x_hat = (x[0, :, at].astype(F32) - mean) * inv_std
        scaled = grad_h * gamma[:, at]
        x_hat_s[:, at] = x_hat
        scaled_s[:, at] = scaled
        sums[0, :, at] += by_sublane(grad_h * x_hat)
        sums[1, :, at] += by_sublane(grad_h)
        return plain + by_lane(scaled), along + by_lane(scaled * x_hat)

    zero = jnp.zeros((rows, 128), F32)
    plain, along = lax.fori_loop(0, width // tile, gather_sums, (zero, zero), unroll=2)
    plain = jnp.sum(plain, axis=-1, keepdims=True) / width
    along = jnp.sum(along, axis=-1, keepdims=True) / width

    @pl.loop(0, width // tile, unroll=2)
    def _(n):
        at = pl.ds(pl.multiple_of(n * tile, tile), tile)
        grad_in = inv_std * (scaled_s[:, at] - plain - x_hat_s[:, at] * along)
        dx[0, :, at] = (dy[0, :, at].astype(F32) + grad_in).astype(BF16)


def norm_backward(grad_h, x_loc, dy_loc, ln_stats, gamma):
    batch, rows, width = x_loc.shape
    block = pl.BlockSpec((1, rows, width), lambda b: (b, 0, 0))
    still = lambda shape: pl.BlockSpec(shape, lambda b: (0,) * len(shape))
    return pl.pallas_call(
        norm_backward_kernel,
        name="norm_backward",
        grid=(batch,),
        out_shape=(jax.ShapeDtypeStruct(x_loc.shape, BF16), jax.ShapeDtypeStruct((2, 8, width), F32)),
        in_specs=[block, block, block, pl.BlockSpec((2, 1, rows, 128), lambda b: (0, b, 0, 0)), still(gamma.shape)],
        out_specs=(block, still((2, 8, width))),
        scratch_shapes=[pltpu.VMEM((rows, width), F32), pltpu.VMEM((rows, width), F32)],
        compiler_params=pltpu.CompilerParams(vmem_limit_bytes=VMEM_LIMIT),
        cost_estimate=pl.CostEstimate(flops=60 * batch * rows * width, bytes_accessed=8 * batch * rows * width, transcendentals=0),
    )(grad_h, x_loc, dy_loc, ln_stats, gamma)


def turn_rows(rows, dst, place):
    count, cols = rows.shape
    chunk = 512

    @pl.loop(0, count, step=chunk)
    def _(k):
        at = pl.ds(pl.multiple_of(k, chunk), chunk)
        dst[place : place + cols, at] = rows[at, :].T


def whole(shape):
    return pl.BlockSpec(shape, lambda n: (0,) * len(shape), pipeline_mode=pl.Buffered(1))


def grad_wq_kernel(rows, grad_q, kv_owned, h, out_q, out_kv, kv_sums, turned, kv_lines):
    tokens, q_width = grad_q.shape
    ring, owned, kv_width = kv_owned.shape
    first = q_width - kv_width

    @pl.when(pl.program_id(0) == 0)
    def _():
        turn_rows(grad_q, turned, 0)

        @pl.loop(0, owned, step=rows)
        def _(r):
            for owner in range(ring):
                place = pl.multiple_of(r * ring + owner * rows, rows)
                kv_lines[pl.ds(place, rows), :] = kv_owned[owner, pl.ds(pl.multiple_of(r, rows), rows), :]

        turn_rows(kv_lines, turned, q_width)
        kv_sums[...] = jnp.zeros_like(kv_sums)

        @pl.loop(0, tokens, step=512)
        def _(k):
            kv_sums[...] += jnp.sum(kv_lines[pl.ds(pl.multiple_of(k, 512), 512), :].astype(F32).reshape(-1, 8, kv_width), axis=0)

    @pl.loop(0, out_q.shape[0], step=256)
    def _(n):
        at = pl.ds(pl.multiple_of(n, 256), 256)
        out_q[at, :first] = jnp.dot(turned[:first, :], h[:, at], preferred_element_type=F32).T
        late = jnp.dot(turned[first:, :], h[:, at], preferred_element_type=F32).T
        out_q[at, first:] = late[:, :kv_width]
        out_kv[at, :] = late[:, kv_width:]


def grad_wq(grad_q, kv_owned, h, rows):
    tokens, q_width = grad_q.shape
    kv_width = kv_owned.shape[2]
    width = h.shape[1]
    tile = 512
    return pl.pallas_call(
        functools.partial(grad_wq_kernel, rows),
        name="grad_wq",
        grid=(width // tile,),
        out_shape=(jax.ShapeDtypeStruct((width, q_width), F32), jax.ShapeDtypeStruct((width, kv_width), F32), jax.ShapeDtypeStruct((8, kv_width), F32)),
        in_specs=[whole(grad_q.shape), whole(kv_owned.shape), pl.BlockSpec((tokens, tile), lambda n: (0, n))],
        out_specs=(pl.BlockSpec((tile, q_width), lambda n: (n, 0)), pl.BlockSpec((tile, kv_width), lambda n: (n, 0)), pl.BlockSpec((8, kv_width), lambda n: (0, 0))),
        scratch_shapes=[pltpu.VMEM((q_width + kv_width, tokens), BF16), pltpu.VMEM((tokens, kv_width), BF16)],
        compiler_params=pltpu.CompilerParams(vmem_limit_bytes=VMEM_LIMIT),
        cost_estimate=pl.CostEstimate(flops=2 * tokens * (q_width + kv_width) * width, bytes_accessed=2 * tokens * width + 4 * (q_width + kv_width) * width, transcendentals=0),
    )(grad_q, kv_owned, h)


def settle(values, count):
    block = pl.BlockSpec((1,) + values.shape[1:], lambda b: (b, 0, 0))

    def body(src, dst):
        dst[...] = src[...]

    return pl.pallas_call(
        body, name="settle", grid=(values.shape[0],), out_shape=jax.ShapeDtypeStruct((count,) + values.shape[1:], values.dtype), in_specs=[block], out_specs=block,
        compiler_params=pltpu.CompilerParams(vmem_limit_bytes=VMEM_LIMIT),
        cost_estimate=pl.CostEstimate(flops=values.size * 100, bytes_accessed=values.size * 4, transcendentals=0))(values)


def finish_y(o_late, x_loc, b_o, started):
    count, rows, width = o_late.shape
    first = x_loc.shape[0] - count
    late = pl.BlockSpec((1, rows, width), lambda b: (b + first, 0, 0))

    def body(o, x, b_o, _, y):
        y[...] = (x[...].astype(F32) + o[...].astype(F32) + b_o[...][None]).astype(BF16)

    return pl.pallas_call(
        body, name="finish_y", grid=(count,), out_shape=jax.ShapeDtypeStruct(x_loc.shape, BF16),
        in_specs=[pl.BlockSpec((1, rows, width), lambda b: (b, 0, 0)), late, pl.BlockSpec((1, width), lambda b: (0, 0)), pl.BlockSpec(memory_space=pl.ANY)],
        out_specs=late, input_output_aliases={3: 0}, compiler_params=pltpu.CompilerParams(vmem_limit_bytes=VMEM_LIMIT),
        cost_estimate=pl.CostEstimate(flops=o_late.size * 100, bytes_accessed=o_late.size * 6, transcendentals=0))(o_late, x_loc, b_o, started)


def sum_kernel(ring, rows, out, parts, gathered, send, recv):
    me = lax.axis_index("tp")
    barrier = pltpu.get_barrier_semaphore()
    others = [lax.rem(me + k, ring) for k in range(1, ring)]
    for other in others:
        pl.semaphore_signal(barrier, inc=1, device_id={"tp": other}, device_id_type=pl.DeviceIdType.MESH)
    groups = rows.shape[2] // 128
    for kind in range(2):
        row = jnp.sum(rows[kind], axis=0, keepdims=True)
        for n in range(groups):
            parts[kind * groups + n : kind * groups + n + 1, :] = row[:, n * 128 : (n + 1) * 128]
    pl.semaphore_wait(barrier, ring - 1)

    def copy(k):
        return pltpu.make_async_remote_copy(
            src_ref=parts, dst_ref=gathered.at[me], send_sem=send.at[k], recv_sem=recv.at[k],
            device_id={"tp": lax.rem(me + k, ring)}, device_id_type=pl.DeviceIdType.MESH)

    for k in range(1, ring):
        copy(k).start()
    gathered[me] = parts[...]
    for k in range(1, ring):
        copy(k).wait_recv()
    total = gathered[0]
    for k in range(1, ring):
        total = total + gathered[k]
    out[...] = total
    for k in range(1, ring):
        copy(k).wait_send()


def sum_over_ring(rows, ring):
    vmem = pl.BlockSpec(memory_space=pltpu.VMEM)
    shape = (2 * rows.shape[2] // 128, 128)
    return pl.pallas_call(
        functools.partial(sum_kernel, ring),
        name="sum_over_ring",
        out_shape=jax.ShapeDtypeStruct(shape, F32),
        in_specs=[vmem],
        out_specs=vmem,
        scratch_shapes=[pltpu.VMEM(shape, F32), pltpu.VMEM((ring,) + shape, F32), pltpu.SemaphoreType.DMA((ring,)), pltpu.SemaphoreType.DMA((ring,))],
        compiler_params=pltpu.CompilerParams(collective_id=2, has_side_effects=True),
    )(rows)


def solution(mesh):
    ring = mesh.shape["tp"]

    def device_block(x_loc, ln_gamma, ln_beta, w_q, b_q, w_kv, b_kv, w_o, b_o, dy_loc):
        head_dim = w_kv.shape[1] // 2
        batch, own_rows, width = x_loc.shape
        early = batch // 4
        normed_full, dy_full, merged, _, grad_q, _, kv_owned, y_early, _, _, o_chip, grad_h, bo_rows, bq_rows, ln_stats = attention_block(
            x_loc, dy_loc, ln_gamma[None, :], ln_beta[None, :], w_q, w_kv, b_q, b_kv, w_o, b_o[None, :], early, ring, head_dim)
        lines = [[i for i in range(ring) if i % 2 == core] for core in range(2)]
        o_late = lax.psum_scatter(o_chip, "tp", scatter_dimension=1, tiled=True, axis_index_groups=lines)

        flat = lambda v: v.reshape(-1, v.shape[-1])
        grad_x, parts = norm_backward(grad_h, x_loc, dy_loc, ln_stats, ln_gamma[None, :])
        sums = sum_over_ring(parts, ring).reshape(2, width)
        wo_grad = jnp.einsum("bse,bsd->ed", merged, dy_full, preferred_element_type=jnp.float32)
        wq_grad, wkv_grad, kv_sums = grad_wq(flat(grad_q), kv_owned, flat(normed_full), own_rows)
        grad_bq, grad_bkv, grad_bo = jnp.sum(bq_rows, axis=0), jnp.sum(kv_sums, axis=0), jnp.sum(bo_rows, axis=0)
        y_loc = finish_y(o_late, x_loc, b_o[None, :], settle(y_early, batch))
        return (y_loc, grad_x, sums[0], sums[1], wq_grad, grad_bq, wkv_grad, grad_bkv, wo_grad, grad_bo)

    return jax.shard_map(
        device_block,
        mesh=mesh,
        in_specs=(P("dp", "tp", None), P(None), P(None), P(None, "tp"), P("tp"), P(None, None), P(None), P("tp", None), P(None), P("dp", "tp", None)),
        out_specs=(P("dp", "tp", None), P("dp", "tp", None), P("dp"), P("dp"), P("dp", "tp"), P(("dp", "tp")), P("dp", None), P("dp"), P(("dp", "tp"), None), P("dp")),
        check_vma=False,
    )
```

```python
import functools

import jax
import jax.numpy as jnp
from jax import lax
from jax.experimental import pallas as pl
from jax.experimental.pallas import tpu as pltpu
from jax.sharding import PartitionSpec as P

LN_EPS = 1e-5
VMEM_LIMIT = 64 * 1024 * 1024 - 65536
BF16 = jnp.bfloat16
F32 = jnp.float32

RIGHT, LEFT, PART, FAR_R, FAR_L, PASS_L, PASS_R, PASS_F = range(8)


def stack_heads(rows, dst, first, heads, dim):
    for h in range(heads):
        dst[h * dim : (h + 1) * dim, :] = rows[first : first + dim, h * dim : (h + 1) * dim]


def scaled_scores(scores_s, lanes, first, dim):
    scores = scores_s[: first + dim, lanes] * dim**-0.5
    keys = lax.broadcasted_iota(jnp.int32, scores.shape, 0)
    queries = lax.broadcasted_iota(jnp.int32, scores.shape, 1) + first
    return jnp.where(keys <= queries, scores, -1e30)


ACROSS = (((1,), (1,)), ((), ()))
DOWN = (((0,), (0,)), ((), ()))


def attend(qkv, out, stats, scores_s, probs_s, q_s, heads, dim):
    rows = qkv.shape[0]
    width = heads * dim
    for first in range(0, rows, dim):
        last = first + dim
        stack_heads(qkv, q_s, first, heads, dim)
        scores_s[:last, :] = lax.dot_general(qkv[:last, width : width + dim], q_s[...], ACROSS, preferred_element_type=F32)

        @pl.loop(0, heads, unroll=2)
        def _(h):
            lanes = pl.ds(pl.multiple_of(h * dim, dim), dim)
            scores = scaled_scores(scores_s, lanes, first, dim)
            top = jnp.max(scores, axis=0, keepdims=True)
            weights = jnp.exp(scores - top)
            share = 1.0 / jnp.sum(weights, axis=0, keepdims=True)
            probs_s[:last, lanes] = (weights * share).astype(BF16)
            stats[h, 0:1, first:last] = top
            stats[h, 1:2, first:last] = share

        turned = lax.dot_general(qkv[:last, width + dim :], probs_s[:last, :], DOWN, preferred_element_type=F32)
        for h in range(heads):
            out[first:last, h * dim : (h + 1) * dim] = turned[:, h * dim : (h + 1) * dim].T.astype(BF16)


def attend_backward(qkv, grad_att, grad_q, grad_kv, stats, scores_s, grad_p_s, probs_s, grad_s_s, q_s, att_s, heads, dim):
    rows = qkv.shape[0]
    width = heads * dim
    grad_kv[...] = jnp.zeros_like(grad_kv)
    for first in range(0, rows, dim):
        last = first + dim
        stack_heads(qkv, q_s, first, heads, dim)
        stack_heads(grad_att, att_s, first, heads, dim)
        scores_s[:last, :] = lax.dot_general(qkv[:last, width : width + dim], q_s[...], ACROSS, preferred_element_type=F32)
        grad_p_s[:last, :] = lax.dot_general(qkv[:last, width + dim :], att_s[...], ACROSS, preferred_element_type=F32)

        @pl.loop(0, heads, unroll=2)
        def _(h):
            lanes = pl.ds(pl.multiple_of(h * dim, dim), dim)
            scores = scaled_scores(scores_s, lanes, first, dim)
            probs = jnp.exp(scores - stats[h, 0:1, first:last]) * stats[h, 1:2, first:last]
            grad_p = grad_p_s[:last, lanes].astype(BF16).astype(F32)
            row_dot = jnp.sum(probs * grad_p, axis=0, keepdims=True)
            grad_s_s[:last, lanes] = (probs * (grad_p - row_dot) * dim**-0.5).astype(BF16)
            probs_s[:last, lanes] = probs.astype(BF16)

        turned = lax.dot_general(qkv[:last, width : width + dim], grad_s_s[:last, :], DOWN, preferred_element_type=F32)
        for h in range(heads):
            grad_q[first:last, h * dim : (h + 1) * dim] = turned[:, h * dim : (h + 1) * dim].T.astype(BF16)
        grad_kv[:last, :dim] += jnp.dot(grad_s_s[:last, :], q_s[...], preferred_element_type=F32)
        grad_kv[:last, dim:] += jnp.dot(probs_s[:last, :], att_s[...], preferred_element_type=F32)


def block_kernel(heads, dim, x_hbm, dy_hbm, gamma, beta, wq_hbm, wkv_hbm, b_q, b_kv, wo_hbm, b_o,
                 h_full, dy_full, att_out, o_part, dq_out, dkv_part, dkv_full, y_out, dh_part, o_theirs, o_chip, dh_sum, dbo, dbq, ln_stats,
                 own, bias, w_buf, wo_buf, h_buf, qkv_buf, att_buf, da_buf, dq_buf, dkv_buf, part_buf, total, stats,
                 scores_s, grad_p_s, probs_s, grad_s_s, q_s, att_s, theirs, far_in, near_in, kv_theirs, kv_far_in, kv_near_in,
                 send, recv, x_sem, dy_sem, keep_sem, w_sem, h_sem, att_sem, dq_sem, dkv_sem, part_sem, load_sem,
                 ours_sem, pair_send, pair_recv, far_send, far_recv, near_send, near_recv, free,
                 kv_ours_sem, kv_pair_send, kv_pair_recv, kv_far_send, kv_far_recv, kv_near_send, kv_near_recv, kv_send, kv_recv, kv_keep_sem, late_send, late_recv, late_sem):
    batch, rows, width = x_hbm.shape
    early = y_out.shape[0]
    half = rows // 2
    wide = width // 2
    units = 2 * batch
    scatters = batch + early
    ring = h_full.shape[1] // rows
    chips = ring // 2
    q_width = heads * dim
    kv_width = 2 * dim
    tile = 512
    me = lax.axis_index("tp")
    partner = me + 1 - 2 * lax.rem(me, 2)
    right, left, far_chip = lax.rem(me + 2, ring), lax.rem(me + ring - 2, ring), lax.rem(me + ring // 2, ring)
    OURS, NEAR, SUM, FAR, X, Y = 0, 4, 10, 13, units, units + 1

    barrier = pltpu.get_barrier_semaphore()
    for other in (left, right, partner):
        pl.semaphore_signal(barrier, inc=1, device_id={"tp": other}, device_id_type=pl.DeviceIdType.MESH)
    pl.semaphore_wait(barrier, 3)

    def remote(src, dst, sems, to):
        return pltpu.make_async_remote_copy(
            src_ref=src, dst_ref=dst, send_sem=sems[0], recv_sem=sems[1], device_id={"tp": to}, device_id_type=pl.DeviceIdType.MESH)

    def columns(low, high, act, step=tile):
        @pl.loop(low, high, step=step)
        def _(n):
            act(pl.ds(pl.multiple_of(n, step), step))

    def block(full, b, owner, first=0, count=rows):
        return full.at[b, pl.ds(pl.multiple_of(owner * rows + first, half), count)]

    def move(kind, full, b, u):
        if kind in (RIGHT, LEFT, PART):
            src, dst = own.at[u], block(full, b, me)
        elif kind in (FAR_R, FAR_L):
            src = dst = block(full, b, left, 0, half) if kind == FAR_R else block(full, b, right, half, half)
        else:
            src = dst = block(full, b, {PASS_L: left, PASS_R: right, PASS_F: far_chip}[kind])
        to = {RIGHT: right, FAR_R: right, LEFT: left, FAR_L: left}.get(kind, partner)
        return remote(src, dst, (send.at[kind, u], recv.at[kind, u]), to)

    def keep(full, b, u):
        return pltpu.make_async_copy(own.at[u], block(full, b, me), keep_sem.at[u])

    def load_x(b):
        return pltpu.make_async_copy(x_hbm.at[b], own.at[units + lax.rem(b, 2)], x_sem.at[lax.rem(b, 2)])

    def load_dy(b):
        return pltpu.make_async_copy(dy_hbm.at[b], own.at[2 * b + 1], dy_sem.at[b])

    def turn(u, h_act, dy_act):
        b = lax.div(u, 2)
        inside = jnp.logical_and(u >= 0, u < units)

        @pl.when(jnp.logical_and(inside, lax.rem(u, 2) == 0))
        def _():
            h_act(b)

        @pl.when(jnp.logical_and(inside, lax.rem(u, 2) == 1))
        def _():
            dy_act(b)

    def unit(u, act):
        turn(u, lambda b: act(h_full, b, u), lambda b: act(dy_full, b, u))

    def normalise(b):
        load_x(b).wait()
        slot = units + lax.rem(b, 2)

        @pl.loop(0, rows, step=16)
        def _(r):
            at = pl.ds(pl.multiple_of(r, 16), 16)
            x_wide = own[slot, at, :].astype(F32)
            mean = jnp.mean(x_wide, axis=-1, keepdims=True)
            centred = x_wide - mean
            inv_std = lax.rsqrt(jnp.mean(centred * centred, axis=-1, keepdims=True) + LN_EPS)
            own[2 * b, at, :] = (centred * inv_std * gamma[...] + beta[...]).astype(BF16)
            ln_stats[0, b, at, :] = jnp.broadcast_to(mean, (16, 128))
            ln_stats[1, b, at, :] = jnp.broadcast_to(inv_std, (16, 128))

        @pl.when(b + 2 < batch)
        def _():
            load_x(b + 2).start()

    def launch(u):
        turn(u, normalise, lambda b: load_dy(b).wait())

        def act(full, b, u):
            for kind in (RIGHT, LEFT, PART):
                move(kind, full, b, u).start()
            keep(full, b, u).start()

        unit(u, act)

    def forward(full, b, u):
        move(RIGHT, full, b, u).wait_recv()
        move(FAR_R, full, b, u).start()
        move(LEFT, full, b, u).wait_recv()
        move(FAR_L, full, b, u).start()

    def share(full, b, u):
        move(PASS_L, full, b, u).start()
        move(PASS_R, full, b, u).start()

    def share_far(full, b, u):
        move(FAR_R, full, b, u).wait_recv()
        move(FAR_L, full, b, u).wait_recv()
        move(PASS_F, full, b, u).start()

    def complete(full, b, u):
        for kind in (PART, PASS_L, PASS_R, PASS_F):
            move(kind, full, b, u).wait_recv()
        keep(full, b, u).wait()

    def retire(full, b, u):
        for kind in range(8):
            move(kind, full, b, u).wait_send()

    def load_block(full, b):
        load = pltpu.make_async_copy(full.at[b], h_buf, h_sem.at[0])
        load.start()
        load.wait()

    def project(b):
        load_block(h_full, b)

        def act(at):
            qkv_buf[:, at] = (jnp.dot(h_buf[...], w_buf[:, at], preferred_element_type=F32) + bias[:, at]).astype(BF16)

        columns(0, q_width + kv_width, act, 256)

    def store_att(b):
        return pltpu.make_async_copy(att_buf, att_out.at[b], att_sem.at[0])

    def store_part(out, b, n):
        at = pl.ds(pl.multiple_of(n, tile), tile)
        slot = lax.rem(lax.div(n, tile), 2)
        return pltpu.make_async_copy(part_buf.at[slot], out.at[b, :, at], part_sem.at[slot])

    def make_part(product, store):
        @pl.loop(0, width, step=tile)
        def _(n):
            @pl.when(n >= 2 * tile)
            def _():
                store_part(o_part, 0, n - 2 * tile).wait()

            part_buf[lax.rem(lax.div(n, tile), 2)] = product(pl.ds(pl.multiple_of(n, tile), tile)).astype(BF16)
            store(n)

        for n in (width - 2 * tile, width - tile):
            store_part(o_part, 0, n).wait()

    def project_out(b):
        make_part(lambda at: jnp.dot(att_buf[...], wo_buf[:, at], preferred_element_type=F32), lambda n: store_part(o_part, b, n).start())

    def project_out_late(b):
        again = pltpu.make_async_copy(att_out.at[b], att_buf, load_sem.at[ring])
        again.start()
        again.wait()
        project_out(b)

    def attend_and_project(b):
        @pl.when(b > 0)
        def _():
            store_att(b - 1).wait()

        attend(qkv_buf, att_buf, stats, scores_s, probs_s, q_s, heads, dim)
        store_att(b).start()

        @pl.when(b < early)
        def _():
            project_out(b)

    def grad_attended(b):
        load_block(dy_full, b)

        def act(at):
            da_buf[:, at] = lax.dot_general(h_buf[...], wo_buf[at, :], ACROSS, preferred_element_type=F32).astype(BF16)

        columns(0, q_width, act, 256)

        def add(at):
            dbo[:, at] += jnp.sum(h_buf[:, at].astype(F32).reshape(-1, 8, tile), axis=0)

        columns(0, width, add)

    def store_dq(b):
        return pltpu.make_async_copy(dq_buf, dq_out.at[b], dq_sem.at[0])

    def store_dkv(b, owner):
        return pltpu.make_async_copy(dkv_buf.at[pl.ds(owner * rows, rows)], dkv_part.at[owner, pl.ds(pl.multiple_of(b * rows, rows), rows)], dkv_sem.at[owner])

    def stored(b):
        store_dq(b).wait()
        for owner in range(ring):
            store_dkv(b, owner).wait()

    def differentiate(b):
        @pl.when(b > 0)
        def _():
            stored(b - 1)

        attend_backward(qkv_buf, da_buf, dq_buf, total, stats, scores_s, grad_p_s, probs_s, grad_s_s, q_s, att_s, heads, dim)
        dkv_buf[...] = total[...].astype(BF16)

        def add(at):
            dbq[:, at] += jnp.sum(dq_buf[:, at].astype(F32).reshape(-1, 8, 256), axis=0)

        columns(0, q_width, add, 256)
        store_dq(b).start()
        for owner in range(ring):
            store_dkv(b, owner).start()

    def grad_part(b):
        def product(at):
            from_q = lax.dot_general(dq_buf[...], w_buf[at, :q_width], ACROSS, preferred_element_type=F32)
            return from_q + lax.dot_general(dkv_buf[...], w_buf[at, q_width:], ACROSS, preferred_element_type=F32)

        make_part(product, lambda n: store_part(dh_part, b, n).start())

    def line(owner):
        return pl.ds(pl.multiple_of(owner * rows, rows), rows)

    def sourced(u, act):
        @pl.when(u < early)
        def _():
            act(o_part.at[u])

        @pl.when(u >= early)
        def _():
            act(dh_part.at[u - early])

    def mine(part, r):
        return pltpu.make_async_copy(part.at[line(lax.rem(me + 2 * r, ring))], own.at[OURS + r], ours_sem.at[r])

    def pair(part, r):
        return remote(part.at[line(lax.rem(partner + 2 * r, ring))], theirs.at[r], (pair_send.at[r], pair_recv.at[r]), partner)

    def far(u, way):
        cols = pl.ds(way * wide, wide)
        return remote(own.at[FAR + lax.rem(u, 2), :, cols], far_in.at[lax.rem(u, 3), :, cols],
                      (far_send.at[lax.rem(u, 2), way], far_recv.at[lax.rem(u, 3), way]), (right, left)[way])

    def near(u, way):
        slot = lax.rem(u, 3)
        return remote(own.at[NEAR + 2 * slot + way], near_in.at[slot, way], (near_send.at[slot, way], near_recv.at[slot, way]), (right, left)[way])

    def fetch(u):
        @pl.when(u >= 1)
        def _():
            pl.semaphore_wait(free, 1)
            for r in range(chips):
                pair(o_part.at[0], r).wait_send()

        def act(part):
            for r in range(chips):
                pair(part, r).start()
            for r in range(chips):
                mine(part, r).start()

        sourced(u, act)

    def combine(u):
        slot2, slot3 = lax.rem(u, 2), lax.rem(u, 3)
        for r in range(chips):
            mine(o_part.at[0], r).wait()
            pair(o_part.at[0], r).wait_recv()

        @pl.when(u >= 2)
        def _():
            for way in range(2):
                far(u - 2, way).wait_send()

        @pl.when(u >= 3)
        def _():
            for way in range(2):
                near(u - 3, way).wait_send()

        def chip_sum(r, at):
            return (own[OURS + r, :, at].astype(F32) + theirs[r, :, at].astype(F32)).astype(BF16)

        def act_far(at):
            own[FAR + slot2, :, at] = chip_sum(chips // 2, at)

        columns(0, width, act_far)
        for way in range(2):
            far(u, way).start()

        def act(at):
            own[NEAR + 2 * slot3, :, at] = chip_sum(1, at)
            own[NEAR + 2 * slot3 + 1, :, at] = chip_sum(chips - 1, at)
            own[SUM + slot3, :, at] = chip_sum(0, at)

        columns(0, width, act)

        @pl.when(u + 1 < scatters)
        def _():
            pl.semaphore_signal(free, inc=1, device_id={"tp": partner}, device_id_type=pl.DeviceIdType.MESH)

    def relay(u):
        slot = lax.rem(u, 3)
        for way in range(2):
            far(u, way).wait_recv()
        for way in range(2):
            def act(at):
                place = NEAR + 2 * slot + way
                own[place, :, at] = (own[place, :, at].astype(F32) + far_in[slot, :, at].astype(F32)).astype(BF16)

            columns(way * wide, way * wide + wide, act)
        for way in range(2):
            near(u, way).start()

    def scatter_x(u):
        return pltpu.make_async_copy(x_hbm.at[u], own.at[X], load_sem.at[ring + 1])

    def store_y(out, b):
        return pltpu.make_async_copy(own.at[Y], out.at[b], load_sem.at[ring + 2])

    def finish(u):
        slot = lax.rem(u, 3)
        for way in range(2):
            near(u, way).wait_recv()

        @pl.when(u > 0)
        def _():
            store_y(y_out, 0).wait()

        def whole(at):
            return own[SUM + slot, :, at].astype(F32) + near_in[slot, 0, :, at].astype(F32) + near_in[slot, 1, :, at].astype(F32)

        @pl.when(u < early)
        def _():
            scatter_x(u).wait()

            def act(at):
                own[Y, :, at] = (own[X, :, at].astype(F32) + whole(at) + b_o[:, at]).astype(BF16)

            columns(0, width, act)
            store_y(y_out, u).start()

        @pl.when(u >= early)
        def _():
            def act(at):
                own[Y, :, at] = whole(at).astype(BF16)

            columns(0, width, act)
            store_y(dh_sum, u - early).start()

        @pl.when(u + 1 < early)
        def _():
            scatter_x(u + 1).start()

    core = lax.rem(me, 2)

    def late_pair(v, chip):
        return remote(o_part.at[early + v, line(2 * chip + 1 - core)], o_theirs.at[v, pl.ds(chip * rows, rows)], (late_send.at[v, chip], late_recv.at[v, chip]), partner)

    def late_loads(v):
        copies = [pltpu.make_async_copy(o_part.at[early + v, line(2 * chip + core)], h_buf.at[pl.ds(chip * rows, rows)], late_sem.at[chip]) for chip in range(chips)]
        return copies + [pltpu.make_async_copy(o_theirs.at[v], h_buf.at[pl.ds(chips * rows, chips * rows)], late_sem.at[chips])]

    def late_stores(v):
        return [pltpu.make_async_copy(h_buf.at[pl.ds(chip * rows, rows)], o_chip.at[chip, pl.ds(pl.multiple_of(v * rows, rows), rows)],
                                      late_sem.at[chips + 1 + chip]) for chip in range(chips)]

    def late_sum(v):
        for chip in range(chips):
            late_pair(v, chip).wait_recv()

        @pl.when(v > 0)
        def _():
            for copy in late_stores(v - 1):
                copy.wait()

        for copy in late_loads(v):
            copy.start()
        for copy in late_loads(v):
            copy.wait()

        def act(at):
            mine_, theirs_ = h_buf[: chips * rows, at].astype(F32), h_buf[chips * rows :, at].astype(F32)
            h_buf[: chips * rows, at] = (mine_ + theirs_).astype(BF16)

        columns(0, width, act)
        for copy in late_stores(v):
            copy.start()

    pick = lambda ref, n: ref.at[:, pl.ds(n * kv_width, kv_width)]
    kv_ours = [pick(probs_s, 0), pick(probs_s, 1), pick(probs_s, 2), pick(grad_s_s, 0)]
    kv_far, kv_sum = pick(grad_s_s, 1), pick(da_buf, 2)
    kv_near = [pick(da_buf, 0), pick(da_buf, 1)]
    kv_rows = batch * rows
    kv_half = kv_rows // 2

    def kv_mine(r):
        return pltpu.make_async_copy(dkv_part.at[lax.rem(me + 2 * r, ring)], kv_ours[r], kv_ours_sem.at[r])

    def kv_pair(r):
        return remote(dkv_part.at[lax.rem(partner + 2 * r, ring)], kv_theirs.at[r], (kv_pair_send.at[r], kv_pair_recv.at[r]), partner)

    def kv_far_copy(way):
        at = pl.ds(way * kv_half, kv_half)
        return remote(kv_far.at[at], kv_far_in.at[at], (kv_far_send.at[way], kv_far_recv.at[way]), (right, left)[way])

    def kv_near_copy(way):
        return remote(kv_near[way], kv_near_in.at[way], (kv_near_send.at[way], kv_near_recv.at[way]), (right, left)[way])

    def kv_move(kind):
        if kind in (RIGHT, LEFT, PART):
            src, dst = kv_sum, dkv_full.at[me]
        elif kind in (FAR_R, FAR_L):
            src = dst = dkv_full.at[left, pl.ds(0, kv_half)] if kind == FAR_R else dkv_full.at[right, pl.ds(kv_half, kv_half)]
        else:
            src = dst = dkv_full.at[{PASS_L: left, PASS_R: right, PASS_F: far_chip}[kind]]
        to = {RIGHT: right, FAR_R: right, LEFT: left, FAR_L: left}.get(kind, partner)
        return remote(src, dst, (kv_send.at[kind], kv_recv.at[kind]), to)

    def kv_keep():
        return pltpu.make_async_copy(kv_sum, dkv_full.at[me], kv_keep_sem.at[0])

    def kv_steps():
        def start():
            stored(batch - 1)
            for r in range(chips):
                kv_pair(r).start()
                kv_mine(r).start()

        def sum_chip():
            for r in range(chips):
                kv_mine(r).wait()
                kv_pair(r).wait_recv()
            chip = lambda r: (kv_ours[r][...].astype(F32) + kv_theirs[r].astype(F32)).astype(BF16)
            kv_far[...] = chip(chips // 2)
            for way in range(2):
                kv_far_copy(way).start()
            kv_near[0][...] = chip(1)
            kv_near[1][...] = chip(chips - 1)

        def relay_far():
            for way in range(2):
                kv_far_copy(way).wait_recv()
            for way in range(2):
                at = slice(way * kv_half, way * kv_half + kv_half)
                kv_near[way][at, :] = (kv_near[way][at, :].astype(F32) + kv_far_in[at, :].astype(F32)).astype(BF16)
            for way in range(2):
                kv_near_copy(way).start()

        def sum_all():
            for way in range(2):
                kv_near_copy(way).wait_recv()
            chip = kv_ours[0][...].astype(F32) + kv_theirs[0].astype(F32)
            kv_sum[...] = (chip + kv_near_in[0].astype(F32) + kv_near_in[1].astype(F32)).astype(BF16)
            for kind in (RIGHT, LEFT, PART):
                kv_move(kind).start()
            kv_keep().start()

        def spread():
            kv_move(RIGHT).wait_recv()
            kv_move(FAR_R).start()
            kv_move(LEFT).wait_recv()
            kv_move(FAR_L).start()
            kv_move(PASS_L).start()
            kv_move(PASS_R).start()

        def spread_far():
            kv_move(FAR_R).wait_recv()
            kv_move(FAR_L).wait_recv()
            kv_move(PASS_F).start()

        def settle_kv():
            for kind in (PART, PASS_L, PASS_R, PASS_F):
                kv_move(kind).wait_recv()
            kv_keep().wait()
            for kind in range(8):
                kv_move(kind).wait_send()
            for way in range(2):
                kv_far_copy(way).wait_send()
                kv_near_copy(way).wait_send()
            for r in range(chips):
                kv_pair(r).wait_send()

        return start, sum_chip, relay_far, sum_all, spread, spread_far, settle_kv

    load_x(0).start()
    load_dy(0).start()
    load_x(1).start()
    weights = (pltpu.make_async_copy(wq_hbm, w_buf.at[:, pl.ds(0, q_width)], w_sem.at[0]),
               pltpu.make_async_copy(wkv_hbm, w_buf.at[:, pl.ds(q_width, kv_width)], w_sem.at[1]),
               pltpu.make_async_copy(wo_hbm, wo_buf, w_sem.at[2]))
    launch(0)
    launch(1)
    for copy in weights:
        copy.start()
    for b in range(1, batch):
        load_dy(b).start()
    dbo[...] = jnp.zeros_like(dbo)
    dbq[...] = jnp.zeros_like(dbq)
    bias[:, pl.ds(0, q_width)] = b_q[...].reshape(1, q_width)
    bias[:, pl.ds(q_width, kv_width)] = b_kv[...].reshape(1, kv_width)
    for copy in weights:
        copy.wait()

    lead = units - 2

    @pl.loop(0, lead + scatters + 3)
    def _(s):
        t = s - lead
        when = lambda low, high: pl.when(jnp.logical_and(t >= low, t < high))

        @pl.when(s < units)
        def _():
            unit(s, forward)

        launch(s + 2)

        @pl.when(s < units)
        def _():
            unit(s, share)

        unit(s - 2, retire)

        @when(1, scatters + 1)
        def _():
            combine(t - 1)

        @when(2, scatters + 2)
        def _():
            relay(t - 2)

        @when(0, scatters)
        def _():
            fetch(t)

        @when(3, 5)
        def _():
            grad_part(batch - 5 + t)

        turn(s - 2, attend_and_project, differentiate)

        @pl.when(jnp.logical_and(s < units - 1, lax.rem(s, 2) == 1))
        def _():
            @pl.when(s >= 3)
            def _():
                grad_part(lax.div(s - 3, 2))

        unit(s - 1, share_far)
        unit(s - 1, complete)
        turn(s - 1, project, grad_attended)

        @when(3, scatters + 3)
        def _():
            finish(t - 3)

        @when(2, 3)
        def _():
            scatter_x(0).start()

        for n, act in enumerate(kv_steps()):
            @when(4 + n, 5 + n)
            def _():
                act()

        @when(6, 6 + batch - early)
        def _():
            late_sum(t - 6)

        @when(4, 5)
        def _():
            store_att(batch - 1).wait()

        @when(5, 5 + batch - early)
        def _():
            project_out_late(early + t - 5)
            for chip in range(chips):
                late_pair(t - 5, chip).start()

    for copy in late_stores(batch - early - 1):
        copy.wait()
    for chip in range(chips):
        for v in range(batch - early):
            late_pair(v, chip).wait_send()
    store_y(y_out, 0).wait()
    for r in range(chips):
        pair(o_part.at[0], r).wait_send()
    for way in range(2):
        for u in (scatters - 2, scatters - 1):
            far(u, way).wait_send()
        for u in (scatters - 3, scatters - 2, scatters - 1):
            near(u, way).wait_send()


def attention_block(x_loc, dy_loc, gamma, beta, w_q, w_kv, b_q, b_kv, w_o, b_o, early, ring, dim):
    batch, rows, width = x_loc.shape
    q_width, kv_width = w_q.shape[1], w_kv.shape[1]
    qkv_width = q_width + kv_width
    seq = rows * ring
    units = 2 * batch
    chips = ring // 2
    heads = q_width // dim
    hbm = pl.BlockSpec(memory_space=pl.ANY)
    vmem = pl.BlockSpec(memory_space=pltpu.VMEM)
    dma = pltpu.SemaphoreType.DMA
    full = lambda n, w: jax.ShapeDtypeStruct((n, seq, w), BF16)
    at_home = lambda n: jax.ShapeDtypeStruct((n, rows, width), BF16)
    half_seq = jax.ShapeDtypeStruct((batch - early, chips * rows, width), BF16)
    owned = jax.ShapeDtypeStruct((ring, batch * rows, kv_width), BF16)
    lo, hi = (lambda *shape: pltpu.VMEM(shape, BF16)), (lambda *shape: pltpu.VMEM(shape, F32))
    return pl.pallas_call(
        functools.partial(block_kernel, heads, dim),
        name="attention_block",
        out_shape=(full(batch, width), full(batch, width), full(batch, q_width), full(batch, width), full(batch, q_width), owned, owned, at_home(early),
                   full(batch, width), half_seq, jax.ShapeDtypeStruct((chips, (batch - early) * rows, width), BF16), at_home(batch),
                   jax.ShapeDtypeStruct((8, width), F32), jax.ShapeDtypeStruct((8, q_width), F32), jax.ShapeDtypeStruct((2, batch, rows, 128), F32)),
        in_specs=[hbm, hbm, vmem, vmem, hbm, hbm, vmem, vmem, hbm, vmem],
        out_specs=(hbm,) * 12 + (vmem, vmem, vmem),
        scratch_shapes=[
            lo(units + 2, rows, width), hi(1, qkv_width), lo(width, qkv_width), lo(q_width, width), lo(seq, width), lo(seq, qkv_width), lo(seq, q_width), lo(seq, q_width),
            lo(seq, q_width), lo(seq, kv_width), lo(2, seq, 512), hi(seq, kv_width), hi(heads, 8, seq),
            hi(seq, q_width), hi(seq, q_width), lo(seq, q_width), lo(seq, q_width), lo(q_width, dim), lo(q_width, dim),
            lo(chips, rows, width), lo(3, rows, width), lo(3, 2, rows, width),
            lo(chips, batch * rows, kv_width), lo(batch * rows, kv_width), lo(2, batch * rows, kv_width),
            dma((8, units)), dma((8, units)), dma((2,)), dma((batch,)), dma((units,)), dma((3,)), dma((1,)), dma((1,)), dma((1,)), dma((ring,)), dma((2,)),
            dma((ring + 3,)),
            dma((chips,)), dma((chips,)), dma((chips,)), dma((2, 2)), dma((3, 2)), dma((3, 2)), dma((3, 2)), pltpu.SemaphoreType.REGULAR,
            dma((chips,)), dma((chips,)), dma((chips,)), dma((2,)), dma((2,)), dma((2,)), dma((2,)), dma((8,)), dma((8,)), dma((1,)),
            dma((batch - early, chips)), dma((batch - early, chips)), dma((2 * chips + 1,))],
        compiler_params=pltpu.CompilerParams(collective_id=0, has_side_effects=True, vmem_limit_bytes=VMEM_LIMIT),
        cost_estimate=pl.CostEstimate(flops=8 * batch * seq * width * qkv_width, bytes_accessed=12 * batch * seq * width, transcendentals=0),
    )(x_loc, dy_loc, gamma, beta, w_q, w_kv, b_q, b_kv, w_o, b_o)


def norm_backward_kernel(dh, x, dy, ln_stats, gamma, dx, sums, x_hat_s, scaled_s):
    rows, width = x.shape[1:]
    tile = 512

    @pl.when(pl.program_id(0) == 0)
    def _():
        sums[...] = jnp.zeros_like(sums)

    mean, inv_std = ln_stats[0, 0, :, :1], ln_stats[1, 0, :, :1]
    by_lane = lambda v: v[:, :128] + v[:, 128:256] + v[:, 256:384] + v[:, 384:]
    by_sublane = lambda v: jnp.sum(v.reshape(-1, 8, tile), axis=0)

    def gather_sums(n, carry):
        plain, along = carry
        at = pl.ds(pl.multiple_of(n * tile, tile), tile)
        grad_h = dh[0, :, at].astype(F32)
        x_hat = (x[0, :, at].astype(F32) - mean) * inv_std
        scaled = grad_h * gamma[:, at]
        x_hat_s[:, at] = x_hat
        scaled_s[:, at] = scaled
        sums[0, :, at] += by_sublane(grad_h * x_hat)
        sums[1, :, at] += by_sublane(grad_h)
        return plain + by_lane(scaled), along + by_lane(scaled * x_hat)

    zero = jnp.zeros((rows, 128), F32)
    plain, along = lax.fori_loop(0, width // tile, gather_sums, (zero, zero), unroll=2)
    plain = jnp.sum(plain, axis=-1, keepdims=True) / width
    along = jnp.sum(along, axis=-1, keepdims=True) / width

    @pl.loop(0, width // tile, unroll=2)
    def _(n):
        at = pl.ds(pl.multiple_of(n * tile, tile), tile)
        grad_in = inv_std * (scaled_s[:, at] - plain - x_hat_s[:, at] * along)
        dx[0, :, at] = (dy[0, :, at].astype(F32) + grad_in).astype(BF16)


def norm_backward(grad_h, x_loc, dy_loc, ln_stats, gamma):
    batch, rows, width = x_loc.shape
    block = pl.BlockSpec((1, rows, width), lambda b: (b, 0, 0))
    still = lambda shape: pl.BlockSpec(shape, lambda b: (0,) * len(shape))
    return pl.pallas_call(
        norm_backward_kernel,
        name="norm_backward",
        grid=(batch,),
        out_shape=(jax.ShapeDtypeStruct(x_loc.shape, BF16), jax.ShapeDtypeStruct((2, 8, width), F32)),
        in_specs=[block, block, block, pl.BlockSpec((2, 1, rows, 128), lambda b: (0, b, 0, 0)), still(gamma.shape)],
        out_specs=(block, still((2, 8, width))),
        scratch_shapes=[pltpu.VMEM((rows, width), F32), pltpu.VMEM((rows, width), F32)],
        compiler_params=pltpu.CompilerParams(vmem_limit_bytes=VMEM_LIMIT),
        cost_estimate=pl.CostEstimate(flops=60 * batch * rows * width, bytes_accessed=8 * batch * rows * width, transcendentals=0),
    )(grad_h, x_loc, dy_loc, ln_stats, gamma)


def turn_rows(rows, dst, place):
    count, cols = rows.shape
    chunk = 512

    @pl.loop(0, count, step=chunk)
    def _(k):
        at = pl.ds(pl.multiple_of(k, chunk), chunk)
        dst[place : place + cols, at] = rows[at, :].T


def whole(shape):
    return pl.BlockSpec(shape, lambda n: (0,) * len(shape), pipeline_mode=pl.Buffered(1))


def grad_wq_kernel(rows, grad_q, kv_owned, h, out_q, out_kv, kv_sums, turned, kv_lines):
    tokens, q_width = grad_q.shape
    ring, owned, kv_width = kv_owned.shape
    first = q_width - kv_width

    @pl.when(pl.program_id(0) == 0)
    def _():
        turn_rows(grad_q, turned, 0)

        @pl.loop(0, owned, step=rows)
        def _(r):
            for owner in range(ring):
                place = pl.multiple_of(r * ring + owner * rows, rows)
                kv_lines[pl.ds(place, rows), :] = kv_owned[owner, pl.ds(pl.multiple_of(r, rows), rows), :]

        turn_rows(kv_lines, turned, q_width)
        kv_sums[...] = jnp.zeros_like(kv_sums)

        @pl.loop(0, tokens, step=512)
        def _(k):
            kv_sums[...] += jnp.sum(kv_lines[pl.ds(pl.multiple_of(k, 512), 512), :].astype(F32).reshape(-1, 8, kv_width), axis=0)

    @pl.loop(0, out_q.shape[0], step=256)
    def _(n):
        at = pl.ds(pl.multiple_of(n, 256), 256)
        out_q[at, :first] = jnp.dot(turned[:first, :], h[:, at], preferred_element_type=F32).T
        late = jnp.dot(turned[first:, :], h[:, at], preferred_element_type=F32).T
        out_q[at, first:] = late[:, :kv_width]
        out_kv[at, :] = late[:, kv_width:]


def grad_wq(grad_q, kv_owned, h, rows):
    tokens, q_width = grad_q.shape
    kv_width = kv_owned.shape[2]
    width = h.shape[1]
    tile = 512
    return pl.pallas_call(
        functools.partial(grad_wq_kernel, rows),
        name="grad_wq",
        grid=(width // tile,),
        out_shape=(jax.ShapeDtypeStruct((width, q_width), F32), jax.ShapeDtypeStruct((width, kv_width), F32), jax.ShapeDtypeStruct((8, kv_width), F32)),
        in_specs=[whole(grad_q.shape), whole(kv_owned.shape), pl.BlockSpec((tokens, tile), lambda n: (0, n))],
        out_specs=(pl.BlockSpec((tile, q_width), lambda n: (n, 0)), pl.BlockSpec((tile, kv_width), lambda n: (n, 0)), pl.BlockSpec((8, kv_width), lambda n: (0, 0))),
        scratch_shapes=[pltpu.VMEM((q_width + kv_width, tokens), BF16), pltpu.VMEM((tokens, kv_width), BF16)],
        compiler_params=pltpu.CompilerParams(vmem_limit_bytes=VMEM_LIMIT),
        cost_estimate=pl.CostEstimate(flops=2 * tokens * (q_width + kv_width) * width, bytes_accessed=2 * tokens * width + 4 * (q_width + kv_width) * width, transcendentals=0),
    )(grad_q, kv_owned, h)


def settle(values, count):
    block = pl.BlockSpec((1,) + values.shape[1:], lambda b: (b, 0, 0))

    def body(src, dst):
        dst[...] = src[...]

    return pl.pallas_call(
        body, name="settle", grid=(values.shape[0],), out_shape=jax.ShapeDtypeStruct((count,) + values.shape[1:], values.dtype), in_specs=[block], out_specs=block,
        compiler_params=pltpu.CompilerParams(vmem_limit_bytes=VMEM_LIMIT),
        cost_estimate=pl.CostEstimate(flops=values.size * 100, bytes_accessed=values.size * 4, transcendentals=0))(values)


def finish_y_kernel(o_hbm, x_hbm, b_o, _, y_hbm, o_buf, x_buf, o_sem, x_sem, y_sem):
    count, rows, width = o_hbm.shape
    first = x_hbm.shape[0] - count
    tile = 512
    load_o = lambda v: pltpu.make_async_copy(o_hbm.at[v], o_buf.at[v], o_sem.at[v])
    load_x = lambda v: pltpu.make_async_copy(x_hbm.at[first + v], x_buf.at[v], x_sem.at[v])
    store_y = lambda v: pltpu.make_async_copy(o_buf.at[v], y_hbm.at[first + v], y_sem.at[v])
    for v in range(count):
        load_o(v).start()
        load_x(v).start()

    @pl.loop(0, count)
    def _(v):
        load_o(v).wait()
        load_x(v).wait()

        @pl.loop(0, width, step=tile)
        def _(n):
            at = pl.ds(pl.multiple_of(n, tile), tile)
            o_buf[v, :, at] = (x_buf[v, :, at].astype(F32) + o_buf[v, :, at].astype(F32) + b_o[:, at]).astype(BF16)

        store_y(v).start()

    for v in range(count):
        store_y(v).wait()


def finish_y(o_late, x_loc, b_o, started):
    count, rows, width = o_late.shape
    hbm = pl.BlockSpec(memory_space=pl.ANY)
    dma = pltpu.SemaphoreType.DMA((count,))
    return pl.pallas_call(
        finish_y_kernel, name="finish_y", out_shape=jax.ShapeDtypeStruct(x_loc.shape, BF16),
        in_specs=[hbm, hbm, pl.BlockSpec(memory_space=pltpu.VMEM), hbm], out_specs=hbm, input_output_aliases={3: 0},
        scratch_shapes=[pltpu.VMEM(o_late.shape, BF16), pltpu.VMEM(o_late.shape, BF16), dma, dma, dma],
        compiler_params=pltpu.CompilerParams(vmem_limit_bytes=VMEM_LIMIT),
        cost_estimate=pl.CostEstimate(flops=o_late.size * 100, bytes_accessed=o_late.size * 6, transcendentals=0))(o_late, x_loc, b_o, started)


def sum_kernel(ring, rows, out, parts, gathered, send, recv):
    me = lax.axis_index("tp")
    barrier = pltpu.get_barrier_semaphore()
    others = [lax.rem(me + k, ring) for k in range(1, ring)]
    for other in others:
        pl.semaphore_signal(barrier, inc=1, device_id={"tp": other}, device_id_type=pl.DeviceIdType.MESH)
    groups = rows.shape[2] // 128
    for kind in range(2):
        row = jnp.sum(rows[kind], axis=0, keepdims=True)
        for n in range(groups):
            parts[kind * groups + n : kind * groups + n + 1, :] = row[:, n * 128 : (n + 1) * 128]
    pl.semaphore_wait(barrier, ring - 1)

    def copy(k):
        return pltpu.make_async_remote_copy(
            src_ref=parts, dst_ref=gathered.at[me], send_sem=send.at[k], recv_sem=recv.at[k],
            device_id={"tp": lax.rem(me + k, ring)}, device_id_type=pl.DeviceIdType.MESH)

    for k in range(1, ring):
        copy(k).start()
    gathered[me] = parts[...]
    for k in range(1, ring):
        copy(k).wait_recv()
    total = gathered[0]
    for k in range(1, ring):
        total = total + gathered[k]
    out[...] = total
    for k in range(1, ring):
        copy(k).wait_send()


def sum_over_ring(rows, ring):
    vmem = pl.BlockSpec(memory_space=pltpu.VMEM)
    shape = (2 * rows.shape[2] // 128, 128)
    return pl.pallas_call(
        functools.partial(sum_kernel, ring),
        name="sum_over_ring",
        out_shape=jax.ShapeDtypeStruct(shape, F32),
        in_specs=[vmem],
        out_specs=vmem,
        scratch_shapes=[pltpu.VMEM(shape, F32), pltpu.VMEM((ring,) + shape, F32), pltpu.SemaphoreType.DMA((ring,)), pltpu.SemaphoreType.DMA((ring,))],
        compiler_params=pltpu.CompilerParams(collective_id=2, has_side_effects=True),
    )(rows)


def solution(mesh):
    ring = mesh.shape["tp"]

    def device_block(x_loc, ln_gamma, ln_beta, w_q, b_q, w_kv, b_kv, w_o, b_o, dy_loc):
        head_dim = w_kv.shape[1] // 2
        batch, own_rows, width = x_loc.shape
        early = batch // 4
        normed_full, dy_full, merged, _, grad_q, _, kv_owned, y_early, _, _, o_chip, grad_h, bo_rows, bq_rows, ln_stats = attention_block(
            x_loc, dy_loc, ln_gamma[None, :], ln_beta[None, :], w_q, w_kv, b_q, b_kv, w_o, b_o[None, :], early, ring, head_dim)
        lines = [[i for i in range(ring) if i % 2 == core] for core in range(2)]
        o_late = lax.psum_scatter(o_chip, "tp", scatter_dimension=0, tiled=True, axis_index_groups=lines).reshape(batch - early, own_rows, width)

        flat = lambda v: v.reshape(-1, v.shape[-1])
        grad_x, parts = norm_backward(grad_h, x_loc, dy_loc, ln_stats, ln_gamma[None, :])
        sums = sum_over_ring(parts, ring).reshape(2, width)
        wo_grad = jnp.einsum("bse,bsd->ed", merged, dy_full, preferred_element_type=jnp.float32)
        wq_grad, wkv_grad, kv_sums = grad_wq(flat(grad_q), kv_owned, flat(normed_full), own_rows)
        grad_bq, grad_bkv, grad_bo = jnp.sum(bq_rows, axis=0), jnp.sum(kv_sums, axis=0), jnp.sum(bo_rows, axis=0)
        y_loc = finish_y(o_late, x_loc, b_o[None, :], settle(y_early, batch))
        return (y_loc, grad_x, sums[0], sums[1], wq_grad, grad_bq, wkv_grad, grad_bkv, wo_grad, grad_bo)

    return jax.shard_map(
        device_block,
        mesh=mesh,
        in_specs=(P("dp", "tp", None), P(None), P(None), P(None, "tp"), P("tp"), P(None, None), P(None), P("tp", None), P(None), P("dp", "tp", None)),
        out_specs=(P("dp", "tp", None), P("dp", "tp", None), P("dp"), P("dp"), P("dp", "tp"), P(("dp", "tp")), P("dp", None), P("dp"), P(("dp", "tp"), None), P("dp")),
        check_vma=False,
    )
```

```python
import functools

import jax
import jax.numpy as jnp
from jax import lax
from jax.experimental import pallas as pl
from jax.experimental.pallas import tpu as pltpu
from jax.sharding import PartitionSpec as P

LN_EPS = 1e-5
VMEM_LIMIT = 64 * 1024 * 1024 - 65536
BF16 = jnp.bfloat16
F32 = jnp.float32

RIGHT, LEFT, PART, FAR_R, FAR_L, PASS_L, PASS_R, PASS_F = range(8)


def stack_heads(rows, dst, first, heads, dim):
    for h in range(heads):
        dst[h * dim : (h + 1) * dim, :] = rows[first : first + dim, h * dim : (h + 1) * dim]


def scaled_scores(scores_s, lanes, first, dim):
    scores = scores_s[: first + dim, lanes] * dim**-0.5
    keys = lax.broadcasted_iota(jnp.int32, scores.shape, 0)
    queries = lax.broadcasted_iota(jnp.int32, scores.shape, 1) + first
    return jnp.where(keys <= queries, scores, -1e30)


ACROSS = (((1,), (1,)), ((), ()))
DOWN = (((0,), (0,)), ((), ()))


def attend(qkv, out, stats, scores_s, probs_s, q_s, heads, dim):
    rows = qkv.shape[0]
    width = heads * dim
    for first in range(0, rows, dim):
        last = first + dim
        stack_heads(qkv, q_s, first, heads, dim)
        scores_s[:last, :] = lax.dot_general(qkv[:last, width : width + dim], q_s[...], ACROSS, preferred_element_type=F32)

        @pl.loop(0, heads, unroll=2)
        def _(h):
            lanes = pl.ds(pl.multiple_of(h * dim, dim), dim)
            scores = scaled_scores(scores_s, lanes, first, dim)
            top = jnp.max(scores, axis=0, keepdims=True)
            weights = jnp.exp(scores - top)
            share = 1.0 / jnp.sum(weights, axis=0, keepdims=True)
            probs_s[:last, lanes] = (weights * share).astype(BF16)
            stats[h, 0:1, first:last] = top
            stats[h, 1:2, first:last] = share

        turned = lax.dot_general(qkv[:last, width + dim :], probs_s[:last, :], DOWN, preferred_element_type=F32)
        for h in range(heads):
            out[first:last, h * dim : (h + 1) * dim] = turned[:, h * dim : (h + 1) * dim].T.astype(BF16)


def attend_backward(qkv, grad_att, grad_q, grad_kv, stats, scores_s, grad_p_s, probs_s, grad_s_s, q_s, att_s, heads, dim):
    rows = qkv.shape[0]
    width = heads * dim
    grad_kv[...] = jnp.zeros_like(grad_kv)
    for first in range(0, rows, dim):
        last = first + dim
        stack_heads(qkv, q_s, first, heads, dim)
        stack_heads(grad_att, att_s, first, heads, dim)
        scores_s[:last, :] = lax.dot_general(qkv[:last, width : width + dim], q_s[...], ACROSS, preferred_element_type=F32)
        grad_p_s[:last, :] = lax.dot_general(qkv[:last, width + dim :], att_s[...], ACROSS, preferred_element_type=F32)

        @pl.loop(0, heads, unroll=2)
        def _(h):
            lanes = pl.ds(pl.multiple_of(h * dim, dim), dim)
            scores = scaled_scores(scores_s, lanes, first, dim)
            probs = jnp.exp(scores - stats[h, 0:1, first:last]) * stats[h, 1:2, first:last]
            grad_p = grad_p_s[:last, lanes].astype(BF16).astype(F32)
            row_dot = jnp.sum(probs * grad_p, axis=0, keepdims=True)
            grad_s_s[:last, lanes] = (probs * (grad_p - row_dot) * dim**-0.5).astype(BF16)
            probs_s[:last, lanes] = probs.astype(BF16)

        turned = lax.dot_general(qkv[:last, width : width + dim], grad_s_s[:last, :], DOWN, preferred_element_type=F32)
        for h in range(heads):
            grad_q[first:last, h * dim : (h + 1) * dim] = turned[:, h * dim : (h + 1) * dim].T.astype(BF16)
        grad_kv[:last, :dim] += jnp.dot(grad_s_s[:last, :], q_s[...], preferred_element_type=F32)
        grad_kv[:last, dim:] += jnp.dot(probs_s[:last, :], att_s[...], preferred_element_type=F32)


def block_kernel(heads, dim, x_hbm, dy_hbm, gamma, beta, wq_hbm, wkv_hbm, b_q, b_kv, wo_hbm, b_o,
                 h_full, dy_full, att_out, o_part, dq_out, dkv_part, dkv_full, y_out, dh_part, o_theirs, o_chip, dh_sum, dbo, dbq, ln_stats,
                 own, bias, w_buf, wo_buf, h_buf, qkv_buf, att_buf, da_buf, dq_buf, dkv_buf, part_buf, total, stats,
                 scores_s, grad_p_s, probs_s, grad_s_s, q_s, att_s, theirs, far_in, near_in, kv_theirs, kv_far_in, kv_near_in,
                 send, recv, x_sem, dy_sem, keep_sem, w_sem, h_sem, att_sem, dq_sem, dkv_sem, part_sem, load_sem,
                 ours_sem, pair_send, pair_recv, far_send, far_recv, near_send, near_recv, free,
                 kv_ours_sem, kv_pair_send, kv_pair_recv, kv_far_send, kv_far_recv, kv_near_send, kv_near_recv, kv_send, kv_recv, kv_keep_sem, late_send, late_recv, late_sem):
    batch, rows, width = x_hbm.shape
    early = y_out.shape[0]
    half = rows // 2
    wide = width // 2
    units = 2 * batch
    scatters = batch + early
    ring = h_full.shape[1] // rows
    chips = ring // 2
    q_width = heads * dim
    kv_width = 2 * dim
    tile = 512
    me = lax.axis_index("tp")
    partner = me + 1 - 2 * lax.rem(me, 2)
    right, left, far_chip = lax.rem(me + 2, ring), lax.rem(me + ring - 2, ring), lax.rem(me + ring // 2, ring)
    OURS, NEAR, SUM, FAR, X, Y = 0, 4, 10, 13, units, units + 1

    barrier = pltpu.get_barrier_semaphore()
    for other in (left, right, partner):
        pl.semaphore_signal(barrier, inc=1, device_id={"tp": other}, device_id_type=pl.DeviceIdType.MESH)

    def remote(src, dst, sems, to):
        return pltpu.make_async_remote_copy(
            src_ref=src, dst_ref=dst, send_sem=sems[0], recv_sem=sems[1], device_id={"tp": to}, device_id_type=pl.DeviceIdType.MESH)

    def columns(low, high, act, step=tile):
        @pl.loop(low, high, step=step)
        def _(n):
            act(pl.ds(pl.multiple_of(n, step), step))

    def block(full, b, owner, first=0, count=rows):
        return full.at[b, pl.ds(pl.multiple_of(owner * rows + first, half), count)]

    def move(kind, full, b, u):
        if kind in (RIGHT, LEFT, PART):
            src, dst = own.at[u], block(full, b, me)
        elif kind in (FAR_R, FAR_L):
            src = dst = block(full, b, left, 0, half) if kind == FAR_R else block(full, b, right, half, half)
        else:
            src = dst = block(full, b, {PASS_L: left, PASS_R: right, PASS_F: far_chip}[kind])
        to = {RIGHT: right, FAR_R: right, LEFT: left, FAR_L: left}.get(kind, partner)
        return remote(src, dst, (send.at[kind, u], recv.at[kind, u]), to)

    def keep(full, b, u):
        return pltpu.make_async_copy(own.at[u], block(full, b, me), keep_sem.at[u])

    def load_x(b):
        return pltpu.make_async_copy(x_hbm.at[b], own.at[units + lax.rem(b, 2)], x_sem.at[lax.rem(b, 2)])

    def load_dy(b):
        return pltpu.make_async_copy(dy_hbm.at[b], own.at[2 * b + 1], dy_sem.at[b])

    def turn(u, h_act, dy_act):
        b = lax.div(u, 2)
        inside = jnp.logical_and(u >= 0, u < units)

        @pl.when(jnp.logical_and(inside, lax.rem(u, 2) == 0))
        def _():
            h_act(b)

        @pl.when(jnp.logical_and(inside, lax.rem(u, 2) == 1))
        def _():
            dy_act(b)

    def unit(u, act):
        turn(u, lambda b: act(h_full, b, u), lambda b: act(dy_full, b, u))

    def normalise(b):
        load_x(b).wait()
        slot = units + lax.rem(b, 2)

        @pl.loop(0, rows, step=16)
        def _(r):
            at = pl.ds(pl.multiple_of(r, 16), 16)
            x_wide = own[slot, at, :].astype(F32)
            mean = jnp.mean(x_wide, axis=-1, keepdims=True)
            centred = x_wide - mean
            inv_std = lax.rsqrt(jnp.mean(centred * centred, axis=-1, keepdims=True) + LN_EPS)
            own[2 * b, at, :] = (centred * inv_std * gamma[...] + beta[...]).astype(BF16)
            ln_stats[0, b, at, :] = jnp.broadcast_to(mean, (16, 128))
            ln_stats[1, b, at, :] = jnp.broadcast_to(inv_std, (16, 128))

        @pl.when(b + 2 < batch)
        def _():
            load_x(b + 2).start()

    def emit(full, b, u):
        for kind in (RIGHT, LEFT, PART):
            move(kind, full, b, u).start()
        keep(full, b, u).start()

    def launch(u):
        turn(u, normalise, lambda b: load_dy(b).wait())
        unit(u, emit)

    def forward(full, b, u):
        move(RIGHT, full, b, u).wait_recv()
        move(FAR_R, full, b, u).start()
        move(LEFT, full, b, u).wait_recv()
        move(FAR_L, full, b, u).start()

    def share(full, b, u):
        move(PASS_L, full, b, u).start()
        move(PASS_R, full, b, u).start()

    def share_far(full, b, u):
        move(FAR_R, full, b, u).wait_recv()
        move(FAR_L, full, b, u).wait_recv()
        move(PASS_F, full, b, u).start()

    def complete(full, b, u):
        for kind in (PART, PASS_L, PASS_R, PASS_F):
            move(kind, full, b, u).wait_recv()
        keep(full, b, u).wait()

    def retire(full, b, u):
        for kind in range(8):
            move(kind, full, b, u).wait_send()

    def load_block(full, b):
        load = pltpu.make_async_copy(full.at[b], h_buf, h_sem.at[0])
        load.start()
        load.wait()

    def project(b):
        load_block(h_full, b)

        def act(at):
            qkv_buf[:, at] = (jnp.dot(h_buf[...], w_buf[:, at], preferred_element_type=F32) + bias[:, at]).astype(BF16)

        columns(0, q_width + kv_width, act, 256)

    def store_att(b):
        return pltpu.make_async_copy(att_buf, att_out.at[b], att_sem.at[0])

    def store_part(out, b, n):
        at = pl.ds(pl.multiple_of(n, tile), tile)
        slot = lax.rem(lax.div(n, tile), 2)
        return pltpu.make_async_copy(part_buf.at[slot], out.at[b, :, at], part_sem.at[slot])

    def make_part(product, store):
        @pl.loop(0, width, step=tile)
        def _(n):
            @pl.when(n >= 2 * tile)
            def _():
                store_part(o_part, 0, n - 2 * tile).wait()

            part_buf[lax.rem(lax.div(n, tile), 2)] = product(pl.ds(pl.multiple_of(n, tile), tile)).astype(BF16)
            store(n)

        for n in (width - 2 * tile, width - tile):
            store_part(o_part, 0, n).wait()

    def project_out(b):
        make_part(lambda at: jnp.dot(att_buf[...], wo_buf[:, at], preferred_element_type=F32), lambda n: store_part(o_part, b, n).start())

    def project_out_late(b):
        again = pltpu.make_async_copy(att_out.at[b], att_buf, load_sem.at[ring])
        again.start()
        again.wait()
        project_out(b)

    def attend_and_project(b):
        @pl.when(b > 0)
        def _():
            store_att(b - 1).wait()

        attend(qkv_buf, att_buf, stats, scores_s, probs_s, q_s, heads, dim)
        store_att(b).start()

        @pl.when(b < early)
        def _():
            project_out(b)

    def grad_attended(b):
        load_block(dy_full, b)

        def act(at):
            da_buf[:, at] = lax.dot_general(h_buf[...], wo_buf[at, :], ACROSS, preferred_element_type=F32).astype(BF16)

        columns(0, q_width, act, 256)

        def add(at):
            dbo[:, at] += jnp.sum(h_buf[:, at].astype(F32).reshape(-1, 8, tile), axis=0)

        columns(0, width, add)

    def store_dq(b):
        return pltpu.make_async_copy(dq_buf, dq_out.at[b], dq_sem.at[0])

    def store_dkv(b, owner):
        return pltpu.make_async_copy(dkv_buf.at[pl.ds(owner * rows, rows)], dkv_part.at[owner, pl.ds(pl.multiple_of(b * rows, rows), rows)], dkv_sem.at[owner])

    def stored(b):
        store_dq(b).wait()
        for owner in range(ring):
            store_dkv(b, owner).wait()

    def differentiate(b):
        @pl.when(b > 0)
        def _():
            stored(b - 1)

        attend_backward(qkv_buf, da_buf, dq_buf, total, stats, scores_s, grad_p_s, probs_s, grad_s_s, q_s, att_s, heads, dim)
        dkv_buf[...] = total[...].astype(BF16)

        def add(at):
            dbq[:, at] += jnp.sum(dq_buf[:, at].astype(F32).reshape(-1, 8, 256), axis=0)

        columns(0, q_width, add, 256)
        store_dq(b).start()
        for owner in range(ring):
            store_dkv(b, owner).start()

    def grad_part(b):
        def product(at):
            from_q = lax.dot_general(dq_buf[...], w_buf[at, :q_width], ACROSS, preferred_element_type=F32)
            return from_q + lax.dot_general(dkv_buf[...], w_buf[at, q_width:], ACROSS, preferred_element_type=F32)

        make_part(product, lambda n: store_part(dh_part, b, n).start())

    def line(owner):
        return pl.ds(pl.multiple_of(owner * rows, rows), rows)

    def sourced(u, act):
        @pl.when(u < early)
        def _():
            act(o_part.at[u])

        @pl.when(u >= early)
        def _():
            act(dh_part.at[u - early])

    def mine(part, r):
        return pltpu.make_async_copy(part.at[line(lax.rem(me + 2 * r, ring))], own.at[OURS + r], ours_sem.at[r])

    def pair(part, r):
        return remote(part.at[line(lax.rem(partner + 2 * r, ring))], theirs.at[r], (pair_send.at[r], pair_recv.at[r]), partner)

    def far(u, way):
        cols = pl.ds(way * wide, wide)
        return remote(own.at[FAR + lax.rem(u, 2), :, cols], far_in.at[lax.rem(u, 3), :, cols],
                      (far_send.at[lax.rem(u, 2), way], far_recv.at[lax.rem(u, 3), way]), (right, left)[way])

    def near(u, way):
        slot = lax.rem(u, 3)
        return remote(own.at[NEAR + 2 * slot + way], near_in.at[slot, way], (near_send.at[slot, way], near_recv.at[slot, way]), (right, left)[way])

    def fetch(u):
        @pl.when(u >= 1)
        def _():
            pl.semaphore_wait(free, 1)
            for r in range(chips):
                pair(o_part.at[0], r).wait_send()

        def act(part):
            for r in range(chips):
                pair(part, r).start()
            for r in range(chips):
                mine(part, r).start()

        sourced(u, act)

    def combine(u):
        slot2, slot3 = lax.rem(u, 2), lax.rem(u, 3)
        for r in range(chips):
            mine(o_part.at[0], r).wait()
            pair(o_part.at[0], r).wait_recv()

        @pl.when(u >= 2)
        def _():
            for way in range(2):
                far(u - 2, way).wait_send()

        @pl.when(u >= 3)
        def _():
            for way in range(2):
                near(u - 3, way).wait_send()

        def chip_sum(r, at):
            return (own[OURS + r, :, at].astype(F32) + theirs[r, :, at].astype(F32)).astype(BF16)

        def act_far(at):
            own[FAR + slot2, :, at] = chip_sum(chips // 2, at)

        columns(0, width, act_far)
        for way in range(2):
            far(u, way).start()

        def act(at):
            own[NEAR + 2 * slot3, :, at] = chip_sum(1, at)
            own[NEAR + 2 * slot3 + 1, :, at] = chip_sum(chips - 1, at)
            own[SUM + slot3, :, at] = chip_sum(0, at)

        columns(0, width, act)

        @pl.when(u + 1 < scatters)
        def _():
            pl.semaphore_signal(free, inc=1, device_id={"tp": partner}, device_id_type=pl.DeviceIdType.MESH)

    def relay(u):
        slot = lax.rem(u, 3)
        for way in range(2):
            far(u, way).wait_recv()
        for way in range(2):
            def act(at):
                place = NEAR + 2 * slot + way
                own[place, :, at] = (own[place, :, at].astype(F32) + far_in[slot, :, at].astype(F32)).astype(BF16)

            columns(way * wide, way * wide + wide, act)
        for way in range(2):
            near(u, way).start()

    def scatter_x(u):
        return pltpu.make_async_copy(x_hbm.at[u], own.at[X], load_sem.at[ring + 1])

    def store_y(out, b):
        return pltpu.make_async_copy(own.at[Y], out.at[b], load_sem.at[ring + 2])

    def finish(u):
        slot = lax.rem(u, 3)
        for way in range(2):
            near(u, way).wait_recv()

        @pl.when(u > 0)
        def _():
            store_y(y_out, 0).wait()

        def whole(at):
            return own[SUM + slot, :, at].astype(F32) + near_in[slot, 0, :, at].astype(F32) + near_in[slot, 1, :, at].astype(F32)

        @pl.when(u < early)
        def _():
            scatter_x(u).wait()

            def act(at):
                own[Y, :, at] = (own[X, :, at].astype(F32) + whole(at) + b_o[:, at]).astype(BF16)

            columns(0, width, act)
            store_y(y_out, u).start()

        @pl.when(u >= early)
        def _():
            def act(at):
                own[Y, :, at] = whole(at).astype(BF16)

            columns(0, width, act)
            store_y(dh_sum, u - early).start()

        @pl.when(u + 1 < early)
        def _():
            scatter_x(u + 1).start()

    core = lax.rem(me, 2)

    def late_pair(v, chip):
        return remote(o_part.at[early + v, line(2 * chip + 1 - core)], o_theirs.at[v, pl.ds(chip * rows, rows)], (late_send.at[v, chip], late_recv.at[v, chip]), partner)

    def late_loads(v):
        copies = [pltpu.make_async_copy(o_part.at[early + v, line(2 * chip + core)], h_buf.at[pl.ds(chip * rows, rows)], late_sem.at[chip]) for chip in range(chips)]
        return copies + [pltpu.make_async_copy(o_theirs.at[v], h_buf.at[pl.ds(chips * rows, chips * rows)], late_sem.at[chips])]

    def late_stores(v):
        return [pltpu.make_async_copy(h_buf.at[pl.ds(chip * rows, rows)], o_chip.at[chip, pl.ds(pl.multiple_of(v * rows, rows), rows)],
                                      late_sem.at[chips + 1 + chip]) for chip in range(chips)]

    def late_sum(v):
        for chip in range(chips):
            late_pair(v, chip).wait_recv()

        @pl.when(v > 0)
        def _():
            for copy in late_stores(v - 1):
                copy.wait()

        for copy in late_loads(v):
            copy.start()
        for copy in late_loads(v):
            copy.wait()

        def act(at):
            mine_, theirs_ = h_buf[: chips * rows, at].astype(F32), h_buf[chips * rows :, at].astype(F32)
            h_buf[: chips * rows, at] = (mine_ + theirs_).astype(BF16)

        columns(0, width, act)
        for copy in late_stores(v):
            copy.start()

    pick = lambda ref, n: ref.at[:, pl.ds(n * kv_width, kv_width)]
    kv_ours = [pick(probs_s, 0), pick(probs_s, 1), pick(probs_s, 2), pick(grad_s_s, 0)]
    kv_far, kv_sum = pick(grad_s_s, 1), pick(da_buf, 2)
    kv_near = [pick(da_buf, 0), pick(da_buf, 1)]
    kv_rows = batch * rows
    kv_half = kv_rows // 2

    def kv_mine(r):
        return pltpu.make_async_copy(dkv_part.at[lax.rem(me + 2 * r, ring)], kv_ours[r], kv_ours_sem.at[r])

    def kv_pair(r):
        return remote(dkv_part.at[lax.rem(partner + 2 * r, ring)], kv_theirs.at[r], (kv_pair_send.at[r], kv_pair_recv.at[r]), partner)

    def kv_far_copy(way):
        at = pl.ds(way * kv_half, kv_half)
        return remote(kv_far.at[at], kv_far_in.at[at], (kv_far_send.at[way], kv_far_recv.at[way]), (right, left)[way])

    def kv_near_copy(way):
        return remote(kv_near[way], kv_near_in.at[way], (kv_near_send.at[way], kv_near_recv.at[way]), (right, left)[way])

    def kv_move(kind):
        if kind in (RIGHT, LEFT, PART):
            src, dst = kv_sum, dkv_full.at[me]
        elif kind in (FAR_R, FAR_L):
            src = dst = dkv_full.at[left, pl.ds(0, kv_half)] if kind == FAR_R else dkv_full.at[right, pl.ds(kv_half, kv_half)]
        else:
            src = dst = dkv_full.at[{PASS_L: left, PASS_R: right, PASS_F: far_chip}[kind]]
        to = {RIGHT: right, FAR_R: right, LEFT: left, FAR_L: left}.get(kind, partner)
        return remote(src, dst, (kv_send.at[kind], kv_recv.at[kind]), to)

    def kv_keep():
        return pltpu.make_async_copy(kv_sum, dkv_full.at[me], kv_keep_sem.at[0])

    def kv_steps():
        def start():
            stored(batch - 1)
            for r in range(chips):
                kv_pair(r).start()
                kv_mine(r).start()

        def sum_chip():
            for r in range(chips):
                kv_mine(r).wait()
                kv_pair(r).wait_recv()
            chip = lambda r: (kv_ours[r][...].astype(F32) + kv_theirs[r].astype(F32)).astype(BF16)
            kv_far[...] = chip(chips // 2)
            for way in range(2):
                kv_far_copy(way).start()
            kv_near[0][...] = chip(1)
            kv_near[1][...] = chip(chips - 1)

        def relay_far():
            for way in range(2):
                kv_far_copy(way).wait_recv()
            for way in range(2):
                at = slice(way * kv_half, way * kv_half + kv_half)
                kv_near[way][at, :] = (kv_near[way][at, :].astype(F32) + kv_far_in[at, :].astype(F32)).astype(BF16)
            for way in range(2):
                kv_near_copy(way).start()

        def sum_all():
            for way in range(2):
                kv_near_copy(way).wait_recv()
            chip = kv_ours[0][...].astype(F32) + kv_theirs[0].astype(F32)
            kv_sum[...] = (chip + kv_near_in[0].astype(F32) + kv_near_in[1].astype(F32)).astype(BF16)
            for kind in (RIGHT, LEFT, PART):
                kv_move(kind).start()
            kv_keep().start()

        def spread():
            kv_move(RIGHT).wait_recv()
            kv_move(FAR_R).start()
            kv_move(LEFT).wait_recv()
            kv_move(FAR_L).start()
            kv_move(PASS_L).start()
            kv_move(PASS_R).start()

        def spread_far():
            kv_move(FAR_R).wait_recv()
            kv_move(FAR_L).wait_recv()
            kv_move(PASS_F).start()

        def settle_kv():
            for kind in (PART, PASS_L, PASS_R, PASS_F):
                kv_move(kind).wait_recv()
            kv_keep().wait()
            for kind in range(8):
                kv_move(kind).wait_send()
            for way in range(2):
                kv_far_copy(way).wait_send()
                kv_near_copy(way).wait_send()
            for r in range(chips):
                kv_pair(r).wait_send()

        return start, sum_chip, relay_far, sum_all, spread, spread_far, settle_kv

    load_x(0).start()
    load_dy(0).start()
    load_x(1).start()
    weights = (pltpu.make_async_copy(wq_hbm, w_buf.at[:, pl.ds(0, q_width)], w_sem.at[0]),
               pltpu.make_async_copy(wkv_hbm, w_buf.at[:, pl.ds(q_width, kv_width)], w_sem.at[1]),
               pltpu.make_async_copy(wo_hbm, wo_buf, w_sem.at[2]))
    normalise(0)
    load_dy(0).wait()
    pl.semaphore_wait(barrier, 3)
    emit(h_full, 0, 0)
    emit(dy_full, 0, 1)
    for copy in weights:
        copy.start()
    for b in range(1, batch):
        load_dy(b).start()
    dbo[...] = jnp.zeros_like(dbo)
    dbq[...] = jnp.zeros_like(dbq)
    bias[:, pl.ds(0, q_width)] = b_q[...].reshape(1, q_width)
    bias[:, pl.ds(q_width, kv_width)] = b_kv[...].reshape(1, kv_width)
    for copy in weights:
        copy.wait()

    lead = units - 2

    @pl.loop(0, lead + scatters + 3)
    def _(s):
        t = s - lead
        when = lambda low, high: pl.when(jnp.logical_and(t >= low, t < high))

        @pl.when(s < units)
        def _():
            unit(s, forward)

        launch(s + 2)

        @pl.when(s < units)
        def _():
            unit(s, share)

        unit(s - 2, retire)

        @when(1, scatters + 1)
        def _():
            combine(t - 1)

        @when(2, scatters + 2)
        def _():
            relay(t - 2)

        @when(0, scatters)
        def _():
            fetch(t)

        @when(3, 5)
        def _():
            grad_part(batch - 5 + t)

        turn(s - 2, attend_and_project, differentiate)

        @pl.when(jnp.logical_and(s < units - 1, lax.rem(s, 2) == 1))
        def _():
            @pl.when(s >= 3)
            def _():
                grad_part(lax.div(s - 3, 2))

        unit(s - 1, share_far)
        unit(s - 1, complete)
        turn(s - 1, project, grad_attended)

        @when(3, scatters + 3)
        def _():
            finish(t - 3)

        @when(2, 3)
        def _():
            scatter_x(0).start()

        for n, act in enumerate(kv_steps()):
            @when(4 + n, 5 + n)
            def _():
                act()

        @when(6, 6 + batch - early)
        def _():
            late_sum(t - 6)

        @when(4, 5)
        def _():
            store_att(batch - 1).wait()

        @when(5, 5 + batch - early)
        def _():
            project_out_late(early + t - 5)
            for chip in range(chips):
                late_pair(t - 5, chip).start()

    for copy in late_stores(batch - early - 1):
        copy.wait()
    for chip in range(chips):
        for v in range(batch - early):
            late_pair(v, chip).wait_send()
    store_y(y_out, 0).wait()
    for r in range(chips):
        pair(o_part.at[0], r).wait_send()
    for way in range(2):
        for u in (scatters - 2, scatters - 1):
            far(u, way).wait_send()
        for u in (scatters - 3, scatters - 2, scatters - 1):
            near(u, way).wait_send()


def attention_block(x_loc, dy_loc, gamma, beta, w_q, w_kv, b_q, b_kv, w_o, b_o, early, ring, dim):
    batch, rows, width = x_loc.shape
    q_width, kv_width = w_q.shape[1], w_kv.shape[1]
    qkv_width = q_width + kv_width
    seq = rows * ring
    units = 2 * batch
    chips = ring // 2
    heads = q_width // dim
    hbm = pl.BlockSpec(memory_space=pl.ANY)
    vmem = pl.BlockSpec(memory_space=pltpu.VMEM)
    dma = pltpu.SemaphoreType.DMA
    full = lambda n, w: jax.ShapeDtypeStruct((n, seq, w), BF16)
    at_home = lambda n: jax.ShapeDtypeStruct((n, rows, width), BF16)
    half_seq = jax.ShapeDtypeStruct((batch - early, chips * rows, width), BF16)
    owned = jax.ShapeDtypeStruct((ring, batch * rows, kv_width), BF16)
    lo, hi = (lambda *shape: pltpu.VMEM(shape, BF16)), (lambda *shape: pltpu.VMEM(shape, F32))
    return pl.pallas_call(
        functools.partial(block_kernel, heads, dim),
        name="attention_block",
        out_shape=(full(batch, width), full(batch, width), full(batch, q_width), full(batch, width), full(batch, q_width), owned, owned, at_home(early),
                   full(batch, width), half_seq, jax.ShapeDtypeStruct((chips, (batch - early) * rows, width), BF16), at_home(batch),
                   jax.ShapeDtypeStruct((8, width), F32), jax.ShapeDtypeStruct((8, q_width), F32), jax.ShapeDtypeStruct((2, batch, rows, 128), F32)),
        in_specs=[hbm, hbm, vmem, vmem, hbm, hbm, vmem, vmem, hbm, vmem],
        out_specs=(hbm,) * 12 + (vmem, vmem, vmem),
        scratch_shapes=[
            lo(units + 2, rows, width), hi(1, qkv_width), lo(width, qkv_width), lo(q_width, width), lo(seq, width), lo(seq, qkv_width), lo(seq, q_width), lo(seq, q_width),
            lo(seq, q_width), lo(seq, kv_width), lo(2, seq, 512), hi(seq, kv_width), hi(heads, 8, seq),
            hi(seq, q_width), hi(seq, q_width), lo(seq, q_width), lo(seq, q_width), lo(q_width, dim), lo(q_width, dim),
            lo(chips, rows, width), lo(3, rows, width), lo(3, 2, rows, width),
            lo(chips, batch * rows, kv_width), lo(batch * rows, kv_width), lo(2, batch * rows, kv_width),
            dma((8, units)), dma((8, units)), dma((2,)), dma((batch,)), dma((units,)), dma((3,)), dma((1,)), dma((1,)), dma((1,)), dma((ring,)), dma((2,)),
            dma((ring + 3,)),
            dma((chips,)), dma((chips,)), dma((chips,)), dma((2, 2)), dma((3, 2)), dma((3, 2)), dma((3, 2)), pltpu.SemaphoreType.REGULAR,
            dma((chips,)), dma((chips,)), dma((chips,)), dma((2,)), dma((2,)), dma((2,)), dma((2,)), dma((8,)), dma((8,)), dma((1,)),
            dma((batch - early, chips)), dma((batch - early, chips)), dma((2 * chips + 1,))],
        compiler_params=pltpu.CompilerParams(collective_id=0, has_side_effects=True, vmem_limit_bytes=VMEM_LIMIT),
        cost_estimate=pl.CostEstimate(flops=8 * batch * seq * width * qkv_width, bytes_accessed=12 * batch * seq * width, transcendentals=0),
    )(x_loc, dy_loc, gamma, beta, w_q, w_kv, b_q, b_kv, w_o, b_o)


def norm_backward_kernel(dh, x, dy, ln_stats, gamma, dx, sums, x_hat_s, scaled_s):
    rows, width = x.shape[1:]
    tile = 512

    @pl.when(pl.program_id(0) == 0)
    def _():
        sums[...] = jnp.zeros_like(sums)

    mean, inv_std = ln_stats[0, 0, :, :1], ln_stats[1, 0, :, :1]
    by_lane = lambda v: v[:, :128] + v[:, 128:256] + v[:, 256:384] + v[:, 384:]
    by_sublane = lambda v: jnp.sum(v.reshape(-1, 8, tile), axis=0)

    def gather_sums(n, carry):
        plain, along = carry
        at = pl.ds(pl.multiple_of(n * tile, tile), tile)
        grad_h = dh[0, :, at].astype(F32)
        x_hat = (x[0, :, at].astype(F32) - mean) * inv_std
        scaled = grad_h * gamma[:, at]
        x_hat_s[:, at] = x_hat
        scaled_s[:, at] = scaled
        sums[0, :, at] += by_sublane(grad_h * x_hat)
        sums[1, :, at] += by_sublane(grad_h)
        return plain + by_lane(scaled), along + by_lane(scaled * x_hat)

    zero = jnp.zeros((rows, 128), F32)
    plain, along = lax.fori_loop(0, width // tile, gather_sums, (zero, zero), unroll=2)
    plain = jnp.sum(plain, axis=-1, keepdims=True) / width
    along = jnp.sum(along, axis=-1, keepdims=True) / width

    @pl.loop(0, width // tile, unroll=2)
    def _(n):
        at = pl.ds(pl.multiple_of(n * tile, tile), tile)
        grad_in = inv_std * (scaled_s[:, at] - plain - x_hat_s[:, at] * along)
        dx[0, :, at] = (dy[0, :, at].astype(F32) + grad_in).astype(BF16)


def norm_backward(grad_h, x_loc, dy_loc, ln_stats, gamma):
    batch, rows, width = x_loc.shape
    block = pl.BlockSpec((1, rows, width), lambda b: (b, 0, 0))
    still = lambda shape: pl.BlockSpec(shape, lambda b: (0,) * len(shape))
    return pl.pallas_call(
        norm_backward_kernel,
        name="norm_backward",
        grid=(batch,),
        out_shape=(jax.ShapeDtypeStruct(x_loc.shape, BF16), jax.ShapeDtypeStruct((2, 8, width), F32)),
        in_specs=[block, block, block, pl.BlockSpec((2, 1, rows, 128), lambda b: (0, b, 0, 0)), still(gamma.shape)],
        out_specs=(block, still((2, 8, width))),
        scratch_shapes=[pltpu.VMEM((rows, width), F32), pltpu.VMEM((rows, width), F32)],
        compiler_params=pltpu.CompilerParams(vmem_limit_bytes=VMEM_LIMIT),
        cost_estimate=pl.CostEstimate(flops=60 * batch * rows * width, bytes_accessed=8 * batch * rows * width, transcendentals=0),
    )(grad_h, x_loc, dy_loc, ln_stats, gamma)


def turn_rows(rows, dst, place):
    count, cols = rows.shape
    chunk = 512

    @pl.loop(0, count, step=chunk)
    def _(k):
        at = pl.ds(pl.multiple_of(k, chunk), chunk)
        dst[place : place + cols, at] = rows[at, :].T


def whole(shape):
    return pl.BlockSpec(shape, lambda n: (0,) * len(shape), pipeline_mode=pl.Buffered(1))


def grad_wq_kernel(rows, grad_q, kv_owned, h, out_q, out_kv, kv_sums, turned, kv_lines):
    tokens, q_width = grad_q.shape
    ring, owned, kv_width = kv_owned.shape
    first = q_width - kv_width

    @pl.when(pl.program_id(0) == 0)
    def _():
        turn_rows(grad_q, turned, 0)

        @pl.loop(0, owned, step=rows)
        def _(r):
            for owner in range(ring):
                place = pl.multiple_of(r * ring + owner * rows, rows)
                kv_lines[pl.ds(place, rows), :] = kv_owned[owner, pl.ds(pl.multiple_of(r, rows), rows), :]

        turn_rows(kv_lines, turned, q_width)
        kv_sums[...] = jnp.zeros_like(kv_sums)

        @pl.loop(0, tokens, step=512)
        def _(k):
            kv_sums[...] += jnp.sum(kv_lines[pl.ds(pl.multiple_of(k, 512), 512), :].astype(F32).reshape(-1, 8, kv_width), axis=0)

    @pl.loop(0, out_q.shape[0], step=256)
    def _(n):
        at = pl.ds(pl.multiple_of(n, 256), 256)
        out_q[at, :first] = jnp.dot(turned[:first, :], h[:, at], preferred_element_type=F32).T
        late = jnp.dot(turned[first:, :], h[:, at], preferred_element_type=F32).T
        out_q[at, first:] = late[:, :kv_width]
        out_kv[at, :] = late[:, kv_width:]


def grad_wq(grad_q, kv_owned, h, rows):
    tokens, q_width = grad_q.shape
    kv_width = kv_owned.shape[2]
    width = h.shape[1]
    tile = 512
    return pl.pallas_call(
        functools.partial(grad_wq_kernel, rows),
        name="grad_wq",
        grid=(width // tile,),
        out_shape=(jax.ShapeDtypeStruct((width, q_width), F32), jax.ShapeDtypeStruct((width, kv_width), F32), jax.ShapeDtypeStruct((8, kv_width), F32)),
        in_specs=[whole(grad_q.shape), whole(kv_owned.shape), pl.BlockSpec((tokens, tile), lambda n: (0, n))],
        out_specs=(pl.BlockSpec((tile, q_width), lambda n: (n, 0)), pl.BlockSpec((tile, kv_width), lambda n: (n, 0)), pl.BlockSpec((8, kv_width), lambda n: (0, 0))),
        scratch_shapes=[pltpu.VMEM((q_width + kv_width, tokens), BF16), pltpu.VMEM((tokens, kv_width), BF16)],
        compiler_params=pltpu.CompilerParams(vmem_limit_bytes=VMEM_LIMIT),
        cost_estimate=pl.CostEstimate(flops=2 * tokens * (q_width + kv_width) * width, bytes_accessed=2 * tokens * width + 4 * (q_width + kv_width) * width, transcendentals=0),
    )(grad_q, kv_owned, h)


def settle(values, count):
    block = pl.BlockSpec((1,) + values.shape[1:], lambda b: (b, 0, 0))

    def body(src, dst):
        dst[...] = src[...]

    return pl.pallas_call(
        body, name="settle", grid=(values.shape[0],), out_shape=jax.ShapeDtypeStruct((count,) + values.shape[1:], values.dtype), in_specs=[block], out_specs=block,
        compiler_params=pltpu.CompilerParams(vmem_limit_bytes=VMEM_LIMIT),
        cost_estimate=pl.CostEstimate(flops=values.size * 100, bytes_accessed=values.size * 4, transcendentals=0))(values)


def finish_y_kernel(o_hbm, x_hbm, b_o, _, y_hbm, o_buf, x_buf, o_sem, x_sem, y_sem):
    count, rows, width = o_hbm.shape
    first = x_hbm.shape[0] - count
    tile = 512
    load_o = lambda v: pltpu.make_async_copy(o_hbm.at[v], o_buf.at[v], o_sem.at[v])
    load_x = lambda v: pltpu.make_async_copy(x_hbm.at[first + v], x_buf.at[v], x_sem.at[v])
    store_y = lambda v: pltpu.make_async_copy(o_buf.at[v], y_hbm.at[first + v], y_sem.at[v])
    for v in range(count):
        load_o(v).start()
        load_x(v).start()

    @pl.loop(0, count)
    def _(v):
        load_o(v).wait()
        load_x(v).wait()

        @pl.loop(0, width, step=tile)
        def _(n):
            at = pl.ds(pl.multiple_of(n, tile), tile)
            o_buf[v, :, at] = (x_buf[v, :, at].astype(F32) + o_buf[v, :, at].astype(F32) + b_o[:, at]).astype(BF16)

        store_y(v).start()

    for v in range(count):
        store_y(v).wait()


def finish_y(o_late, x_loc, b_o, started):
    count, rows, width = o_late.shape
    hbm = pl.BlockSpec(memory_space=pl.ANY)
    dma = pltpu.SemaphoreType.DMA((count,))
    return pl.pallas_call(
        finish_y_kernel, name="finish_y", out_shape=jax.ShapeDtypeStruct(x_loc.shape, BF16),
        in_specs=[hbm, hbm, pl.BlockSpec(memory_space=pltpu.VMEM), hbm], out_specs=hbm, input_output_aliases={3: 0},
        scratch_shapes=[pltpu.VMEM(o_late.shape, BF16), pltpu.VMEM(o_late.shape, BF16), dma, dma, dma],
        compiler_params=pltpu.CompilerParams(vmem_limit_bytes=VMEM_LIMIT),
        cost_estimate=pl.CostEstimate(flops=o_late.size * 100, bytes_accessed=o_late.size * 6, transcendentals=0))(o_late, x_loc, b_o, started)


def sum_kernel(ring, rows, out, parts, gathered, send, recv):
    me = lax.axis_index("tp")
    barrier = pltpu.get_barrier_semaphore()
    others = [lax.rem(me + k, ring) for k in range(1, ring)]
    for other in others:
        pl.semaphore_signal(barrier, inc=1, device_id={"tp": other}, device_id_type=pl.DeviceIdType.MESH)
    groups = rows.shape[2] // 128
    for kind in range(2):
        row = jnp.sum(rows[kind], axis=0, keepdims=True)
        for n in range(groups):
            parts[kind * groups + n : kind * groups + n + 1, :] = row[:, n * 128 : (n + 1) * 128]
    pl.semaphore_wait(barrier, ring - 1)

    def copy(k):
        return pltpu.make_async_remote_copy(
            src_ref=parts, dst_ref=gathered.at[me], send_sem=send.at[k], recv_sem=recv.at[k],
            device_id={"tp": lax.rem(me + k, ring)}, device_id_type=pl.DeviceIdType.MESH)

    for k in range(1, ring):
        copy(k).start()
    gathered[me] = parts[...]
    for k in range(1, ring):
        copy(k).wait_recv()
    total = gathered[0]
    for k in range(1, ring):
        total = total + gathered[k]
    out[...] = total
    for k in range(1, ring):
        copy(k).wait_send()


def sum_over_ring(rows, ring):
    vmem = pl.BlockSpec(memory_space=pltpu.VMEM)
    shape = (2 * rows.shape[2] // 128, 128)
    return pl.pallas_call(
        functools.partial(sum_kernel, ring),
        name="sum_over_ring",
        out_shape=jax.ShapeDtypeStruct(shape, F32),
        in_specs=[vmem],
        out_specs=vmem,
        scratch_shapes=[pltpu.VMEM(shape, F32), pltpu.VMEM((ring,) + shape, F32), pltpu.SemaphoreType.DMA((ring,)), pltpu.SemaphoreType.DMA((ring,))],
        compiler_params=pltpu.CompilerParams(collective_id=2, has_side_effects=True),
    )(rows)


def solution(mesh):
    ring = mesh.shape["tp"]

    def device_block(x_loc, ln_gamma, ln_beta, w_q, b_q, w_kv, b_kv, w_o, b_o, dy_loc):
        head_dim = w_kv.shape[1] // 2
        batch, own_rows, width = x_loc.shape
        early = batch // 4
        normed_full, dy_full, merged, _, grad_q, _, kv_owned, y_early, _, _, o_chip, grad_h, bo_rows, bq_rows, ln_stats = attention_block(
            x_loc, dy_loc, ln_gamma[None, :], ln_beta[None, :], w_q, w_kv, b_q, b_kv, w_o, b_o[None, :], early, ring, head_dim)
        lines = [[i for i in range(ring) if i % 2 == core] for core in range(2)]
        o_late = lax.psum_scatter(o_chip, "tp", scatter_dimension=0, tiled=True, axis_index_groups=lines).reshape(batch - early, own_rows, width)

        flat = lambda v: v.reshape(-1, v.shape[-1])
        grad_x, parts = norm_backward(grad_h, x_loc, dy_loc, ln_stats, ln_gamma[None, :])
        sums = sum_over_ring(parts, ring).reshape(2, width)
        wo_grad = jnp.einsum("bse,bsd->ed", merged, dy_full, preferred_element_type=jnp.float32)
        wq_grad, wkv_grad, kv_sums = grad_wq(flat(grad_q), kv_owned, flat(normed_full), own_rows)
        grad_bq, grad_bkv, grad_bo = jnp.sum(bq_rows, axis=0), jnp.sum(kv_sums, axis=0), jnp.sum(bo_rows, axis=0)
        y_loc = finish_y(o_late, x_loc, b_o[None, :], settle(y_early, batch))
        return (y_loc, grad_x, sums[0], sums[1], wq_grad, grad_bq, wkv_grad, grad_bkv, wo_grad, grad_bo)

    return jax.shard_map(
        device_block,
        mesh=mesh,
        in_specs=(P("dp", "tp", None), P(None), P(None), P(None, "tp"), P("tp"), P(None, None), P(None), P("tp", None), P(None), P("dp", "tp", None)),
        out_specs=(P("dp", "tp", None), P("dp", "tp", None), P("dp"), P("dp"), P("dp", "tp"), P(("dp", "tp")), P("dp", None), P("dp"), P(("dp", "tp"), None), P("dp")),
        check_vma=False,
    )
```
